32 devices in a mesh: dp: 4 (over z), expert: 8 (over y, x, core).
Axes of the slice: x: 2, y: 2, z: 4, core: 2. Of those that a mesh axis runs over, the one named last changes fastest.
Arguments:
- tokens: bfloat16 [256, 192, 1024], P(None, ('dp', 'expert')), may hold values from -200 to 200
- grad_out: bfloat16 [256, 192, 1024], P(None, ('dp', 'expert')), may hold values from -6 to 6
- slot_out: bfloat16 [512, 192, 1024], P('expert', 'dp'), may hold values from -6 to 6
- slot_params: bfloat16 [512, 1024], P('expert'), may hold values from -2 to 2
Outputs:
- grad_tokens: bfloat16 [256, 192, 1024], P(None, ('dp', 'expert'))
- grad_slot_out: bfloat16 [512, 192, 1024], P('expert', 'dp')
- grad_params: float32 [512, 1024], P('expert', 'dp')
The draws below stay inside these ranges and needn't reach their ends.
All inputs are finite; a program needn't handle non-finite values.
Results may differ from the reference program's by a relative error of at most 0.018.
Values may be sent and summed in bfloat16 or wider, within the bound.
A program may use at most 128 MiB of HBM per device.

```python
import math
import jax
import jax.numpy as jnp

D = 1024
SLOTS = 512
PATCHES = 256
IMAGES = 192


def slot_table(key):
    inner = jax.random.fold_in(key, 11)
    spread = 2.0 / math.sqrt(D)
    values = jnp.clip(jax.random.normal(inner, (SLOTS, D)) * spread, -6.0 * spread, 6.0 * spread)
    return values.astype(jnp.bfloat16).astype(jnp.float32)


def draw_slot_params(key, part):
    return slot_table(key).astype(jnp.bfloat16)


def draw_tokens(key, part):
    key_base = jax.random.fold_in(jax.random.fold_in(key, 23), 0)
    values = jnp.clip(jax.random.normal(key_base, (PATCHES, IMAGES, D)), -6.0, 6.0)
    return values.astype(jnp.bfloat16)


def block_levels(own_key, dims, pieces, smallest, largest):
    level, own = 1.0, jax.random.fold_in(own_key, 6)
    for axis_at, parts in pieces:
        steps = jnp.exp(jax.random.uniform(jax.random.fold_in(own, axis_at), (parts,), jnp.float32, smallest / len(pieces), largest / len(pieces)))
        level = level * jnp.repeat(steps, dims[axis_at] // parts).reshape([-1 if axis == axis_at else 1 for axis in range(len(dims))])
    return level


def gaussian(rng, dims, width, reach, cuts=(), kind=jnp.bfloat16):
    loudness = block_levels(rng, dims, cuts, -0.22, 0.18) if cuts else 1.0
    drawn = jax.random.normal(rng, dims, jnp.float32) * width * loudness
    return jnp.minimum(jnp.maximum(drawn, -reach), reach).astype(kind)


def setup_inputs(seed: int = 0) -> dict:
    key_of = jax.random.split(jax.random.key(seed), 5)
    return {
        "tokens": draw_tokens(jax.random.fold_in(key_of[4], 71), 0),
        "grad_out": gaussian(key_of[1], (PATCHES, IMAGES, D), 1.0, 6.0, ((1, 32),)),
        "slot_out": gaussian(key_of[2], (SLOTS, IMAGES, D), 1.0, 6.0, ((0, 8), (1, 4))),
        "slot_params": draw_slot_params(jax.random.fold_in(key_of[4], 71), 0),
    }


def reference(tokens, grad_out, slot_out, slot_params):
    tok_wide = tokens.astype(jnp.float32)
    grad_wide = grad_out.astype(jnp.float32)
    param_wide = slot_params.astype(jnp.float32)
    logits = jnp.einsum('tbd,sd->tbs', tok_wide, param_wide)
    combine = jax.nn.softmax(logits, axis=-1)
    combine_low = combine.astype(jnp.bfloat16)
    grad_slot = jnp.einsum('tbs,tbd->sbd', combine_low.astype(jnp.float32), grad_wide).astype(jnp.bfloat16)
    grad_comb = jnp.einsum('tbd,sbd->tbs', grad_wide, slot_out.astype(jnp.float32))
    rowdot = jnp.sum(combine * grad_comb, axis=-1, keepdims=True)
    grad_logits = (combine * (grad_comb - rowdot)).astype(jnp.bfloat16)
    logit_wide = grad_logits.astype(jnp.float32)
    grad_tok = jnp.einsum('tbs,sd->tbd', logit_wide, param_wide).astype(jnp.bfloat16)
    grad_params = jnp.einsum('tbs,tbd->sd', logit_wide, tok_wide)
    return grad_tok, grad_slot, grad_params
```

```python
import functools

import jax
import jax.numpy as jnp
from jax import lax
from jax.experimental import pallas as pl
from jax.experimental.pallas import tpu as pltpu
from jax.sharding import PartitionSpec as P

BF = jnp.bfloat16
F32 = jnp.float32
GROUP = 16
LANES = 128


def flip(index, mask, size):
    total, bit = 0, 1
    while bit < size:
        total = total + ((index // bit + mask // bit) % 2) * bit
        bit *= 2
    return total


def send_order(n, core):
    if n != 8:
        return list(range(n - 1, 0, -1))
    masks = []
    for low in range(2):
        masks += [6 + low - 4 * core, 2 + low + 2 * core, 4 + low + 2 * core]
    return masks + [1]


def rows_last(lhs, rhs):
    return lax.dot_general(lhs, rhs, (((1,), (1,)), ((), ())), preferred_element_type=F32)


def exchange_kernel(
    n, m, tok_hbm, go_hbm, so_hbm, par_hbm,
    grec, gt_out, gp_out,
    tok, go, so, par, allp, stage, rows, gs, comb, gt, acc, psend, precv, xsend, xrecv, gp,
    local_sem, p_send, p_recv, q_send, q_recv, a_send, a_recv, g_send, g_recv,
    z_send, z_recv, x_send, x_recv,
):
    me = lax.axis_index("expert")
    mz = lax.axis_index("dp")
    core = me % 2
    imgs = tok.shape[0]
    own = par.shape[0]
    all_img = so.shape[1]
    cols = allp.shape[1] // m
    width = allp.shape[1]
    slots = allp.shape[0]
    my_cols = pl.ds(pl.multiple_of(mz * cols, 128), cols)
    my_rows = pl.ds(pl.multiple_of(me * own, GROUP), own)

    loads = [
        pltpu.make_async_copy(src, dst, local_sem.at[i])
        for i, (src, dst) in enumerate([(par_hbm, par), (so_hbm, so), (tok_hbm, tok), (go_hbm, go)])
    ]
    for load in loads:
        load.start()

    barrier = pltpu.get_barrier_semaphore()
    for k in range(1, n):
        pl.semaphore_signal(barrier, inc=1, device_id=(mz, flip(me, k, n)), device_id_type=pl.DeviceIdType.MESH)
    for k in range(1, m):
        pl.semaphore_signal(barrier, inc=1, device_id=(flip(mz, k, m), me), device_id_type=pl.DeviceIdType.MESH)
    pl.semaphore_wait(barrier, n + m - 2)

    def to_expert(src, dst, send, recv, k):
        return pltpu.make_async_remote_copy(
            src_ref=src, dst_ref=dst, send_sem=send.at[k], recv_sem=recv.at[k],
            device_id=(mz, flip(me, k, n)), device_id_type=pl.DeviceIdType.MESH,
        )

    def to_dp(src, dst, send, recv, k):
        return pltpu.make_async_remote_copy(
            src_ref=src, dst_ref=dst, send_sem=send.at[k], recv_sem=recv.at[k],
            device_id=(flip(mz, k, m), me), device_id_type=pl.DeviceIdType.MESH,
        )

    loads[0].wait()
    p_copies = [to_expert(par.at[:, my_cols], allp.at[my_rows, my_cols], p_send, p_recv, k) for k in range(1, n)]
    for copy in p_copies:
        copy.start()
    allp[my_rows, my_cols] = par[:, my_cols]

    loads[1].wait()
    out_r = lax.broadcasted_iota(jnp.int32, (imgs * GROUP, GROUP * all_img), 0)
    in_c = lax.broadcasted_iota(jnp.int32, (imgs * GROUP, GROUP * all_img), 1)
    base = in_c - (out_r % GROUP) * all_img - out_r // GROUP

    def relayout(dest, out):
        pick = jnp.where(base == dest * imgs, 1.0, 0.0).astype(BF)

        def one(g, carry):
            s0 = pl.multiple_of(g * GROUP, GROUP)
            block = so[pl.ds(s0, GROUP)].reshape(GROUP * all_img, width)
            moved = jnp.dot(pick, block, preferred_element_type=F32).astype(BF)
            out[:, pl.ds(s0, GROUP), :] = moved.reshape(imgs, GROUP, width)
            return carry

        lax.fori_loop(0, own // GROUP, one, 0)

    order = send_order(n, core)
    a_copies = []
    for k in order:
        relayout(flip(me, k, n), stage.at[k])
        copy = to_expert(stage.at[k], rows.at[me], a_send, a_recv, k)
        copy.start()
        a_copies.append(copy)
    relayout(me, rows.at[me])

    for copy in p_copies:
        copy.wait_recv()
    q_copies = [to_dp(allp.at[:, my_cols], allp.at[:, my_cols], q_send, q_recv, k) for k in range(1, m)]
    for copy in q_copies:
        copy.start()
    loads[2].wait()
    loads[3].wait()
    for copy in q_copies:
        copy.wait_recv()

    def forward(b, carry):
        logits = rows_last(allp[...], tok[b])
        peak = jnp.max(logits, axis=0, keepdims=True)
        raised = jnp.exp(logits - peak)
        weights = raised / jnp.sum(raised, axis=0, keepdims=True)
        comb[b] = weights
        grads = jnp.dot(weights.astype(BF), go[b], preferred_element_type=F32).astype(BF)
        gs[:, b] = grads.reshape(n, own, width)
        return carry

    lax.fori_loop(0, imgs, forward, 0)

    keep = pltpu.make_async_copy(gs.at[me], grec.at[me], local_sem.at[4])
    keep.start()
    g_copies = []
    for k in order:
        copy = to_expert(gs.at[flip(me, k, n)], grec.at[me], g_send, g_recv, k)
        copy.start()
        g_copies.append(copy)

    for copy in a_copies:
        copy.wait_recv()
    acc[...] = jnp.zeros_like(acc)

    def backward(b, carry):
        grad_comb = rows_last(rows[:, b].reshape(slots, width), go[b])
        weights = comb[b]
        rowdot = jnp.sum(weights * grad_comb, axis=0, keepdims=True)
        wide = weights * (grad_comb - rowdot)
        acc[...] += jnp.dot(wide.astype(BF), tok[b], preferred_element_type=F32)
        gt[b] = jnp.dot(wide.T.astype(BF), allp[...], preferred_element_type=F32).astype(BF)
        return carry

    lax.fori_loop(0, imgs, backward, 0)

    for k in range(1, m):
        there = flip(mz, k, m)
        psend[k] = acc[:, pl.ds(pl.multiple_of(there * cols, 128), cols)].astype(BF)
    z_copies = [to_dp(psend.at[k], precv.at[k], z_send, z_recv, k) for k in range(1, m)]
    for copy in z_copies:
        copy.start()
    put = pltpu.make_async_copy(gt, gt_out, local_sem.at[5])
    put.start()
    for copy in z_copies:
        copy.wait_recv()
    total = acc[:, my_cols]
    for k in range(1, m):
        total = total + precv[k].astype(F32)
    acc[:, my_cols] = total
    for k in range(1, n):
        there = flip(me, k, n)
        xsend[k] = acc[pl.ds(pl.multiple_of(there * own, GROUP), own), my_cols].astype(BF)
    x_copies = [to_expert(xsend.at[k], xrecv.at[k], x_send, x_recv, k) for k in range(1, n)]
    for copy in x_copies:
        copy.start()
    for copy in x_copies:
        copy.wait_recv()
    owned = acc[my_rows, my_cols]
    for k in range(1, n):
        owned = owned + xrecv[k].astype(F32)
    gp[...] = owned
    give = pltpu.make_async_copy(gp, gp_out, local_sem.at[6])
    give.start()

    for copy in g_copies:
        copy.wait_recv()
    for copy in p_copies + a_copies + q_copies + g_copies + z_copies + x_copies:
        copy.wait_send()
    keep.wait()
    put.wait()
    give.wait()


def exchange(n, m, tok, go, so, par):
    imgs, patches, width = tok.shape
    own, all_img, _ = so.shape
    slots, cols = own * n, width // m
    dma = pltpu.SemaphoreType.DMA
    return pl.pallas_call(
        functools.partial(exchange_kernel, n, m),
        out_shape=(
            jax.ShapeDtypeStruct((n, imgs, own, width), BF),
            jax.ShapeDtypeStruct((imgs, patches, width), BF),
            jax.ShapeDtypeStruct((own, cols), F32),
        ),
        in_specs=[pl.BlockSpec(memory_space=pl.ANY)] * 4,
        out_specs=(pl.BlockSpec(memory_space=pl.ANY),) * 3,
        scratch_shapes=[
            pltpu.VMEM((imgs, patches, width), BF),
            pltpu.VMEM((imgs, patches, width), BF),
            pltpu.VMEM((own, all_img, width), BF),
            pltpu.VMEM((own, width), BF),
            pltpu.VMEM((slots, width), BF),
            pltpu.VMEM((n, imgs, own, width), BF),
            pltpu.VMEM((n, imgs, own, width), BF),
            pltpu.VMEM((n, imgs, own, width), BF),
            pltpu.VMEM((imgs, slots, patches), F32),
            pltpu.VMEM((imgs, patches, width), BF),
            pltpu.VMEM((slots, width), F32),
            pltpu.VMEM((m, slots, cols), BF),
            pltpu.VMEM((m, slots, cols), BF),
            pltpu.VMEM((n, own, cols), BF),
            pltpu.VMEM((n, own, cols), BF),
            pltpu.VMEM((own, cols), F32),
            dma((7,)),
            dma((n,)), dma((n,)), dma((m,)), dma((m,)),
            dma((n,)), dma((n,)), dma((n,)), dma((n,)),
            dma((m,)), dma((m,)), dma((n,)), dma((n,)),
        ],
        compiler_params=pltpu.CompilerParams(
            collective_id=0, has_side_effects=True, vmem_limit_bytes=66 * 1000 * 1000
        ),
    )(tok, go, so, par)


AXES = ((2, (4, 5, 1)), (4, (2, 3, 1)))


def side_spot(which, index):
    high = index // 4 if which == 0 else (index // 2) % 2
    return high * 2 + index % 2


def paired_kernel(
    n, m, tok_hbm, go_hbm, so_hbm, par_hbm,
    done, last, gt, gp,
    tok, go, mate, so, par, allp, stage, rows, gs, comb, gcf, low, low_send, gc_send, gc_recv,
    grec, acc, ksend, krecv, red, psend, precv, xsend, xrecv,
    local_sem, keep_sem, p_send, p_recv, q_send, q_recv, f_send, f_recv, k_send, k_recv, o_send, o_recv, a_send, a_recv, w_send, w_recv,
    c_send, c_recv, g_send, g_recv, z_send, z_recv, x_send, x_recv,
):
    me = lax.axis_index("expert")
    mz = lax.axis_index("dp")
    imgs = tok.shape[0]
    half = imgs // 2
    own = par.shape[0]
    all_img = so.shape[1]
    slots, width = allp.shape
    patches = tok.shape[1]
    cols = width // m
    quarter = slots // 4
    my_cols = pl.ds(pl.multiple_of(mz * cols, 128), cols)
    my_rows = pl.ds(pl.multiple_of(me * own, GROUP), own)
    sides = ((me // 2) % 2, me // 4)

    def piece(which, other, p):
        side = 1 - sides[which] if other else sides[which]
        start = p * 2 * quarter + side * quarter if which == 0 else side * 2 * quarter + p * quarter
        return pl.ds(pl.multiple_of(start, quarter), quarter)

    loads = [
        pltpu.make_async_copy(src, dst, local_sem.at[i])
        for i, (src, dst) in enumerate([(par_hbm, par), (so_hbm, so), (tok_hbm, tok), (go_hbm, go)])
    ]
    for i in (0, 3, 1, 2):
        loads[i].start()

    barrier = pltpu.get_barrier_semaphore()
    for k in range(1, n):
        pl.semaphore_signal(barrier, inc=1, device_id=(mz, flip(me, k, n)), device_id_type=pl.DeviceIdType.MESH)
    for k in range(1, m):
        pl.semaphore_signal(barrier, inc=1, device_id=(flip(mz, k, m), me), device_id_type=pl.DeviceIdType.MESH)
    pl.semaphore_wait(barrier, n + m - 2)

    def to_expert(src, dst, send, recv, k):
        return pltpu.make_async_remote_copy(
            src_ref=src, dst_ref=dst, send_sem=send, recv_sem=recv,
            device_id=(mz, flip(me, k, n)), device_id_type=pl.DeviceIdType.MESH,
        )

    def to_dp(src, dst, send, recv):
        return [
            pltpu.make_async_remote_copy(
                src_ref=src(k), dst_ref=dst(k), send_sem=send.at[k], recv_sem=recv.at[k],
                device_id=(flip(mz, k, m), me), device_id_type=pl.DeviceIdType.MESH,
            )
            for k in range(1, m)
        ]

    sent = []

    def launch(copies):
        for copy in copies:
            copy.start()
        sent.extend(copies)
        return copies

    def arrive(copies):
        for copy in copies:
            copy.wait_recv()

    loads[0].wait()
    p_copies = launch([
        to_expert(par.at[:, my_cols], allp.at[my_rows, my_cols], p_send.at[k], p_recv.at[k], k)
        for k in range(2, n, 2)
    ])
    allp[my_rows, my_cols] = par[:, my_cols]
    loads[3].wait()
    o_copies = launch([
        to_expert(go.at[pl.ds(q * half, half)], mate.at[q], o_send.at[q], o_recv.at[q], AXES[q][0]) for q in range(2)
    ])

    loads[1].wait()
    out_r = lax.broadcasted_iota(jnp.int32, (imgs * GROUP, GROUP * all_img), 0)
    in_c = lax.broadcasted_iota(jnp.int32, (imgs * GROUP, GROUP * all_img), 1)
    base = in_c - (out_r % GROUP) * all_img - (out_r // GROUP) % half
    first = out_r < half * GROUP

    def relayout(q, dest, out):
        own_at = dest * imgs + q * half
        mate_at = flip(dest, AXES[q][0], n) * imgs + q * half
        pick = jnp.where(base == jnp.where(first, own_at, mate_at), 1.0, 0.0).astype(BF)

        def one(g, carry):
            s0 = pl.multiple_of(g * GROUP, GROUP)
            block = so[pl.ds(s0, GROUP)].reshape(GROUP * all_img, width)
            moved = jnp.dot(pick, block, preferred_element_type=F32).astype(BF)
            out[:, pl.ds(s0, GROUP), :] = moved.reshape(imgs, GROUP, width)
            return carry

        lax.fori_loop(0, own // GROUP, one, 0)

    a_copies = []
    for i in range(3):
        for q in range(2):
            k = AXES[q][1][i]
            relayout(q, flip(me, k, n), stage.at[q, i])
            a_copies += launch([
                to_expert(stage.at[q, i], rows.at[q, side_spot(q, me)], a_send.at[q, i], a_recv.at[q, i], k)
            ])
    for q in range(2):
        relayout(q, me, rows.at[q, side_spot(q, me)])

    arrive(p_copies)
    q_copies = []
    for i in range(n // 2):
        block = allp.at[pl.ds(pl.multiple_of(flip(me, 2 * i, n) * own, GROUP), own), my_cols]
        q_copies += launch(to_dp(lambda k: block, lambda k: block, q_send.at[i], q_recv.at[i]))
    loads[2].wait()
    arrive(q_copies)
    f_copies = []
    for i in range(n // 2):
        block = allp.at[pl.ds(pl.multiple_of(flip(me, 2 * i, n) * own, GROUP), own)]
        f_copies += launch([to_expert(block, block, f_send.at[i], f_recv.at[i], 1)])
    arrive(f_copies)

    w_copies = []
    for q in range(2):

        def forward(t, carry):
            b = q * half + t
            logits = rows_last(allp[...], tok[b])
            peak = jnp.max(logits, axis=0, keepdims=True)
            raised = jnp.exp(logits - peak)
            comb[b] = raised / jnp.sum(raised, axis=0, keepdims=True)
            for p in range(2):
                low[q, t, p * quarter : (p + 1) * quarter] = comb[b, piece(q, False, p)].astype(BF)
                low_send[q, t, p * quarter : (p + 1) * quarter] = comb[b, piece(q, True, p)].astype(BF)
            return carry

        lax.fori_loop(0, half, forward, 0)
        w_copies += launch([
            to_expert(low_send.at[q], low.at[q, pl.ds(half, half)], w_send.at[q], w_recv.at[q], AXES[q][0])
        ])

    def slot_grads(q, i, grads_in):
        out = jnp.dot(low[q, i], grads_in, preferred_element_type=F32).astype(BF)
        gs[q, :, i] = out.reshape(4, own, width)

    def comb_grads(q, i, grads_in):
        return rows_last(rows[q, :, i].reshape(4 * own, width), grads_in)

    for q in range(2):

        def own_slots(t, carry):
            slot_grads(q, t, go[q * half + t])
            return carry

        lax.fori_loop(0, half, own_slots, 0)

    arrive(o_copies)
    arrive(a_copies)
    c_copies = []
    for q in range(2):

        def mate_comb(t, carry):
            gc_send[q, t] = comb_grads(q, half + t, mate[q, t]).astype(BF)
            return carry

        lax.fori_loop(0, half, mate_comb, 0)
        c_copies += launch([to_expert(gc_send.at[q], gc_recv.at[q], c_send.at[q], c_recv.at[q], AXES[q][0])])

    chunks = own // GROUP
    keeps = []

    def landing(holder, images, j):
        if j == chunks - 1:
            return last.at[holder, images]
        return grec.at[holder, images, pl.ds(j * GROUP, GROUP)]

    def return_grads(h, parts):
        part = pl.ds(h * half, half)
        for j in parts:
            for i in range(3):
                for q in range(2):
                    k = AXES[q][1][i]
                    holder = flip(me, AXES[q][0], n) if h else me
                    to_expert(
                        gs.at[q, side_spot(q, flip(me, k, n)), part, pl.ds(j * GROUP, GROUP)],
                        landing(holder, pl.ds(q * half, half), j), g_send.at[j], g_recv.at[j], k,
                    ).start()
            for q in range(2):
                holder = flip(me, AXES[q][0], n) if h else me
                keep = pltpu.make_async_copy(
                    gs.at[q, side_spot(q, me), part, pl.ds(j * GROUP, GROUP)],
                    landing(holder, pl.ds(q * half, half), j), keep_sem.at[h, q, j],
                )
                keep.start()
                keeps.append(keep)

    def grads_moved(j):
        every = last.at[: n - 2] if j == chunks - 1 else grec.at[: n - 2, :, pl.ds(j * GROUP, GROUP)]
        return to_expert(every, every, g_send.at[j], g_recv.at[j], 1)

    return_grads(0, range(chunks))
    arrive(w_copies)
    for q in range(2):

        def mate_slots(t, carry):
            slot_grads(q, half + t, mate[q, t])
            return carry

        lax.fori_loop(0, half, mate_slots, 0)
    return_grads(1, range(chunks - 1))

    for q in range(2):

        def own_comb(t, carry):
            grads = comb_grads(q, t, go[q * half + t])
            for p in range(2):
                gcf[q * half + t, piece(q, False, p)] = grads[p * quarter : (p + 1) * quarter]
            return carry

        lax.fori_loop(0, half, own_comb, 0)
    acc[...] = jnp.zeros_like(acc)
    arrive(c_copies)
    for q in range(2):

        def backward(t, carry):
            b = q * half + t
            for p in range(2):
                gcf[b, piece(q, True, p)] = gc_recv[q, t, p * quarter : (p + 1) * quarter].astype(F32)
            grad_comb = gcf[b]
            weights = comb[b]
            rowdot = jnp.sum(weights * grad_comb, axis=0, keepdims=True)
            wide = weights * (grad_comb - rowdot)
            gcf[b] = wide
            acc[...] += jnp.dot(wide.astype(BF), tok[b], preferred_element_type=F32)
            return carry

        lax.fori_loop(0, half, backward, 0)

    core = me % 2
    for i in range(n // 2):
        ksend[i] = acc[pl.ds(pl.multiple_of((2 * i + 1 - core) * own, GROUP), own)].astype(BF)
    k_copies = launch([to_expert(ksend, krecv, k_send.at[0], k_recv.at[0], 1)])
    arrive(k_copies)
    for i in range(n // 2):
        red[i] = acc[pl.ds(pl.multiple_of((2 * i + core) * own, GROUP), own)] + krecv[i].astype(F32)
    for k in range(1, m):
        there = flip(mz, k, m)
        psend[k] = red[:, :, pl.ds(pl.multiple_of(there * cols, 128), cols)].astype(BF)
    z_copies = launch(to_dp(lambda k: psend.at[k], lambda k: precv.at[k], z_send, z_recv))

    def token_grads(b, carry):
        gt[b] = jnp.dot(gcf[b].T.astype(BF), allp[...], preferred_element_type=F32).astype(BF)
        return carry

    lax.fori_loop(0, imgs, token_grads, 0)
    arrive(z_copies)
    total = red[:, :, my_cols]
    for k in range(1, m):
        total = total + precv[k].astype(F32)
    red[:, :, my_cols] = total
    for k in range(2, n, 2):
        xsend[k // 2] = red[flip(me, k, n) // 2, :, my_cols].astype(BF)
    x_copies = launch([
        to_expert(xsend.at[k // 2], xrecv.at[k // 2], x_send.at[k], x_recv.at[k], k) for k in range(2, n, 2)
    ])
    return_grads(1, (chunks - 1,))
    for keep in keeps:
        keep.wait()
    for j in range(chunks - 1):
        grads_moved(j).wait_recv()

        def swap(c, carry):
            lanes = pl.ds(pl.multiple_of(c * LANES, LANES), LANES)
            block = grec[:, :, j * GROUP : (j + 1) * GROUP, lanes].reshape(n * imgs, GROUP, LANES)
            done[j * GROUP : (j + 1) * GROUP, :, lanes] = jnp.swapaxes(block, 0, 1)
            return carry

        lax.fori_loop(0, width // LANES, swap, 0)
    arrive(x_copies)
    owned = red[me // 2, :, my_cols]
    for k in range(2, n, 2):
        owned = owned + xrecv[k // 2].astype(F32)
    gp[...] = owned
    for copy in sent:
        copy.wait_send()
    for j in range(chunks):
        grads_moved(j).wait_send()
    grads_moved(chunks - 1).wait_recv()


def paired_exchange(n, m, tok, go, so, par):
    imgs, patches, width = tok.shape
    own, all_img, _ = so.shape
    slots, cols, half = own * n, width // m, imgs // 2
    dma = pltpu.SemaphoreType.DMA
    return pl.pallas_call(
        functools.partial(paired_kernel, n, m),
        out_shape=(
            pltpu.VMEM((own - GROUP, all_img, width), BF),
            pltpu.VMEM((n, imgs, GROUP, width), BF),
            pltpu.VMEM((imgs, patches, width), BF),
            pltpu.VMEM((own, cols), F32),
        ),
        in_specs=[pl.BlockSpec(memory_space=pl.ANY)] * 4,
        out_specs=(pl.BlockSpec(memory_space=pltpu.VMEM),) * 4,
        scratch_shapes=[
            pltpu.VMEM((imgs, patches, width), BF),
            pltpu.VMEM((imgs, patches, width), BF),
            pltpu.VMEM((2, half, patches, width), BF),
            pltpu.VMEM((own, all_img, width), BF),
            pltpu.VMEM((own, width), BF),
            pltpu.VMEM((slots, width), BF),
            pltpu.VMEM((2, 3, imgs, own, width), BF),
            pltpu.VMEM((2, 4, imgs, own, width), BF),
            pltpu.VMEM((2, 4, imgs, own, width), BF),
            pltpu.VMEM((imgs, slots, patches), F32),
            pltpu.VMEM((imgs, slots, patches), F32),
            pltpu.VMEM((2, imgs, slots // 2, patches), BF),
            pltpu.VMEM((2, half, slots // 2, patches), BF),
            pltpu.VMEM((2, half, slots // 2, patches), BF),
            pltpu.VMEM((2, half, slots // 2, patches), BF),
            pltpu.VMEM((n, imgs, own - GROUP, width), BF),
            pltpu.VMEM((slots, width), F32),
            pltpu.VMEM((n // 2, own, width), BF),
            pltpu.VMEM((n // 2, own, width), BF),
            pltpu.VMEM((n // 2, own, width), F32),
            pltpu.VMEM((m, n // 2, own, cols), BF),
            pltpu.VMEM((m, n // 2, own, cols), BF),
            pltpu.VMEM((n // 2, own, cols), BF),
            pltpu.VMEM((n // 2, own, cols), BF),
            dma((4,)), dma((2, 2, own // GROUP)),
            dma((n,)), dma((n,)), dma((n // 2, m)), dma((n // 2, m)),
            dma((n // 2,)), dma((n // 2,)), dma((1,)), dma((1,)),
            dma((2,)), dma((2,)), dma((2, 3)), dma((2, 3)), dma((2,)), dma((2,)),
            dma((2,)), dma((2,)), dma((own // GROUP,)), dma((own // GROUP,)),
            dma((m,)), dma((m,)), dma((n,)), dma((n,)),
        ],
        compiler_params=pltpu.CompilerParams(
            collective_id=0, has_side_effects=True, vmem_limit_bytes=56 * 1000 * 1000
        ),
    )(tok, go, so, par)


def settle_kernel(arrived, gp_in, out, gp_out):
    out[...] = jnp.swapaxes(arrived[...], 0, 1)
    gp_out[...] = gp_in[...]


def settle(arrived, grad_par):
    all_img, own, width = arrived.shape
    small = pl.BlockSpec((GROUP, grad_par.shape[1]), lambda i: (i, 0))
    return pl.pallas_call(
        settle_kernel,
        grid=(own // GROUP,),
        out_shape=(
            jax.ShapeDtypeStruct((own, all_img, width), BF),
            jax.ShapeDtypeStruct(grad_par.shape, F32),
        ),
        in_specs=[pl.BlockSpec((all_img, GROUP, width), lambda i: (0, i, 0)), small],
        out_specs=(pl.BlockSpec((GROUP, all_img, width), lambda i: (i, 0, 0)), small),
    )(arrived, grad_par)


def finish_kernel(done, last, gt, gp, slot_out, tok_out, par_out, turned, sem):
    own = done.shape[0]
    copies = [
        pltpu.make_async_copy(done, slot_out.at[pl.ds(0, own)], sem.at[0]),
        pltpu.make_async_copy(gt, tok_out, sem.at[1]),
        pltpu.make_async_copy(gp, par_out, sem.at[2]),
    ]
    for copy in copies:
        copy.start()
    group, all_img, width = turned.shape

    def swap(c, carry):
        lanes = pl.ds(pl.multiple_of(c * LANES, LANES), LANES)
        turned[:, :, lanes] = jnp.swapaxes(last[:, :, :, lanes].reshape(all_img, group, LANES), 0, 1)
        return carry

    lax.fori_loop(0, width // LANES, swap, 0)
    copies.append(pltpu.make_async_copy(turned, slot_out.at[pl.ds(own, group)], sem.at[3]))
    copies[3].start()
    for copy in copies:
        copy.wait()


def finish(done, last, gt, gp):
    own, all_img, width = done.shape
    return pl.pallas_call(
        finish_kernel,
        out_shape=(
            jax.ShapeDtypeStruct((own + GROUP, all_img, width), BF),
            jax.ShapeDtypeStruct(gt.shape, BF),
            jax.ShapeDtypeStruct(gp.shape, F32),
        ),
        in_specs=[pl.BlockSpec(memory_space=pltpu.VMEM)] * 4,
        out_specs=(pl.BlockSpec(memory_space=pl.ANY),) * 3,
        scratch_shapes=[pltpu.VMEM((GROUP, all_img, width), BF), pltpu.SemaphoreType.DMA((4,))],
        compiler_params=pltpu.CompilerParams(vmem_limit_bytes=16 * 1000 * 1000),
    )(done, last, gt, gp)


def per_device(n, m, tokens, grad_out, slot_out, slot_params):
    tok = jnp.transpose(tokens, (1, 0, 2))
    go = jnp.transpose(grad_out, (1, 0, 2))
    if n == 8 and tok.shape[0] % 2 == 0:
        grad_slot, grad_tok, grad_par = finish(*paired_exchange(n, m, tok, go, slot_out, slot_params))
    else:
        arrived, grad_tok, grad_par = exchange(n, m, tok, go, slot_out, slot_params)
        own, all_img, width = slot_out.shape
        grad_slot, grad_par = settle(arrived.reshape(all_img, own, width), grad_par)
    return jnp.transpose(grad_tok, (1, 0, 2)), grad_slot, grad_par


def solution(mesh):
    return jax.shard_map(
        functools.partial(per_device, mesh.shape["expert"], mesh.shape["dp"]),
        mesh=mesh,
        in_specs=(
            P(None, ("dp", "expert"), None),
            P(None, ("dp", "expert"), None),
            P("expert", "dp", None),
            P("expert", None),
        ),
        out_specs=(P(None, ("dp", "expert"), None), P("expert", "dp", None), P("expert", "dp")),
        check_vma=False,
    )
```

```python
import functools

import jax
import jax.numpy as jnp
from jax import lax
from jax.experimental import pallas as pl
from jax.experimental.pallas import tpu as pltpu
from jax.sharding import PartitionSpec as P

BF = jnp.bfloat16
F32 = jnp.float32
GROUP = 16
LANES = 128


def flip(index, mask, size):
    total, bit = 0, 1
    while bit < size:
        total = total + ((index // bit + mask // bit) % 2) * bit
        bit *= 2
    return total


def send_order(n, core):
    if n != 8:
        return list(range(n - 1, 0, -1))
    masks = []
    for low in range(2):
        masks += [6 + low - 4 * core, 2 + low + 2 * core, 4 + low + 2 * core]
    return masks + [1]


def rows_last(lhs, rhs):
    return lax.dot_general(lhs, rhs, (((1,), (1,)), ((), ())), preferred_element_type=F32)


def exchange_kernel(
    n, m, tok_hbm, go_hbm, so_hbm, par_hbm,
    grec, gt_out, gp_out,
    tok, go, so, par, allp, stage, rows, gs, comb, gt, acc, psend, precv, xsend, xrecv, gp,
    local_sem, p_send, p_recv, q_send, q_recv, a_send, a_recv, g_send, g_recv,
    z_send, z_recv, x_send, x_recv,
):
    me = lax.axis_index("expert")
    mz = lax.axis_index("dp")
    core = me % 2
    imgs = tok.shape[0]
    own = par.shape[0]
    all_img = so.shape[1]
    cols = allp.shape[1] // m
    width = allp.shape[1]
    slots = allp.shape[0]
    my_cols = pl.ds(pl.multiple_of(mz * cols, 128), cols)
    my_rows = pl.ds(pl.multiple_of(me * own, GROUP), own)

    loads = [
        pltpu.make_async_copy(src, dst, local_sem.at[i])
        for i, (src, dst) in enumerate([(par_hbm, par), (so_hbm, so), (tok_hbm, tok), (go_hbm, go)])
    ]
    for load in loads:
        load.start()

    barrier = pltpu.get_barrier_semaphore()
    for k in range(1, n):
        pl.semaphore_signal(barrier, inc=1, device_id=(mz, flip(me, k, n)), device_id_type=pl.DeviceIdType.MESH)
    for k in range(1, m):
        pl.semaphore_signal(barrier, inc=1, device_id=(flip(mz, k, m), me), device_id_type=pl.DeviceIdType.MESH)
    pl.semaphore_wait(barrier, n + m - 2)

    def to_expert(src, dst, send, recv, k):
        return pltpu.make_async_remote_copy(
            src_ref=src, dst_ref=dst, send_sem=send.at[k], recv_sem=recv.at[k],
            device_id=(mz, flip(me, k, n)), device_id_type=pl.DeviceIdType.MESH,
        )

    def to_dp(src, dst, send, recv, k):
        return pltpu.make_async_remote_copy(
            src_ref=src, dst_ref=dst, send_sem=send.at[k], recv_sem=recv.at[k],
            device_id=(flip(mz, k, m), me), device_id_type=pl.DeviceIdType.MESH,
        )

    loads[0].wait()
    p_copies = [to_expert(par.at[:, my_cols], allp.at[my_rows, my_cols], p_send, p_recv, k) for k in range(1, n)]
    for copy in p_copies:
        copy.start()
    allp[my_rows, my_cols] = par[:, my_cols]

    loads[1].wait()
    out_r = lax.broadcasted_iota(jnp.int32, (imgs * GROUP, GROUP * all_img), 0)
    in_c = lax.broadcasted_iota(jnp.int32, (imgs * GROUP, GROUP * all_img), 1)
    base = in_c - (out_r % GROUP) * all_img - out_r // GROUP

    def relayout(dest, out):
        pick = jnp.where(base == dest * imgs, 1.0, 0.0).astype(BF)

        def one(g, carry):
            s0 = pl.multiple_of(g * GROUP, GROUP)
            block = so[pl.ds(s0, GROUP)].reshape(GROUP * all_img, width)
            moved = jnp.dot(pick, block, preferred_element_type=F32).astype(BF)
            out[:, pl.ds(s0, GROUP), :] = moved.reshape(imgs, GROUP, width)
            return carry

        lax.fori_loop(0, own // GROUP, one, 0)

    order = send_order(n, core)
    a_copies = []
    for k in order:
        relayout(flip(me, k, n), stage.at[k])
        copy = to_expert(stage.at[k], rows.at[me], a_send, a_recv, k)
        copy.start()
        a_copies.append(copy)
    relayout(me, rows.at[me])

    for copy in p_copies:
        copy.wait_recv()
    q_copies = [to_dp(allp.at[:, my_cols], allp.at[:, my_cols], q_send, q_recv, k) for k in range(1, m)]
    for copy in q_copies:
        copy.start()
    loads[2].wait()
    loads[3].wait()
    for copy in q_copies:
        copy.wait_recv()

    def forward(b, carry):
        logits = rows_last(allp[...], tok[b])
        peak = jnp.max(logits, axis=0, keepdims=True)
        raised = jnp.exp(logits - peak)
        weights = raised / jnp.sum(raised, axis=0, keepdims=True)
        comb[b] = weights
        grads = jnp.dot(weights.astype(BF), go[b], preferred_element_type=F32).astype(BF)
        gs[:, b] = grads.reshape(n, own, width)
        return carry

    lax.fori_loop(0, imgs, forward, 0)

    keep = pltpu.make_async_copy(gs.at[me], grec.at[me], local_sem.at[4])
    keep.start()
    g_copies = []
    for k in order:
        copy = to_expert(gs.at[flip(me, k, n)], grec.at[me], g_send, g_recv, k)
        copy.start()
        g_copies.append(copy)

    for copy in a_copies:
        copy.wait_recv()
    acc[...] = jnp.zeros_like(acc)

    def backward(b, carry):
        grad_comb = rows_last(rows[:, b].reshape(slots, width), go[b])
        weights = comb[b]
        rowdot = jnp.sum(weights * grad_comb, axis=0, keepdims=True)
        wide = weights * (grad_comb - rowdot)
        acc[...] += jnp.dot(wide.astype(BF), tok[b], preferred_element_type=F32)
        gt[b] = jnp.dot(wide.T.astype(BF), allp[...], preferred_element_type=F32).astype(BF)
        return carry

    lax.fori_loop(0, imgs, backward, 0)

    for k in range(1, m):
        there = flip(mz, k, m)
        psend[k] = acc[:, pl.ds(pl.multiple_of(there * cols, 128), cols)].astype(BF)
    z_copies = [to_dp(psend.at[k], precv.at[k], z_send, z_recv, k) for k in range(1, m)]
    for copy in z_copies:
        copy.start()
    put = pltpu.make_async_copy(gt, gt_out, local_sem.at[5])
    put.start()
    for copy in z_copies:
        copy.wait_recv()
    total = acc[:, my_cols]
    for k in range(1, m):
        total = total + precv[k].astype(F32)
    acc[:, my_cols] = total
    for k in range(1, n):
        there = flip(me, k, n)
        xsend[k] = acc[pl.ds(pl.multiple_of(there * own, GROUP), own), my_cols].astype(BF)
    x_copies = [to_expert(xsend.at[k], xrecv.at[k], x_send, x_recv, k) for k in range(1, n)]
    for copy in x_copies:
        copy.start()
    for copy in x_copies:
        copy.wait_recv()
    owned = acc[my_rows, my_cols]
    for k in range(1, n):
        owned = owned + xrecv[k].astype(F32)
    gp[...] = owned
    give = pltpu.make_async_copy(gp, gp_out, local_sem.at[6])
    give.start()

    for copy in g_copies:
        copy.wait_recv()
    for copy in p_copies + a_copies + q_copies + g_copies + z_copies + x_copies:
        copy.wait_send()
    keep.wait()
    put.wait()
    give.wait()


def exchange(n, m, tok, go, so, par):
    imgs, patches, width = tok.shape
    own, all_img, _ = so.shape
    slots, cols = own * n, width // m
    dma = pltpu.SemaphoreType.DMA
    return pl.pallas_call(
        functools.partial(exchange_kernel, n, m),
        out_shape=(
            jax.ShapeDtypeStruct((n, imgs, own, width), BF),
            jax.ShapeDtypeStruct((imgs, patches, width), BF),
            jax.ShapeDtypeStruct((own, cols), F32),
        ),
        in_specs=[pl.BlockSpec(memory_space=pl.ANY)] * 4,
        out_specs=(pl.BlockSpec(memory_space=pl.ANY),) * 3,
        scratch_shapes=[
            pltpu.VMEM((imgs, patches, width), BF),
            pltpu.VMEM((imgs, patches, width), BF),
            pltpu.VMEM((own, all_img, width), BF),
            pltpu.VMEM((own, width), BF),
            pltpu.VMEM((slots, width), BF),
            pltpu.VMEM((n, imgs, own, width), BF),
            pltpu.VMEM((n, imgs, own, width), BF),
            pltpu.VMEM((n, imgs, own, width), BF),
            pltpu.VMEM((imgs, slots, patches), F32),
            pltpu.VMEM((imgs, patches, width), BF),
            pltpu.VMEM((slots, width), F32),
            pltpu.VMEM((m, slots, cols), BF),
            pltpu.VMEM((m, slots, cols), BF),
            pltpu.VMEM((n, own, cols), BF),
            pltpu.VMEM((n, own, cols), BF),
            pltpu.VMEM((own, cols), F32),
            dma((7,)),
            dma((n,)), dma((n,)), dma((m,)), dma((m,)),
            dma((n,)), dma((n,)), dma((n,)), dma((n,)),
            dma((m,)), dma((m,)), dma((n,)), dma((n,)),
        ],
        compiler_params=pltpu.CompilerParams(
            collective_id=0, has_side_effects=True, vmem_limit_bytes=66 * 1000 * 1000
        ),
    )(tok, go, so, par)


NEAR = (1, 2, 3, 4, 5)
AXES = ((2, (4, 5, 1)), (4, (2, 3, 1)))


def side_spot(which, index):
    high = index // 4 if which == 0 else (index // 2) % 2
    return high * 2 + index % 2


def paired_kernel(
    n, m, tok_hbm, go_hbm, so_hbm, par_hbm,
    done, last, gt, gp,
    tok, go, mate, so, par, allp, stage, rows, gs, comb, gcf, low, low_send, gc_send, gc_recv,
    grec, acc, ksend, krecv, red, psend, precv, xsend, xrecv,
    ready, corner, local_sem, keep_sem, p_sems, q_sems, f_sems, k_sems, o_sems, a_sems, w_sems,
    c_sems, g_sems, z_sems, x_sems,
):
    me = lax.axis_index("expert")
    mz = lax.axis_index("dp")
    imgs = tok.shape[0]
    half = imgs // 2
    own = par.shape[0]
    all_img = so.shape[1]
    slots, width = allp.shape
    patches = tok.shape[1]
    cols = width // m
    quarter = slots // 4
    my_cols = pl.ds(pl.multiple_of(mz * cols, 128), cols)
    my_rows = pl.ds(pl.multiple_of(me * own, GROUP), own)
    sides = ((me // 2) % 2, me // 4)

    def piece(which, other, p):
        side = 1 - sides[which] if other else sides[which]
        start = p * 2 * quarter + side * quarter if which == 0 else side * 2 * quarter + p * quarter
        return pl.ds(pl.multiple_of(start, quarter), quarter)

    loads = [
        pltpu.make_async_copy(src, dst, local_sem.at[i])
        for i, (src, dst) in enumerate([(par_hbm, par), (so_hbm, so), (tok_hbm, tok), (go_hbm, go)])
    ]
    for i in (0, 3, 1, 2):
        loads[i].start()

    gate = n - 1
    barrier = pltpu.get_barrier_semaphore()

    def tell(sem, plane, index):
        pl.semaphore_signal(sem, inc=1, device_id=(plane, index), device_id_type=pl.DeviceIdType.MESH)

    for k in NEAR:

        @pl.when(flip(me, k, n) != gate)
        def greet():
            tell(barrier, mz, flip(me, k, n))

    @pl.when(me != gate)
    def meet():
        pl.semaphore_wait(barrier, len(NEAR))

    @pl.when(me == gate - 1)
    def admit():
        tell(ready, mz, gate)

    @pl.when(me == gate)
    def enter():
        pl.semaphore_wait(ready, 1)

    tell(corner, mz, flip(me, 2, n))

    def meet_corner():
        pl.semaphore_wait(corner, 1)

        @pl.when(me == gate)
        def announce():
            for k in range(1, m):
                tell(barrier, flip(mz, k, m), gate)

    def meet_planes():
        @pl.when(me == gate)
        def spread():
            pl.semaphore_wait(barrier, m - 1)
            for k in range(1, n):
                tell(ready, mz, flip(me, k, n))

        @pl.when(me != gate)
        def follow():
            pl.semaphore_wait(ready, 1)

    def to_expert(src, dst, send, recv, k):
        return pltpu.make_async_remote_copy(
            src_ref=src, dst_ref=dst, send_sem=send, recv_sem=recv,
            device_id=(mz, flip(me, k, n)), device_id_type=pl.DeviceIdType.MESH,
        )

    def to_dp(src, dst, sems):
        for k in range(1, m):
            pltpu.make_async_remote_copy(
                src_ref=src(k), dst_ref=dst(k), send_sem=sems.at[0], recv_sem=sems.at[1],
                device_id=(flip(mz, k, m), me), device_id_type=pl.DeviceIdType.MESH,
            ).start()

    def send(src, dst, sems, k):
        to_expert(src, dst, sems.at[0], sems.at[1], k).start()

    groups = []

    def group(every, sems):
        groups.append(to_expert(every, every, sems.at[0], sems.at[1], 1))
        return groups[-1]

    def arrive(moved):
        moved.wait_recv()

    loads[0].wait()
    def send_params(peers):
        for k in peers:
            send(par.at[:, my_cols], allp.at[my_rows, my_cols], p_sems, k)

    send_params((2, 4))
    loads[3].wait()
    for q in range(2):
        send(go.at[pl.ds(q * half, half)], mate.at[q], o_sems, AXES[q][0])
    o_moved = group(mate, o_sems)
    meet_corner()
    send_params((6,))
    p_moved = group(allp.at[pl.ds(0, 3 * own), my_cols], p_sems)
    allp[my_rows, my_cols] = par[:, my_cols]

    loads[1].wait()
    out_r = lax.broadcasted_iota(jnp.int32, (imgs * GROUP, GROUP * all_img), 0)
    in_c = lax.broadcasted_iota(jnp.int32, (imgs * GROUP, GROUP * all_img), 1)
    base = in_c - (out_r % GROUP) * all_img - (out_r // GROUP) % half
    first = out_r < half * GROUP

    def relayout(q, dest, out):
        own_at = dest * imgs + q * half
        mate_at = flip(dest, AXES[q][0], n) * imgs + q * half
        pick = jnp.where(base == jnp.where(first, own_at, mate_at), 1.0, 0.0).astype(BF)

        def one(g, carry):
            s0 = pl.multiple_of(g * GROUP, GROUP)
            block = so[pl.ds(s0, GROUP)].reshape(GROUP * all_img, width)
            moved = jnp.dot(pick, block, preferred_element_type=F32).astype(BF)
            out[:, pl.ds(s0, GROUP), :] = moved.reshape(imgs, GROUP, width)
            return carry

        lax.fori_loop(0, own // GROUP, one, 0)

    for i in range(3):
        for q in range(2):
            k = AXES[q][1][i]
            relayout(q, flip(me, k, n), stage.at[q, i])
            send(stage.at[q, i], rows.at[q, side_spot(q, me)], a_sems, k)
    a_moved = group(stage, a_sems)
    for q in range(2):
        relayout(q, me, rows.at[q, side_spot(q, me)])

    arrive(p_moved)
    meet_planes()
    for i in range(n // 2):
        block = allp.at[pl.ds(pl.multiple_of(flip(me, 2 * i, n) * own, GROUP), own), my_cols]
        to_dp(lambda k: block, lambda k: block, q_sems.at[i])
    q_moved = [group(precv.at[pl.ds(1, m - 1), 0], q_sems.at[i]) for i in range(n // 2)]
    loads[2].wait()
    for moved in q_moved:
        arrive(moved)
    for i in range(n // 2):
        block = allp.at[pl.ds(pl.multiple_of(flip(me, 2 * i, n) * own, GROUP), own)]
        send(block, block, f_sems, 1)
    f_moved = group(allp.at[pl.ds(0, n // 2 * own)], f_sems)
    arrive(f_moved)

    for q in range(2):

        def forward(t, carry):
            b = q * half + t
            logits = rows_last(allp[...], tok[b])
            peak = jnp.max(logits, axis=0, keepdims=True)
            raised = jnp.exp(logits - peak)
            comb[b] = raised / jnp.sum(raised, axis=0, keepdims=True)
            for p in range(2):
                low[q, t, p * quarter : (p + 1) * quarter] = comb[b, piece(q, False, p)].astype(BF)
                low_send[q, t, p * quarter : (p + 1) * quarter] = comb[b, piece(q, True, p)].astype(BF)
            return carry

        lax.fori_loop(0, half, forward, 0)
        send(low_send.at[q], low.at[q, pl.ds(half, half)], w_sems, AXES[q][0])
    w_moved = group(low_send, w_sems)

    def slot_grads(q, i, grads_in):
        out = jnp.dot(low[q, i], grads_in, preferred_element_type=F32).astype(BF)
        gs[q, :, i] = out.reshape(4, own, width)

    def comb_grads(q, i, grads_in):
        return rows_last(rows[q, :, i].reshape(4 * own, width), grads_in)

    for q in range(2):

        def own_slots(t, carry):
            slot_grads(q, t, go[q * half + t])
            return carry

        lax.fori_loop(0, half, own_slots, 0)

    arrive(o_moved)
    arrive(a_moved)
    for q in range(2):

        def mate_comb(t, carry):
            gc_send[q, t] = comb_grads(q, half + t, mate[q, t]).astype(BF)
            return carry

        lax.fori_loop(0, half, mate_comb, 0)
        send(gc_send.at[q], gc_recv.at[q], c_sems, AXES[q][0])
    c_moved = group(gc_send, c_sems)

    chunks = own // GROUP

    def landing(holder, images, j):
        if j == chunks - 1:
            return last.at[holder, images]
        return grec.at[holder, images, pl.ds(j * GROUP, GROUP)]

    def return_grads(h, parts):
        part = pl.ds(h * half, half)
        for j in parts:
            for i in range(3):
                for q in range(2):
                    k = AXES[q][1][i]
                    holder = flip(me, AXES[q][0], n) if h else me
                    send(
                        gs.at[q, side_spot(q, flip(me, k, n)), part, pl.ds(j * GROUP, GROUP)],
                        landing(holder, pl.ds(q * half, half), j), g_sems.at[j], k,
                    )
            for q in range(2):
                holder = flip(me, AXES[q][0], n) if h else me
                pltpu.make_async_copy(
                    gs.at[q, side_spot(q, me), part, pl.ds(j * GROUP, GROUP)],
                    landing(holder, pl.ds(q * half, half), j), keep_sem.at[j],
                ).start()

    def all_grads(j, holders):
        return last.at[:holders] if j == chunks - 1 else grec.at[:holders, :, pl.ds(j * GROUP, GROUP)]

    g_moved = [group(all_grads(j, n - 2), g_sems.at[j]) for j in range(chunks)]

    return_grads(0, range(chunks))
    arrive(w_moved)
    for q in range(2):

        def mate_slots(t, carry):
            slot_grads(q, half + t, mate[q, t])
            return carry

        lax.fori_loop(0, half, mate_slots, 0)
    return_grads(1, range(chunks - 1))

    for q in range(2):

        def own_comb(t, carry):
            grads = comb_grads(q, t, go[q * half + t])
            for p in range(2):
                gcf[q * half + t, piece(q, False, p)] = grads[p * quarter : (p + 1) * quarter]
            return carry

        lax.fori_loop(0, half, own_comb, 0)
    acc[...] = jnp.zeros_like(acc)
    arrive(c_moved)
    for q in range(2):

        def backward(t, carry):
            b = q * half + t
            for p in range(2):
                gcf[b, piece(q, True, p)] = gc_recv[q, t, p * quarter : (p + 1) * quarter].astype(F32)
            grad_comb = gcf[b]
            weights = comb[b]
            rowdot = jnp.sum(weights * grad_comb, axis=0, keepdims=True)
            wide = weights * (grad_comb - rowdot)
            gcf[b] = wide
            acc[...] += jnp.dot(wide.astype(BF), tok[b], preferred_element_type=F32)
            return carry

        lax.fori_loop(0, half, backward, 0)

    core = me % 2
    for i in range(n // 2):
        ksend[i] = acc[pl.ds(pl.multiple_of((2 * i + 1 - core) * own, GROUP), own)].astype(BF)
    send(ksend, krecv, k_sems, 1)
    k_moved = group(ksend, k_sems)
    arrive(k_moved)
    for i in range(n // 2):
        red[i] = acc[pl.ds(pl.multiple_of((2 * i + core) * own, GROUP), own)] + krecv[i].astype(F32)
    for k in range(1, m):
        there = flip(mz, k, m)
        psend[k] = red[:, :, pl.ds(pl.multiple_of(there * cols, 128), cols)].astype(BF)
    to_dp(lambda k: psend.at[k], lambda k: precv.at[k], z_sems)
    z_moved = group(psend.at[pl.ds(1, m - 1)], z_sems)

    def token_grads(b, carry):
        gt[b] = jnp.dot(gcf[b].T.astype(BF), allp[...], preferred_element_type=F32).astype(BF)
        return carry

    lax.fori_loop(0, imgs, token_grads, 0)
    arrive(z_moved)
    total = red[:, :, my_cols]
    for k in range(1, m):
        total = total + precv[k].astype(F32)
    red[:, :, my_cols] = total
    for k in range(2, n, 2):
        xsend[k // 2] = red[flip(me, k, n) // 2, :, my_cols].astype(BF)
    for k in range(2, n, 2):
        send(xsend.at[k // 2], xrecv.at[k // 2], x_sems, k)
    x_moved = group(xsend.at[pl.ds(1, n // 2 - 1)], x_sems)
    return_grads(1, (chunks - 1,))
    for j in range(chunks):
        every = all_grads(j, 2)
        pltpu.make_async_copy(every, every, keep_sem.at[j]).wait()
    for j in range(chunks - 1):
        arrive(g_moved[j])

        def swap(c, carry):
            lanes = pl.ds(pl.multiple_of(c * LANES, LANES), LANES)
            block = grec[:, :, j * GROUP : (j + 1) * GROUP, lanes].reshape(n * imgs, GROUP, LANES)
            done[j * GROUP : (j + 1) * GROUP, :, lanes] = jnp.swapaxes(block, 0, 1)
            return carry

        lax.fori_loop(0, width // LANES, swap, 0)
    arrive(x_moved)
    owned = red[me // 2, :, my_cols]
    for k in range(2, n, 2):
        owned = owned + xrecv[k // 2].astype(F32)
    gp[...] = owned
    for moved in groups:
        moved.wait_send()
    arrive(g_moved[chunks - 1])


def paired_exchange(n, m, tok, go, so, par):
    imgs, patches, width = tok.shape
    own, all_img, _ = so.shape
    slots, cols, half = own * n, width // m, imgs // 2
    dma = pltpu.SemaphoreType.DMA
    return pl.pallas_call(
        functools.partial(paired_kernel, n, m),
        out_shape=(
            pltpu.VMEM((own - GROUP, all_img, width), BF),
            pltpu.VMEM((n, imgs, GROUP, width), BF),
            pltpu.VMEM((imgs, patches, width), BF),
            pltpu.VMEM((own, cols), F32),
        ),
        in_specs=[pl.BlockSpec(memory_space=pl.ANY)] * 4,
        out_specs=(pl.BlockSpec(memory_space=pltpu.VMEM),) * 4,
        scratch_shapes=[
            pltpu.VMEM((imgs, patches, width), BF),
            pltpu.VMEM((imgs, patches, width), BF),
            pltpu.VMEM((2, half, patches, width), BF),
            pltpu.VMEM((own, all_img, width), BF),
            pltpu.VMEM((own, width), BF),
            pltpu.VMEM((slots, width), BF),
            pltpu.VMEM((2, 3, imgs, own, width), BF),
            pltpu.VMEM((2, 4, imgs, own, width), BF),
            pltpu.VMEM((2, 4, imgs, own, width), BF),
            pltpu.VMEM((imgs, slots, patches), F32),
            pltpu.VMEM((imgs, slots, patches), F32),
            pltpu.VMEM((2, imgs, slots // 2, patches), BF),
            pltpu.VMEM((2, half, slots // 2, patches), BF),
            pltpu.VMEM((2, half, slots // 2, patches), BF),
            pltpu.VMEM((2, half, slots // 2, patches), BF),
            pltpu.VMEM((n, imgs, own - GROUP, width), BF),
            pltpu.VMEM((slots, width), F32),
            pltpu.VMEM((n // 2, own, width), BF),
            pltpu.VMEM((n // 2, own, width), BF),
            pltpu.VMEM((n // 2, own, width), F32),
            pltpu.VMEM((m, n // 2, own, cols), BF),
            pltpu.VMEM((m, n // 2, own, cols), BF),
            pltpu.VMEM((n // 2, own, cols), BF),
            pltpu.VMEM((n // 2, own, cols), BF),
            pltpu.SemaphoreType.REGULAR, pltpu.SemaphoreType.REGULAR, dma((4,)), dma((own // GROUP,)),
            dma((2,)), dma((n // 2, 2)), dma((2,)), dma((2,)), dma((2,)), dma((2,)), dma((2,)),
            dma((2,)), dma((own // GROUP, 2)), dma((2,)), dma((2,)),
        ],
        compiler_params=pltpu.CompilerParams(
            collective_id=0, has_side_effects=True, vmem_limit_bytes=56 * 1000 * 1000
        ),
    )(tok, go, so, par)


def settle_kernel(arrived, gp_in, out, gp_out):
    out[...] = jnp.swapaxes(arrived[...], 0, 1)
    gp_out[...] = gp_in[...]


def settle(arrived, grad_par):
    all_img, own, width = arrived.shape
    small = pl.BlockSpec((GROUP, grad_par.shape[1]), lambda i: (i, 0))
    return pl.pallas_call(
        settle_kernel,
        grid=(own // GROUP,),
        out_shape=(
            jax.ShapeDtypeStruct((own, all_img, width), BF),
            jax.ShapeDtypeStruct(grad_par.shape, F32),
        ),
        in_specs=[pl.BlockSpec((all_img, GROUP, width), lambda i: (0, i, 0)), small],
        out_specs=(pl.BlockSpec((GROUP, all_img, width), lambda i: (i, 0, 0)), small),
    )(arrived, grad_par)


def finish_kernel(done, last, gt, gp, slot_out, tok_out, par_out, turned, sem):
    own = done.shape[0]
    group, all_img, width = turned.shape
    copies = []

    def put(src, dst, at):
        copies.append(pltpu.make_async_copy(src, dst, sem.at[at]))
        copies[-1].start()

    for g in range(own // group):
        rows = pl.ds(g * group, group)
        put(done.at[rows], slot_out.at[rows], 0)
    for b in range(gt.shape[0]):
        put(gt.at[b], tok_out.at[b], 1)
    put(gp, par_out, 2)
    tiles = width // LANES
    for part in range(2):

        def swap(c, carry):
            lanes = pl.ds(pl.multiple_of((part * (tiles // 2) + c) * LANES, LANES), LANES)
            turned[:, :, lanes] = jnp.swapaxes(last[:, :, :, lanes].reshape(all_img, group, LANES), 0, 1)
            return carry

        lax.fori_loop(0, tiles // 2, swap, 0)
        lanes = pl.ds(part * (width // 2), width // 2)
        put(turned.at[:, :, lanes], slot_out.at[pl.ds(own, group), :, lanes], 3)
    for copy in copies:
        copy.wait()


def finish(done, last, gt, gp):
    own, all_img, width = done.shape
    return pl.pallas_call(
        finish_kernel,
        out_shape=(
            jax.ShapeDtypeStruct((own + GROUP, all_img, width), BF),
            jax.ShapeDtypeStruct(gt.shape, BF),
            jax.ShapeDtypeStruct(gp.shape, F32),
        ),
        in_specs=[pl.BlockSpec(memory_space=pltpu.VMEM)] * 4,
        out_specs=(pl.BlockSpec(memory_space=pl.ANY),) * 3,
        scratch_shapes=[pltpu.VMEM((GROUP, all_img, width), BF), pltpu.SemaphoreType.DMA((4,))],
        compiler_params=pltpu.CompilerParams(vmem_limit_bytes=16 * 1000 * 1000),
    )(done, last, gt, gp)


def per_device(n, m, tokens, grad_out, slot_out, slot_params):
    tok = jnp.transpose(tokens, (1, 0, 2))
    go = jnp.transpose(grad_out, (1, 0, 2))
    if n == 8 and tok.shape[0] % 2 == 0:
        grad_slot, grad_tok, grad_par = finish(*paired_exchange(n, m, tok, go, slot_out, slot_params))
    else:
        arrived, grad_tok, grad_par = exchange(n, m, tok, go, slot_out, slot_params)
        own, all_img, width = slot_out.shape
        grad_slot, grad_par = settle(arrived.reshape(all_img, own, width), grad_par)
    return jnp.transpose(grad_tok, (1, 0, 2)), grad_slot, grad_par


def solution(mesh):
    return jax.shard_map(
        functools.partial(per_device, mesh.shape["expert"], mesh.shape["dp"]),
        mesh=mesh,
        in_specs=(
            P(None, ("dp", "expert"), None),
            P(None, ("dp", "expert"), None),
            P("expert", "dp", None),
            P("expert", None),
        ),
        out_specs=(P(None, ("dp", "expert"), None), P("expert", "dp", None), P("expert", "dp")),
        check_vma=False,
    )
```

```python
import functools

import jax
import jax.numpy as jnp
from jax import lax
from jax.experimental import pallas as pl
from jax.experimental.pallas import tpu as pltpu
from jax.sharding import PartitionSpec as P

BF = jnp.bfloat16
F32 = jnp.float32
GROUP = 16
LANES = 128


def flip(index, mask, size):
    total, bit = 0, 1
    while bit < size:
        total = total + ((index // bit + mask // bit) % 2) * bit
        bit *= 2
    return total


def send_order(n, core):
    if n != 8:
        return list(range(n - 1, 0, -1))
    masks = []
    for low in range(2):
        masks += [6 + low - 4 * core, 2 + low + 2 * core, 4 + low + 2 * core]
    return masks + [1]


def rows_last(lhs, rhs):
    return lax.dot_general(lhs, rhs, (((1,), (1,)), ((), ())), preferred_element_type=F32)


def exchange_kernel(
    n, m, tok_hbm, go_hbm, so_hbm, par_hbm,
    grec, gt_out, gp_out,
    tok, go, so, par, allp, stage, rows, gs, comb, gt, acc, psend, precv, xsend, xrecv, gp,
    local_sem, p_send, p_recv, q_send, q_recv, a_send, a_recv, g_send, g_recv,
    z_send, z_recv, x_send, x_recv,
):
    me = lax.axis_index("expert")
    mz = lax.axis_index("dp")
    core = me % 2
    imgs = tok.shape[0]
    own = par.shape[0]
    all_img = so.shape[1]
    cols = allp.shape[1] // m
    width = allp.shape[1]
    slots = allp.shape[0]
    my_cols = pl.ds(pl.multiple_of(mz * cols, 128), cols)
    my_rows = pl.ds(pl.multiple_of(me * own, GROUP), own)

    loads = [
        pltpu.make_async_copy(src, dst, local_sem.at[i])
        for i, (src, dst) in enumerate([(par_hbm, par), (so_hbm, so), (tok_hbm, tok), (go_hbm, go)])
    ]
    for load in loads:
        load.start()

    barrier = pltpu.get_barrier_semaphore()
    for k in range(1, n):
        pl.semaphore_signal(barrier, inc=1, device_id=(mz, flip(me, k, n)), device_id_type=pl.DeviceIdType.MESH)
    for k in range(1, m):
        pl.semaphore_signal(barrier, inc=1, device_id=(flip(mz, k, m), me), device_id_type=pl.DeviceIdType.MESH)
    pl.semaphore_wait(barrier, n + m - 2)

    def to_expert(src, dst, send, recv, k):
        return pltpu.make_async_remote_copy(
            src_ref=src, dst_ref=dst, send_sem=send.at[k], recv_sem=recv.at[k],
            device_id=(mz, flip(me, k, n)), device_id_type=pl.DeviceIdType.MESH,
        )

    def to_dp(src, dst, send, recv, k):
        return pltpu.make_async_remote_copy(
            src_ref=src, dst_ref=dst, send_sem=send.at[k], recv_sem=recv.at[k],
            device_id=(flip(mz, k, m), me), device_id_type=pl.DeviceIdType.MESH,
        )

    loads[0].wait()
    p_copies = [to_expert(par.at[:, my_cols], allp.at[my_rows, my_cols], p_send, p_recv, k) for k in range(1, n)]
    for copy in p_copies:
        copy.start()
    allp[my_rows, my_cols] = par[:, my_cols]

    loads[1].wait()
    out_r = lax.broadcasted_iota(jnp.int32, (imgs * GROUP, GROUP * all_img), 0)
    in_c = lax.broadcasted_iota(jnp.int32, (imgs * GROUP, GROUP * all_img), 1)
    base = in_c - (out_r % GROUP) * all_img - out_r // GROUP

    def relayout(dest, out):
        pick = jnp.where(base == dest * imgs, 1.0, 0.0).astype(BF)

        def one(g, carry):
            s0 = pl.multiple_of(g * GROUP, GROUP)
            block = so[pl.ds(s0, GROUP)].reshape(GROUP * all_img, width)
            moved = jnp.dot(pick, block, preferred_element_type=F32).astype(BF)
            out[:, pl.ds(s0, GROUP), :] = moved.reshape(imgs, GROUP, width)
            return carry

        lax.fori_loop(0, own // GROUP, one, 0)

    order = send_order(n, core)
    a_copies = []
    for k in order:
        relayout(flip(me, k, n), stage.at[k])
        copy = to_expert(stage.at[k], rows.at[me], a_send, a_recv, k)
        copy.start()
        a_copies.append(copy)
    relayout(me, rows.at[me])

    for copy in p_copies:
        copy.wait_recv()
    q_copies = [to_dp(allp.at[:, my_cols], allp.at[:, my_cols], q_send, q_recv, k) for k in range(1, m)]
    for copy in q_copies:
        copy.start()
    loads[2].wait()
    loads[3].wait()
    for copy in q_copies:
        copy.wait_recv()

    def forward(b, carry):
        logits = rows_last(allp[...], tok[b])
        peak = jnp.max(logits, axis=0, keepdims=True)
        raised = jnp.exp(logits - peak)
        weights = raised / jnp.sum(raised, axis=0, keepdims=True)
        comb[b] = weights
        grads = jnp.dot(weights.astype(BF), go[b], preferred_element_type=F32).astype(BF)
        gs[:, b] = grads.reshape(n, own, width)
        return carry

    lax.fori_loop(0, imgs, forward, 0)

    keep = pltpu.make_async_copy(gs.at[me], grec.at[me], local_sem.at[4])
    keep.start()
    g_copies = []
    for k in order:
        copy = to_expert(gs.at[flip(me, k, n)], grec.at[me], g_send, g_recv, k)
        copy.start()
        g_copies.append(copy)

    for copy in a_copies:
        copy.wait_recv()
    acc[...] = jnp.zeros_like(acc)

    def backward(b, carry):
        grad_comb = rows_last(rows[:, b].reshape(slots, width), go[b])
        weights = comb[b]
        rowdot = jnp.sum(weights * grad_comb, axis=0, keepdims=True)
        wide = weights * (grad_comb - rowdot)
        acc[...] += jnp.dot(wide.astype(BF), tok[b], preferred_element_type=F32)
        gt[b] = jnp.dot(wide.T.astype(BF), allp[...], preferred_element_type=F32).astype(BF)
        return carry

    lax.fori_loop(0, imgs, backward, 0)

    for k in range(1, m):
        there = flip(mz, k, m)
        psend[k] = acc[:, pl.ds(pl.multiple_of(there * cols, 128), cols)].astype(BF)
    z_copies = [to_dp(psend.at[k], precv.at[k], z_send, z_recv, k) for k in range(1, m)]
    for copy in z_copies:
        copy.start()
    put = pltpu.make_async_copy(gt, gt_out, local_sem.at[5])
    put.start()
    for copy in z_copies:
        copy.wait_recv()
    total = acc[:, my_cols]
    for k in range(1, m):
        total = total + precv[k].astype(F32)
    acc[:, my_cols] = total
    for k in range(1, n):
        there = flip(me, k, n)
        xsend[k] = acc[pl.ds(pl.multiple_of(there * own, GROUP), own), my_cols].astype(BF)
    x_copies = [to_expert(xsend.at[k], xrecv.at[k], x_send, x_recv, k) for k in range(1, n)]
    for copy in x_copies:
        copy.start()
    for copy in x_copies:
        copy.wait_recv()
    owned = acc[my_rows, my_cols]
    for k in range(1, n):
        owned = owned + xrecv[k].astype(F32)
    gp[...] = owned
    give = pltpu.make_async_copy(gp, gp_out, local_sem.at[6])
    give.start()

    for copy in g_copies:
        copy.wait_recv()
    for copy in p_copies + a_copies + q_copies + g_copies + z_copies + x_copies:
        copy.wait_send()
    keep.wait()
    put.wait()
    give.wait()


def exchange(n, m, tok, go, so, par):
    imgs, patches, width = tok.shape
    own, all_img, _ = so.shape
    slots, cols = own * n, width // m
    dma = pltpu.SemaphoreType.DMA
    return pl.pallas_call(
        functools.partial(exchange_kernel, n, m),
        out_shape=(
            jax.ShapeDtypeStruct((n, imgs, own, width), BF),
            jax.ShapeDtypeStruct((imgs, patches, width), BF),
            jax.ShapeDtypeStruct((own, cols), F32),
        ),
        in_specs=[pl.BlockSpec(memory_space=pl.ANY)] * 4,
        out_specs=(pl.BlockSpec(memory_space=pl.ANY),) * 3,
        scratch_shapes=[
            pltpu.VMEM((imgs, patches, width), BF),
            pltpu.VMEM((imgs, patches, width), BF),
            pltpu.VMEM((own, all_img, width), BF),
            pltpu.VMEM((own, width), BF),
            pltpu.VMEM((slots, width), BF),
            pltpu.VMEM((n, imgs, own, width), BF),
            pltpu.VMEM((n, imgs, own, width), BF),
            pltpu.VMEM((n, imgs, own, width), BF),
            pltpu.VMEM((imgs, slots, patches), F32),
            pltpu.VMEM((imgs, patches, width), BF),
            pltpu.VMEM((slots, width), F32),
            pltpu.VMEM((m, slots, cols), BF),
            pltpu.VMEM((m, slots, cols), BF),
            pltpu.VMEM((n, own, cols), BF),
            pltpu.VMEM((n, own, cols), BF),
            pltpu.VMEM((own, cols), F32),
            dma((7,)),
            dma((n,)), dma((n,)), dma((m,)), dma((m,)),
            dma((n,)), dma((n,)), dma((n,)), dma((n,)),
            dma((m,)), dma((m,)), dma((n,)), dma((n,)),
        ],
        compiler_params=pltpu.CompilerParams(
            collective_id=0, has_side_effects=True, vmem_limit_bytes=66 * 1000 * 1000
        ),
    )(tok, go, so, par)


AXES = ((2, (4, 5, 1)), (4, (2, 3, 1)))


def side_spot(which, index):
    high = index // 4 if which == 0 else (index // 2) % 2
    return high * 2 + index % 2


def paired_kernel(
    n, m, tok_hbm, go_hbm, so_hbm, par_hbm,
    done, last, gt, gp,
    tok, go, mate, so, par, allp, stage, rows, gs, comb, gcf, low, low_send, gc_send, gc_recv,
    grec, acc, ksend, krecv, red, psend, precv, xsend, xrecv,
    ready, corner, planes, local_sem, keep_sem, p_sems, r_sems, q_sems, f_sems, k_sems, o_sems, a_sems, w_sems,
    c_sems, g_sems, z_sems, x_sems, y_sems,
):
    me = lax.axis_index("expert")
    mz = lax.axis_index("dp")
    imgs = tok.shape[0]
    half = imgs // 2
    own = par.shape[0]
    all_img = so.shape[1]
    slots, width = allp.shape
    patches = tok.shape[1]
    cols = width // m
    quarter = slots // 4
    my_cols = pl.ds(pl.multiple_of(mz * cols, 128), cols)
    my_rows = pl.ds(pl.multiple_of(me * own, GROUP), own)
    sides = ((me // 2) % 2, me // 4)

    def piece(which, other, p):
        side = 1 - sides[which] if other else sides[which]
        start = p * 2 * quarter + side * quarter if which == 0 else side * 2 * quarter + p * quarter
        return pl.ds(pl.multiple_of(start, quarter), quarter)

    def load(src, dst, at):
        copy = pltpu.make_async_copy(src, dst, local_sem.at[at])
        copy.start()
        return copy

    par_load = load(par_hbm, par, 0)
    go_loads = [load(go_hbm.at[q * half], go.at[q * half], 1 + q) for q in range(2)]

    gate = n - 1
    barrier = pltpu.get_barrier_semaphore()

    def tell(sem, plane, index):
        pl.semaphore_signal(sem, inc=1, device_id=(plane, index), device_id_type=pl.DeviceIdType.MESH)

    partner = flip(me, 1, n)
    along_y = flip(me, 4, n) // 2 * 2 + 1
    tell(barrier, mz, flip(me, 2, n) // 2 * 2)
    tell(barrier, mz, jnp.where(along_y == gate, gate - 1, along_y))

    @pl.when(partner != gate)
    def greet():
        tell(barrier, mz, partner)

    @pl.when(me < gate - 1)
    def meet():
        pl.semaphore_wait(barrier, 3)

    @pl.when(me == gate - 1)
    def meet_all():
        pl.semaphore_wait(barrier, 5)

    @pl.when(me != gate)
    def pass_on():
        tell(ready, mz, partner)

    @pl.when(me == gate)
    def enter():
        pl.semaphore_wait(ready, 1)

    def meet_side():
        @pl.when(me < gate - 1)
        def side():
            pl.semaphore_wait(ready, 1)

        tell(corner, mz, flip(me, 2, n))

    def meet_planes():
        pl.semaphore_wait(corner, 1)

        @pl.when(me == gate)
        def spread():
            for k in range(1, m):
                tell(barrier, flip(mz, k, m), gate)
            pl.semaphore_wait(barrier, m - 1)
            for k in range(1, n):
                tell(planes, mz, flip(me, k, n))

        @pl.when(me != gate)
        def follow():
            pl.semaphore_wait(planes, 1)

    def to_expert(src, dst, send, recv, k):
        return pltpu.make_async_remote_copy(
            src_ref=src, dst_ref=dst, send_sem=send, recv_sem=recv,
            device_id=(mz, flip(me, k, n)), device_id_type=pl.DeviceIdType.MESH,
        )

    def to_dp(src, dst, sems):
        for k in range(1, m):
            pltpu.make_async_remote_copy(
                src_ref=src(k), dst_ref=dst(k), send_sem=sems.at[0], recv_sem=sems.at[1],
                device_id=(flip(mz, k, m), me), device_id_type=pl.DeviceIdType.MESH,
            ).start()

    def send(src, dst, sems, k):
        to_expert(src, dst, sems.at[0], sems.at[1], k).start()

    groups = []

    def group(every, sems):
        groups.append(to_expert(every, every, sems.at[0], sems.at[1], 1))
        return groups[-1]

    def arrive(moved):
        moved.wait_recv()

    def rows_of(mask, start, size):
        return pl.ds(pl.multiple_of(flip(me, mask, n) * own + start, GROUP), size)

    def send_params(q):
        send(par.at[:, my_cols], allp.at[my_rows, my_cols], p_sems, 2 + 2 * q)

    def send_first(q):
        send(go.at[q * half], mate.at[q, 0], o_sems, 2 + 2 * q)

    par_load.wait()
    send_params(me % 2)
    for copy in go_loads:
        copy.wait()
    send_first(me % 2)
    meet_side()
    send_params(1 - me % 2)
    send_first(1 - me % 2)
    rest = [pl.ds(q * half + 1, half - 1) for q in range(2)]
    rest_loads = [load(go_hbm.at[part], go.at[part], 3 + q) for q, part in enumerate(rest)]
    so_load = load(so_hbm, so, 5)
    tok_load = load(tok_hbm, tok, 6)
    allp[my_rows, my_cols] = par[:, my_cols]
    arrive(group(allp.at[pl.ds(0, 2 * own), my_cols], p_sems))
    for q in range(2):
        block = allp.at[rows_of(4 - 2 * q, (1 - q) * (own // 2), own // 2), my_cols]
        send(block, block, r_sems, AXES[q][0])
        rest_loads[q].wait()
        send(go.at[rest[q]], mate.at[q, pl.ds(1, half - 1)], o_sems, AXES[q][0])
    r_moved = group(allp.at[pl.ds(0, own), my_cols], r_sems)
    o_moved = group(mate, o_sems)

    so_load.wait()
    out_r = lax.broadcasted_iota(jnp.int32, (imgs * GROUP, GROUP * all_img), 0)
    in_c = lax.broadcasted_iota(jnp.int32, (imgs * GROUP, GROUP * all_img), 1)
    base = in_c - (out_r % GROUP) * all_img - (out_r // GROUP) % half
    first = out_r < half * GROUP

    def relayout(q, dest, out):
        own_at = dest * imgs + q * half
        mate_at = flip(dest, AXES[q][0], n) * imgs + q * half
        pick = jnp.where(base == jnp.where(first, own_at, mate_at), 1.0, 0.0).astype(BF)

        def one(g, carry):
            s0 = pl.multiple_of(g * GROUP, GROUP)
            block = so[pl.ds(s0, GROUP)].reshape(GROUP * all_img, width)
            moved = jnp.dot(pick, block, preferred_element_type=F32).astype(BF)
            out[:, pl.ds(s0, GROUP), :] = moved.reshape(imgs, GROUP, width)
            return carry

        lax.fori_loop(0, own // GROUP, one, 0)

    for i in range(3):
        for q in range(2):
            k = AXES[q][1][i]
            relayout(q, flip(me, k, n), stage.at[q, i])
            send(stage.at[q, i], rows.at[q, side_spot(q, me)], a_sems, k)
    a_moved = group(stage, a_sems)
    for q in range(2):
        relayout(q, me, rows.at[q, side_spot(q, me)])

    arrive(r_moved)
    meet_planes()
    for i in range(n // 2):
        block = allp.at[rows_of(2 * i, 0, own), my_cols]
        to_dp(lambda k: block, lambda k: block, q_sems.at[i])
    q_moved = [group(precv.at[pl.ds(1, m - 1), 0], q_sems.at[i]) for i in range(n // 2)]
    tok_load.wait()
    for moved in q_moved:
        arrive(moved)
    for i in range(n // 2):
        block = allp.at[rows_of(2 * i, 0, own)]
        send(block, block, f_sems, 1)
    f_moved = group(allp.at[pl.ds(0, n // 2 * own)], f_sems)
    arrive(f_moved)

    for q in range(2):

        def forward(t, carry):
            b = q * half + t
            logits = rows_last(allp[...], tok[b])
            peak = jnp.max(logits, axis=0, keepdims=True)
            raised = jnp.exp(logits - peak)
            comb[b] = raised / jnp.sum(raised, axis=0, keepdims=True)
            for p in range(2):
                low[q, t, p * quarter : (p + 1) * quarter] = comb[b, piece(q, False, p)].astype(BF)
                low_send[q, t, p * quarter : (p + 1) * quarter] = comb[b, piece(q, True, p)].astype(BF)
            return carry

        lax.fori_loop(0, half, forward, 0)
        send(low_send.at[q], low.at[q, pl.ds(half, half)], w_sems, AXES[q][0])
    w_moved = group(low_send, w_sems)

    def slot_grads(q, i, grads_in):
        out = jnp.dot(low[q, i], grads_in, preferred_element_type=F32).astype(BF)
        gs[q, :, i] = out.reshape(4, own, width)

    def comb_grads(q, i, grads_in):
        return rows_last(rows[q, :, i].reshape(4 * own, width), grads_in)

    for q in range(2):

        def own_slots(t, carry):
            slot_grads(q, t, go[q * half + t])
            return carry

        lax.fori_loop(0, half, own_slots, 0)

    arrive(o_moved)
    arrive(a_moved)
    for q in range(2):

        def mate_comb(t, carry):
            gc_send[q, t] = comb_grads(q, half + t, mate[q, t]).astype(BF)
            return carry

        lax.fori_loop(0, half, mate_comb, 0)
        send(gc_send.at[q], gc_recv.at[q], c_sems, AXES[q][0])
    c_moved = group(gc_send, c_sems)

    chunks = own // GROUP

    def landing(holder, images, j):
        if j == chunks - 1:
            return last.at[holder, images]
        return grec.at[holder, images, pl.ds(j * GROUP, GROUP)]

    def return_grads(h, parts, steps=(0, 1, 2)):
        part = pl.ds(h * half, half)
        for j in parts:
            for i in steps:
                for q in range(2):
                    k = AXES[q][1][i]
                    holder = flip(me, AXES[q][0], n) if h else me
                    send(
                        gs.at[q, side_spot(q, flip(me, k, n)), part, pl.ds(j * GROUP, GROUP)],
                        landing(holder, pl.ds(q * half, half), j), g_sems.at[j], k,
                    )
            for q in range(2 if 2 in steps else 0):
                holder = flip(me, AXES[q][0], n) if h else me
                pltpu.make_async_copy(
                    gs.at[q, side_spot(q, me), part, pl.ds(j * GROUP, GROUP)],
                    landing(holder, pl.ds(q * half, half), j), keep_sem.at[j],
                ).start()

    def all_grads(j, holders):
        return last.at[:holders] if j == chunks - 1 else grec.at[:holders, :, pl.ds(j * GROUP, GROUP)]

    g_moved = [group(all_grads(j, n - 2), g_sems.at[j]) for j in range(chunks)]

    return_grads(0, range(chunks))
    arrive(w_moved)
    for q in range(2):

        def mate_slots(t, carry):
            slot_grads(q, half + t, mate[q, t])
            return carry

        lax.fori_loop(0, half, mate_slots, 0)
    return_grads(1, range(chunks - 2))

    for q in range(2):

        def own_comb(t, carry):
            grads = comb_grads(q, t, go[q * half + t])
            for p in range(2):
                gcf[q * half + t, piece(q, False, p)] = grads[p * quarter : (p + 1) * quarter]
            return carry

        lax.fori_loop(0, half, own_comb, 0)
    acc[...] = jnp.zeros_like(acc)
    arrive(c_moved)
    for q in range(2):

        def backward(t, carry):
            b = q * half + t
            for p in range(2):
                gcf[b, piece(q, True, p)] = gc_recv[q, t, p * quarter : (p + 1) * quarter].astype(F32)
            grad_comb = gcf[b]
            weights = comb[b]
            rowdot = jnp.sum(weights * grad_comb, axis=0, keepdims=True)
            wide = weights * (grad_comb - rowdot)
            gcf[b] = wide
            acc[...] += jnp.dot(wide.astype(BF), tok[b], preferred_element_type=F32)
            return carry

        lax.fori_loop(0, half, backward, 0)

    core = me % 2
    for i in range(n // 2):
        ksend[i] = acc[pl.ds(pl.multiple_of((2 * i + 1 - core) * own, GROUP), own)].astype(BF)
    send(ksend, krecv, k_sems, 1)
    k_moved = group(ksend, k_sems)
    arrive(k_moved)
    for i in range(n // 2):
        red[i] = acc[pl.ds(pl.multiple_of((2 * i + core) * own, GROUP), own)] + krecv[i].astype(F32)
    for k in range(1, m):
        there = flip(mz, k, m)
        psend[k] = red[:, :, pl.ds(pl.multiple_of(there * cols, 128), cols)].astype(BF)
    to_dp(lambda k: psend.at[k], lambda k: precv.at[k], z_sems)
    z_moved = group(psend.at[pl.ds(1, m - 1)], z_sems)

    def token_grads(b, carry):
        gt[b] = jnp.dot(gcf[b].T.astype(BF), allp[...], preferred_element_type=F32).astype(BF)
        return carry

    lax.fori_loop(0, imgs, token_grads, 0)
    arrive(z_moved)
    total = red[:, :, my_cols]
    for k in range(1, m):
        total = total + precv[k].astype(F32)
    red[:, :, my_cols] = total

    def share(mask, q):
        return flip(me, mask, n) // 2, slice(q * (own // 2), (q + 1) * (own // 2)), my_cols

    for q in range(2):
        for i, mask in enumerate((AXES[q][0], 6)):
            xsend[q, i] = red[share(mask, q)].astype(BF)
        send(xsend.at[q, pl.ds(0, 2)], xrecv.at[q, pl.ds(0, 2)], x_sems, AXES[q][0])
    x_moved = group(xsend.at[:, pl.ds(0, 2)], x_sems)
    return_grads(1, (chunks - 2,))
    return_grads(1, (chunks - 1,), (0,))

    def settle_grads(j):
        every = all_grads(j, 2)
        pltpu.make_async_copy(every, every, keep_sem.at[j]).wait()
        arrive(g_moved[j])

        def swap(c, carry):
            lanes = pl.ds(pl.multiple_of(c * LANES, LANES), LANES)
            block = grec[:, :, j * GROUP : (j + 1) * GROUP, lanes].reshape(n * imgs, GROUP, LANES)
            done[j * GROUP : (j + 1) * GROUP, :, lanes] = jnp.swapaxes(block, 0, 1)
            return carry

        lax.fori_loop(0, width // LANES, swap, 0)

    for j in range(chunks - 3):
        settle_grads(j)
    arrive(x_moved)
    for q in range(2):
        for i, mask in enumerate((0, 4 - 2 * q)):
            red[share(mask, q)] += xrecv[q, i].astype(F32)
        xsend[q, 2] = red[share(4 - 2 * q, q)].astype(BF)
        send(xsend.at[q, 2], xrecv.at[q, 2], y_sems, 4 - 2 * q)
    y_moved = group(xsend.at[:, 2], y_sems)
    return_grads(1, (chunks - 1,), (1, 2))
    for j in range(chunks - 3, chunks - 1):
        settle_grads(j)
    arrive(y_moved)
    for q in range(2):
        gp[q * (own // 2) : (q + 1) * (own // 2)] = red[share(0, q)] + xrecv[q, 2].astype(F32)
    every = all_grads(chunks - 1, 2)
    pltpu.make_async_copy(every, every, keep_sem.at[chunks - 1]).wait()
    for moved in groups:
        moved.wait_send()
    arrive(g_moved[chunks - 1])


def paired_exchange(n, m, tok, go, so, par):
    imgs, patches, width = tok.shape
    own, all_img, _ = so.shape
    slots, cols, half = own * n, width // m, imgs // 2
    dma = pltpu.SemaphoreType.DMA
    return pl.pallas_call(
        functools.partial(paired_kernel, n, m),
        out_shape=(
            pltpu.VMEM((own - GROUP, all_img, width), BF),
            pltpu.VMEM((n, imgs, GROUP, width), BF),
            pltpu.VMEM((imgs, patches, width), BF),
            pltpu.VMEM((own, cols), F32),
        ),
        in_specs=[pl.BlockSpec(memory_space=pl.ANY)] * 4,
        out_specs=(pl.BlockSpec(memory_space=pltpu.VMEM),) * 4,
        scratch_shapes=[
            pltpu.VMEM((imgs, patches, width), BF),
            pltpu.VMEM((imgs, patches, width), BF),
            pltpu.VMEM((2, half, patches, width), BF),
            pltpu.VMEM((own, all_img, width), BF),
            pltpu.VMEM((own, width), BF),
            pltpu.VMEM((slots, width), BF),
            pltpu.VMEM((2, 3, imgs, own, width), BF),
            pltpu.VMEM((2, 4, imgs, own, width), BF),
            pltpu.VMEM((2, 4, imgs, own, width), BF),
            pltpu.VMEM((imgs, slots, patches), F32),
            pltpu.VMEM((imgs, slots, patches), F32),
            pltpu.VMEM((2, imgs, slots // 2, patches), BF),
            pltpu.VMEM((2, half, slots // 2, patches), BF),
            pltpu.VMEM((2, half, slots // 2, patches), BF),
            pltpu.VMEM((2, half, slots // 2, patches), BF),
            pltpu.VMEM((n, imgs, own - GROUP, width), BF),
            pltpu.VMEM((slots, width), F32),
            pltpu.VMEM((n // 2, own, width), BF),
            pltpu.VMEM((n // 2, own, width), BF),
            pltpu.VMEM((n // 2, own, width), F32),
            pltpu.VMEM((m, n // 2, own, cols), BF),
            pltpu.VMEM((m, n // 2, own, cols), BF),
            pltpu.VMEM((2, 3, own // 2, cols), BF),
            pltpu.VMEM((2, 3, own // 2, cols), BF),
            pltpu.SemaphoreType.REGULAR, pltpu.SemaphoreType.REGULAR, pltpu.SemaphoreType.REGULAR,
            dma((7,)), dma((own // GROUP,)), dma((2,)), dma((2,)), dma((n // 2, 2)), dma((2,)), dma((2,)), dma((2,)), dma((2,)), dma((2,)),
            dma((2,)), dma((own // GROUP, 2)), dma((2,)), dma((2,)), dma((2,)),
        ],
        compiler_params=pltpu.CompilerParams(
            collective_id=0, has_side_effects=True, vmem_limit_bytes=56 * 1000 * 1000
        ),
    )(tok, go, so, par)


def settle_kernel(arrived, gp_in, out, gp_out):
    out[...] = jnp.swapaxes(arrived[...], 0, 1)
    gp_out[...] = gp_in[...]


def settle(arrived, grad_par):
    all_img, own, width = arrived.shape
    small = pl.BlockSpec((GROUP, grad_par.shape[1]), lambda i: (i, 0))
    return pl.pallas_call(
        settle_kernel,
        grid=(own // GROUP,),
        out_shape=(
            jax.ShapeDtypeStruct((own, all_img, width), BF),
            jax.ShapeDtypeStruct(grad_par.shape, F32),
        ),
        in_specs=[pl.BlockSpec((all_img, GROUP, width), lambda i: (0, i, 0)), small],
        out_specs=(pl.BlockSpec((GROUP, all_img, width), lambda i: (i, 0, 0)), small),
    )(arrived, grad_par)


def finish_kernel(done, last, gt, gp, slot_out, tok_out, par_out, turned, sem):
    own = done.shape[0]
    group, all_img, width = turned.shape
    copies = []

    def put(src, dst, at):
        copies.append(pltpu.make_async_copy(src, dst, sem.at[at]))
        copies[-1].start()

    for g in range(own // group):
        rows = pl.ds(g * group, group)
        put(done.at[rows], slot_out.at[rows], 0)
    for b in range(gt.shape[0]):
        put(gt.at[b], tok_out.at[b], 1)
    put(gp, par_out, 2)
    tiles = width // LANES
    for part in range(2):

        def swap(c, carry):
            lanes = pl.ds(pl.multiple_of((part * (tiles // 2) + c) * LANES, LANES), LANES)
            turned[:, :, lanes] = jnp.swapaxes(last[:, :, :, lanes].reshape(all_img, group, LANES), 0, 1)
            return carry

        lax.fori_loop(0, tiles // 2, swap, 0)
        lanes = pl.ds(part * (width // 2), width // 2)
        put(turned.at[:, :, lanes], slot_out.at[pl.ds(own, group), :, lanes], 3)
    for copy in copies:
        copy.wait()


def finish(done, last, gt, gp):
    own, all_img, width = done.shape
    return pl.pallas_call(
        finish_kernel,
        out_shape=(
            jax.ShapeDtypeStruct((own + GROUP, all_img, width), BF),
            jax.ShapeDtypeStruct(gt.shape, BF),
            jax.ShapeDtypeStruct(gp.shape, F32),
        ),
        in_specs=[pl.BlockSpec(memory_space=pltpu.VMEM)] * 4,
        out_specs=(pl.BlockSpec(memory_space=pl.ANY),) * 3,
        scratch_shapes=[pltpu.VMEM((GROUP, all_img, width), BF), pltpu.SemaphoreType.DMA((4,))],
        compiler_params=pltpu.CompilerParams(vmem_limit_bytes=16 * 1000 * 1000),
    )(done, last, gt, gp)


def per_device(n, m, tokens, grad_out, slot_out, slot_params):
    tok = jnp.transpose(tokens, (1, 0, 2))
    go = jnp.transpose(grad_out, (1, 0, 2))
    if n == 8 and tok.shape[0] % 2 == 0 and tok.shape[0] > 2:
        grad_slot, grad_tok, grad_par = finish(*paired_exchange(n, m, tok, go, slot_out, slot_params))
    else:
        arrived, grad_tok, grad_par = exchange(n, m, tok, go, slot_out, slot_params)
        own, all_img, width = slot_out.shape
        grad_slot, grad_par = settle(arrived.reshape(all_img, own, width), grad_par)
    return jnp.transpose(grad_tok, (1, 0, 2)), grad_slot, grad_par


def solution(mesh):
    return jax.shard_map(
        functools.partial(per_device, mesh.shape["expert"], mesh.shape["dp"]),
        mesh=mesh,
        in_specs=(
            P(None, ("dp", "expert"), None),
            P(None, ("dp", "expert"), None),
            P("expert", "dp", None),
            P("expert", None),
        ),
        out_specs=(P(None, ("dp", "expert"), None), P("expert", "dp", None), P("expert", "dp")),
        check_vma=False,
    )
```

```python
import functools

import jax
import jax.numpy as jnp
from jax import lax
from jax.experimental import pallas as pl
from jax.experimental.pallas import tpu as pltpu
from jax.sharding import PartitionSpec as P

BF = jnp.bfloat16
F32 = jnp.float32
GROUP = 16
LANES = 128


def flip(index, mask, size):
    total, bit = 0, 1
    while bit < size:
        total = total + ((index // bit + mask // bit) % 2) * bit
        bit *= 2
    return total


def send_order(n, core):
    if n != 8:
        return list(range(n - 1, 0, -1))
    masks = []
    for low in range(2):
        masks += [6 + low - 4 * core, 2 + low + 2 * core, 4 + low + 2 * core]
    return masks + [1]


def rows_last(lhs, rhs):
    return lax.dot_general(lhs, rhs, (((1,), (1,)), ((), ())), preferred_element_type=F32)


def exchange_kernel(
    n, m, tok_hbm, go_hbm, so_hbm, par_hbm,
    grec, gt_out, gp_out,
    tok, go, so, par, allp, stage, rows, gs, comb, gt, acc, psend, precv, xsend, xrecv, gp,
    local_sem, p_send, p_recv, q_send, q_recv, a_send, a_recv, g_send, g_recv,
    z_send, z_recv, x_send, x_recv,
):
    me = lax.axis_index("expert")
    mz = lax.axis_index("dp")
    core = me % 2
    imgs = tok.shape[0]
    own = par.shape[0]
    all_img = so.shape[1]
    cols = allp.shape[1] // m
    width = allp.shape[1]
    slots = allp.shape[0]
    my_cols = pl.ds(pl.multiple_of(mz * cols, 128), cols)
    my_rows = pl.ds(pl.multiple_of(me * own, GROUP), own)

    loads = [
        pltpu.make_async_copy(src, dst, local_sem.at[i])
        for i, (src, dst) in enumerate([(par_hbm, par), (so_hbm, so), (tok_hbm, tok), (go_hbm, go)])
    ]
    for load in loads:
        load.start()

    barrier = pltpu.get_barrier_semaphore()
    for k in range(1, n):
        pl.semaphore_signal(barrier, inc=1, device_id=(mz, flip(me, k, n)), device_id_type=pl.DeviceIdType.MESH)
    for k in range(1, m):
        pl.semaphore_signal(barrier, inc=1, device_id=(flip(mz, k, m), me), device_id_type=pl.DeviceIdType.MESH)
    pl.semaphore_wait(barrier, n + m - 2)

    def to_expert(src, dst, send, recv, k):
        return pltpu.make_async_remote_copy(
            src_ref=src, dst_ref=dst, send_sem=send.at[k], recv_sem=recv.at[k],
            device_id=(mz, flip(me, k, n)), device_id_type=pl.DeviceIdType.MESH,
        )

    def to_dp(src, dst, send, recv, k):
        return pltpu.make_async_remote_copy(
            src_ref=src, dst_ref=dst, send_sem=send.at[k], recv_sem=recv.at[k],
            device_id=(flip(mz, k, m), me), device_id_type=pl.DeviceIdType.MESH,
        )

    loads[0].wait()
    p_copies = [to_expert(par.at[:, my_cols], allp.at[my_rows, my_cols], p_send, p_recv, k) for k in range(1, n)]
    for copy in p_copies:
        copy.start()
    allp[my_rows, my_cols] = par[:, my_cols]

    loads[1].wait()
    out_r = lax.broadcasted_iota(jnp.int32, (imgs * GROUP, GROUP * all_img), 0)
    in_c = lax.broadcasted_iota(jnp.int32, (imgs * GROUP, GROUP * all_img), 1)
    base = in_c - (out_r % GROUP) * all_img - out_r // GROUP

    def relayout(dest, out):
        pick = jnp.where(base == dest * imgs, 1.0, 0.0).astype(BF)

        def one(g, carry):
            s0 = pl.multiple_of(g * GROUP, GROUP)
            block = so[pl.ds(s0, GROUP)].reshape(GROUP * all_img, width)
            moved = jnp.dot(pick, block, preferred_element_type=F32).astype(BF)
            out[:, pl.ds(s0, GROUP), :] = moved.reshape(imgs, GROUP, width)
            return carry

        lax.fori_loop(0, own // GROUP, one, 0)

    order = send_order(n, core)
    a_copies = []
    for k in order:
        relayout(flip(me, k, n), stage.at[k])
        copy = to_expert(stage.at[k], rows.at[me], a_send, a_recv, k)
        copy.start()
        a_copies.append(copy)
    relayout(me, rows.at[me])

    for copy in p_copies:
        copy.wait_recv()
    q_copies = [to_dp(allp.at[:, my_cols], allp.at[:, my_cols], q_send, q_recv, k) for k in range(1, m)]
    for copy in q_copies:
        copy.start()
    loads[2].wait()
    loads[3].wait()
    for copy in q_copies:
        copy.wait_recv()

    def forward(b, carry):
        logits = rows_last(allp[...], tok[b])
        peak = jnp.max(logits, axis=0, keepdims=True)
        raised = jnp.exp(logits - peak)
        weights = raised / jnp.sum(raised, axis=0, keepdims=True)
        comb[b] = weights
        grads = jnp.dot(weights.astype(BF), go[b], preferred_element_type=F32).astype(BF)
        gs[:, b] = grads.reshape(n, own, width)
        return carry

    lax.fori_loop(0, imgs, forward, 0)

    keep = pltpu.make_async_copy(gs.at[me], grec.at[me], local_sem.at[4])
    keep.start()
    g_copies = []
    for k in order:
        copy = to_expert(gs.at[flip(me, k, n)], grec.at[me], g_send, g_recv, k)
        copy.start()
        g_copies.append(copy)

    for copy in a_copies:
        copy.wait_recv()
    acc[...] = jnp.zeros_like(acc)

    def backward(b, carry):
        grad_comb = rows_last(rows[:, b].reshape(slots, width), go[b])
        weights = comb[b]
        rowdot = jnp.sum(weights * grad_comb, axis=0, keepdims=True)
        wide = weights * (grad_comb - rowdot)
        acc[...] += jnp.dot(wide.astype(BF), tok[b], preferred_element_type=F32)
        gt[b] = jnp.dot(wide.T.astype(BF), allp[...], preferred_element_type=F32).astype(BF)
        return carry

    lax.fori_loop(0, imgs, backward, 0)

    for k in range(1, m):
        there = flip(mz, k, m)
        psend[k] = acc[:, pl.ds(pl.multiple_of(there * cols, 128), cols)].astype(BF)
    z_copies = [to_dp(psend.at[k], precv.at[k], z_send, z_recv, k) for k in range(1, m)]
    for copy in z_copies:
        copy.start()
    put = pltpu.make_async_copy(gt, gt_out, local_sem.at[5])
    put.start()
    for copy in z_copies:
        copy.wait_recv()
    total = acc[:, my_cols]
    for k in range(1, m):
        total = total + precv[k].astype(F32)
    acc[:, my_cols] = total
    for k in range(1, n):
        there = flip(me, k, n)
        xsend[k] = acc[pl.ds(pl.multiple_of(there * own, GROUP), own), my_cols].astype(BF)
    x_copies = [to_expert(xsend.at[k], xrecv.at[k], x_send, x_recv, k) for k in range(1, n)]
    for copy in x_copies:
        copy.start()
    for copy in x_copies:
        copy.wait_recv()
    owned = acc[my_rows, my_cols]
    for k in range(1, n):
        owned = owned + xrecv[k].astype(F32)
    gp[...] = owned
    give = pltpu.make_async_copy(gp, gp_out, local_sem.at[6])
    give.start()

    for copy in g_copies:
        copy.wait_recv()
    for copy in p_copies + a_copies + q_copies + g_copies + z_copies + x_copies:
        copy.wait_send()
    keep.wait()
    put.wait()
    give.wait()


def exchange(n, m, tok, go, so, par):
    imgs, patches, width = tok.shape
    own, all_img, _ = so.shape
    slots, cols = own * n, width // m
    dma = pltpu.SemaphoreType.DMA
    return pl.pallas_call(
        functools.partial(exchange_kernel, n, m),
        out_shape=(
            jax.ShapeDtypeStruct((n, imgs, own, width), BF),
            jax.ShapeDtypeStruct((imgs, patches, width), BF),
            jax.ShapeDtypeStruct((own, cols), F32),
        ),
        in_specs=[pl.BlockSpec(memory_space=pl.ANY)] * 4,
        out_specs=(pl.BlockSpec(memory_space=pl.ANY),) * 3,
        scratch_shapes=[
            pltpu.VMEM((imgs, patches, width), BF),
            pltpu.VMEM((imgs, patches, width), BF),
            pltpu.VMEM((own, all_img, width), BF),
            pltpu.VMEM((own, width), BF),
            pltpu.VMEM((slots, width), BF),
            pltpu.VMEM((n, imgs, own, width), BF),
            pltpu.VMEM((n, imgs, own, width), BF),
            pltpu.VMEM((n, imgs, own, width), BF),
            pltpu.VMEM((imgs, slots, patches), F32),
            pltpu.VMEM((imgs, patches, width), BF),
            pltpu.VMEM((slots, width), F32),
            pltpu.VMEM((m, slots, cols), BF),
            pltpu.VMEM((m, slots, cols), BF),
            pltpu.VMEM((n, own, cols), BF),
            pltpu.VMEM((n, own, cols), BF),
            pltpu.VMEM((own, cols), F32),
            dma((7,)),
            dma((n,)), dma((n,)), dma((m,)), dma((m,)),
            dma((n,)), dma((n,)), dma((n,)), dma((n,)),
            dma((m,)), dma((m,)), dma((n,)), dma((n,)),
        ],
        compiler_params=pltpu.CompilerParams(
            collective_id=0, has_side_effects=True, vmem_limit_bytes=66 * 1000 * 1000
        ),
    )(tok, go, so, par)


AXES = ((2, (4, 5, 1)), (4, (2, 3, 1)))


def side_spot(which, index):
    high = index // 4 if which == 0 else (index // 2) % 2
    return high * 2 + index % 2


def paired_kernel(
    n, m, tok_hbm, go_hbm, so_hbm, par_hbm,
    done, last, gt, gp,
    tok, go, mate, so, allp, stage, rows, gs, comb, gcf, low, low_send, gc_send, gc_recv,
    grec, acc, ksend, krecv, red, psend, precv, xsend, xrecv,
    ready, corner, planes, local_sem, keep_sem, p_sems, r_sems, q_sems, f_sems, k_sems, o_sems, a_sems, w_sems,
    c_sems, g_sems, z_sems, x_sems, y_sems,
):
    me = lax.axis_index("expert")
    mz = lax.axis_index("dp")
    imgs = tok.shape[0]
    half = imgs // 2
    own = par_hbm.shape[0]
    all_img = so.shape[1]
    slots, width = allp.shape
    patches = tok.shape[1]
    cols = width // m
    quarter = slots // 4
    my_cols = pl.ds(pl.multiple_of(mz * cols, 128), cols)
    my_rows = pl.ds(pl.multiple_of(me * own, GROUP), own)
    sides = ((me // 2) % 2, me // 4)

    def piece(which, other, p):
        side = 1 - sides[which] if other else sides[which]
        start = p * 2 * quarter + side * quarter if which == 0 else side * 2 * quarter + p * quarter
        return pl.ds(pl.multiple_of(start, quarter), quarter)

    def load(src, dst, at):
        copy = pltpu.make_async_copy(src, dst, local_sem.at[at])
        copy.start()
        return copy

    par_load = load(par_hbm.at[:, my_cols], allp.at[my_rows, my_cols], 0)

    gate = n - 1
    barrier = pltpu.get_barrier_semaphore()

    def tell(sem, plane, index):
        pl.semaphore_signal(sem, inc=1, device_id=(plane, index), device_id_type=pl.DeviceIdType.MESH)

    partner = flip(me, 1, n)
    along_y = flip(me, 4, n) // 2 * 2 + 1
    tell(barrier, mz, flip(me, 2, n) // 2 * 2)
    tell(barrier, mz, jnp.where(along_y == gate, gate - 1, along_y))

    @pl.when(partner != gate)
    def greet():
        tell(barrier, mz, partner)

    @pl.when(me < gate - 1)
    def meet():
        pl.semaphore_wait(barrier, 3)

    @pl.when(me == gate - 1)
    def meet_all():
        pl.semaphore_wait(barrier, 5)

    @pl.when(me != gate)
    def pass_on():
        tell(ready, mz, partner)

    @pl.when(me == gate)
    def enter():
        pl.semaphore_wait(ready, 1)

    def meet_side():
        @pl.when(me < gate - 1)
        def side():
            pl.semaphore_wait(ready, 1)

        tell(corner, mz, flip(me, 2, n))

    def meet_planes():
        pl.semaphore_wait(corner, 1)

        @pl.when(me == gate)
        def spread():
            for k in range(1, m):
                tell(barrier, flip(mz, k, m), gate)
            pl.semaphore_wait(barrier, m - 1)
            for k in range(1, n):
                tell(planes, mz, flip(me, k, n))

        @pl.when(me != gate)
        def follow():
            pl.semaphore_wait(planes, 1)

    def to_expert(src, dst, send, recv, k):
        return pltpu.make_async_remote_copy(
            src_ref=src, dst_ref=dst, send_sem=send, recv_sem=recv,
            device_id=(mz, flip(me, k, n)), device_id_type=pl.DeviceIdType.MESH,
        )

    def to_dp(src, dst, sems):
        for k in range(1, m):
            pltpu.make_async_remote_copy(
                src_ref=src(k), dst_ref=dst(k), send_sem=sems.at[0], recv_sem=sems.at[1],
                device_id=(flip(mz, k, m), me), device_id_type=pl.DeviceIdType.MESH,
            ).start()

    def send(src, dst, sems, k):
        to_expert(src, dst, sems.at[0], sems.at[1], k).start()

    groups = []

    def group(every, sems):
        groups.append(to_expert(every, every, sems.at[0], sems.at[1], 1))
        return groups[-1]

    def arrive(moved):
        moved.wait_recv()

    def rows_of(mask, start, size):
        return pl.ds(pl.multiple_of(flip(me, mask, n) * own + start, GROUP), size)

    def open_axis(q):
        send(par_hbm.at[:, my_cols], allp.at[my_rows, my_cols], p_sems, 2 + 2 * q)
        send(go_hbm.at[q * half], mate.at[q, 0], o_sems, 2 + 2 * q)

    open_axis(me % 2)
    meet_side()
    open_axis(1 - me % 2)
    so_load = load(so_hbm, so, 1)
    go_load = load(go_hbm, go, 2)
    arrive(group(allp.at[pl.ds(0, 2 * own), my_cols], p_sems))
    for q in range(2):
        block = allp.at[rows_of(4 - 2 * q, (1 - q) * (own // 2), own // 2), my_cols]
        send(block, block, r_sems, AXES[q][0])
        send(go_hbm.at[pl.ds(q * half + 1, half - 1)], mate.at[q, pl.ds(1, half - 1)], o_sems, AXES[q][0])
    tok_load = load(tok_hbm, tok, 3)
    r_moved = group(allp.at[pl.ds(0, own), my_cols], r_sems)
    o_moved = group(mate, o_sems)

    so_load.wait()
    out_r = lax.broadcasted_iota(jnp.int32, (imgs * GROUP, GROUP * all_img), 0)
    in_c = lax.broadcasted_iota(jnp.int32, (imgs * GROUP, GROUP * all_img), 1)
    base = in_c - (out_r % GROUP) * all_img - (out_r // GROUP) % half
    first = out_r < half * GROUP

    def relayout(q, dest, out):
        own_at = dest * imgs + q * half
        mate_at = flip(dest, AXES[q][0], n) * imgs + q * half
        pick = jnp.where(base == jnp.where(first, own_at, mate_at), 1.0, 0.0).astype(BF)

        def one(g, carry):
            s0 = pl.multiple_of(g * GROUP, GROUP)
            block = so[pl.ds(s0, GROUP)].reshape(GROUP * all_img, width)
            moved = jnp.dot(pick, block, preferred_element_type=F32).astype(BF)
            out[:, pl.ds(s0, GROUP), :] = moved.reshape(imgs, GROUP, width)
            return carry

        lax.fori_loop(0, own // GROUP, one, 0)

    for i in range(3):
        for q in range(2):
            k = AXES[q][1][i]
            relayout(q, flip(me, k, n), stage.at[q, i])
            send(stage.at[q, i], rows.at[q, side_spot(q, me)], a_sems, k)
    a_moved = group(stage, a_sems)
    for q in range(2):
        relayout(q, me, rows.at[q, side_spot(q, me)])

    par_load.wait()
    arrive(r_moved)
    meet_planes()
    for i in range(n // 2):
        block = allp.at[rows_of(2 * i, 0, own), my_cols]
        to_dp(lambda k: block, lambda k: block, q_sems)
    q_moved = group(precv.at[pl.ds(1, m - 1)], q_sems)
    go_load.wait()
    tok_load.wait()
    arrive(q_moved)
    for i in range(n // 2):
        block = allp.at[rows_of(2 * i, 0, own)]
        send(block, block, f_sems, 1)
    f_moved = group(allp.at[pl.ds(0, n // 2 * own)], f_sems)
    arrive(f_moved)

    for q in range(2):

        def forward(t, carry):
            b = q * half + t
            logits = rows_last(allp[...], tok[b])
            peak = jnp.max(logits, axis=0, keepdims=True)
            raised = jnp.exp(logits - peak)
            comb[b] = raised / jnp.sum(raised, axis=0, keepdims=True)
            for p in range(2):
                low[q, t, p * quarter : (p + 1) * quarter] = comb[b, piece(q, False, p)].astype(BF)
                low_send[q, t, p * quarter : (p + 1) * quarter] = comb[b, piece(q, True, p)].astype(BF)
            return carry

        lax.fori_loop(0, half, forward, 0)
        send(low_send.at[q], low.at[q, pl.ds(half, half)], w_sems, AXES[q][0])
    w_moved = group(low_send, w_sems)

    def slot_grads(q, i, grads_in):
        out = jnp.dot(low[q, i], grads_in, preferred_element_type=F32).astype(BF)
        gs[q, :, i] = out.reshape(4, own, width)

    def comb_grads(q, i, grads_in):
        return rows_last(rows[q, :, i].reshape(4 * own, width), grads_in)

    for q in range(2):

        def own_slots(t, carry):
            slot_grads(q, t, go[q * half + t])
            return carry

        lax.fori_loop(0, half, own_slots, 0)

    arrive(o_moved)
    arrive(a_moved)
    for q in range(2):

        def mate_comb(t, carry):
            gc_send[q, t] = comb_grads(q, half + t, mate[q, t]).astype(BF)
            return carry

        lax.fori_loop(0, half, mate_comb, 0)
        send(gc_send.at[q], gc_recv.at[q], c_sems, AXES[q][0])
    c_moved = group(gc_send, c_sems)

    chunks = own // GROUP

    def landing(holder, images, j):
        if j == chunks - 1:
            return last.at[holder, images]
        return grec.at[holder, images, pl.ds(j * GROUP, GROUP)]

    def return_grads(h, parts, steps=(0, 1, 2)):
        part = pl.ds(h * half, half)
        for j in parts:
            for i in steps:
                for q in range(2):
                    k = AXES[q][1][i]
                    holder = flip(me, AXES[q][0], n) if h else me
                    send(
                        gs.at[q, side_spot(q, flip(me, k, n)), part, pl.ds(j * GROUP, GROUP)],
                        landing(holder, pl.ds(q * half, half), j), g_sems.at[j], k,
                    )
            for q in range(2 if 2 in steps else 0):
                holder = flip(me, AXES[q][0], n) if h else me
                pltpu.make_async_copy(
                    gs.at[q, side_spot(q, me), part, pl.ds(j * GROUP, GROUP)],
                    landing(holder, pl.ds(q * half, half), j), keep_sem.at[j],
                ).start()

    def all_grads(j, holders):
        return last.at[:holders] if j == chunks - 1 else grec.at[:holders, :, pl.ds(j * GROUP, GROUP)]

    g_moved = [group(all_grads(j, n - 2), g_sems.at[j]) for j in range(chunks)]

    return_grads(0, range(chunks))
    arrive(w_moved)
    for q in range(2):

        def mate_slots(t, carry):
            slot_grads(q, half + t, mate[q, t])
            return carry

        lax.fori_loop(0, half, mate_slots, 0)
    return_grads(1, range(chunks - 2))

    for q in range(2):

        def own_comb(t, carry):
            grads = comb_grads(q, t, go[q * half + t])
            for p in range(2):
                gcf[q * half + t, piece(q, False, p)] = grads[p * quarter : (p + 1) * quarter]
            return carry

        lax.fori_loop(0, half, own_comb, 0)
    acc[...] = jnp.zeros_like(acc)
    arrive(c_moved)
    for q in range(2):

        def backward(t, carry):
            b = q * half + t
            for p in range(2):
                gcf[b, piece(q, True, p)] = gc_recv[q, t, p * quarter : (p + 1) * quarter].astype(F32)
            grad_comb = gcf[b]
            weights = comb[b]
            rowdot = jnp.sum(weights * grad_comb, axis=0, keepdims=True)
            wide = weights * (grad_comb - rowdot)
            gcf[b] = wide
            acc[...] += jnp.dot(wide.astype(BF), tok[b], preferred_element_type=F32)
            return carry

        lax.fori_loop(0, half, backward, 0)

    core = me % 2
    for i in range(n // 2):
        ksend[i] = acc[pl.ds(pl.multiple_of((2 * i + 1 - core) * own, GROUP), own)].astype(BF)
    send(ksend, krecv, k_sems, 1)
    k_moved = group(ksend, k_sems)
    arrive(k_moved)
    for i in range(n // 2):
        red[i] = acc[pl.ds(pl.multiple_of((2 * i + core) * own, GROUP), own)] + krecv[i].astype(F32)
    for k in range(1, m):
        there = flip(mz, k, m)
        psend[k] = red[:, :, pl.ds(pl.multiple_of(there * cols, 128), cols)].astype(BF)
    to_dp(lambda k: psend.at[k], lambda k: precv.at[k], z_sems)
    z_moved = group(psend.at[pl.ds(1, m - 1)], z_sems)

    def token_grads(b, carry):
        gt[b] = jnp.dot(gcf[b].T.astype(BF), allp[...], preferred_element_type=F32).astype(BF)
        return carry

    lax.fori_loop(0, imgs, token_grads, 0)
    arrive(z_moved)
    total = red[:, :, my_cols]
    for k in range(1, m):
        total = total + precv[k].astype(F32)
    red[:, :, my_cols] = total

    def share(mask, q):
        return flip(me, mask, n) // 2, slice(q * (own // 2), (q + 1) * (own // 2)), my_cols

    for q in range(2):
        for i, mask in enumerate((AXES[q][0], 6)):
            xsend[q, i] = red[share(mask, q)].astype(BF)
        send(xsend.at[q, pl.ds(0, 2)], xrecv.at[q, pl.ds(0, 2)], x_sems, AXES[q][0])
    x_moved = group(xsend.at[:, pl.ds(0, 2)], x_sems)
    return_grads(1, (chunks - 2,))
    return_grads(1, (chunks - 1,), (0,))

    def settle_grads(j):
        every = all_grads(j, 2)
        pltpu.make_async_copy(every, every, keep_sem.at[j]).wait()
        arrive(g_moved[j])

        def swap(c, carry):
            lanes = pl.ds(pl.multiple_of(c * LANES, LANES), LANES)
            block = grec[:, :, j * GROUP : (j + 1) * GROUP, lanes].reshape(n * imgs, GROUP, LANES)
            done[j * GROUP : (j + 1) * GROUP, :, lanes] = jnp.swapaxes(block, 0, 1)
            return carry

        lax.fori_loop(0, width // LANES, swap, 0)

    for j in range(chunks - 3):
        settle_grads(j)
    arrive(x_moved)
    for q in range(2):
        for i, mask in enumerate((0, 4 - 2 * q)):
            red[share(mask, q)] += xrecv[q, i].astype(F32)
        xsend[q, 2] = red[share(4 - 2 * q, q)].astype(BF)
        send(xsend.at[q, 2], xrecv.at[q, 2], y_sems, 4 - 2 * q)
    y_moved = group(xsend.at[:, 2], y_sems)
    return_grads(1, (chunks - 1,), (1, 2))
    for j in range(chunks - 3, chunks - 1):
        settle_grads(j)
    arrive(y_moved)
    for q in range(2):
        gp[q * (own // 2) : (q + 1) * (own // 2)] = red[share(0, q)] + xrecv[q, 2].astype(F32)
    every = all_grads(chunks - 1, 2)
    pltpu.make_async_copy(every, every, keep_sem.at[chunks - 1]).wait()
    for moved in groups:
        moved.wait_send()
    arrive(g_moved[chunks - 1])


def paired_exchange(n, m, tok, go, so, par):
    imgs, patches, width = tok.shape
    own, all_img, _ = so.shape
    slots, cols, half = own * n, width // m, imgs // 2
    dma = pltpu.SemaphoreType.DMA
    return pl.pallas_call(
        functools.partial(paired_kernel, n, m),
        out_shape=(
            pltpu.VMEM((own - GROUP, all_img, width), BF),
            pltpu.VMEM((n, imgs, GROUP, width), BF),
            pltpu.VMEM((imgs, patches, width), BF),
            pltpu.VMEM((own, cols), F32),
        ),
        in_specs=[pl.BlockSpec(memory_space=pl.ANY)] * 4,
        out_specs=(pl.BlockSpec(memory_space=pltpu.VMEM),) * 4,
        scratch_shapes=[
            pltpu.VMEM((imgs, patches, width), BF),
            pltpu.VMEM((imgs, patches, width), BF),
            pltpu.VMEM((2, half, patches, width), BF),
            pltpu.VMEM((own, all_img, width), BF),
            pltpu.VMEM((slots, width), BF),
            pltpu.VMEM((2, 3, imgs, own, width), BF),
            pltpu.VMEM((2, 4, imgs, own, width), BF),
            pltpu.VMEM((2, 4, imgs, own, width), BF),
            pltpu.VMEM((imgs, slots, patches), F32),
            pltpu.VMEM((imgs, slots, patches), F32),
            pltpu.VMEM((2, imgs, slots // 2, patches), BF),
            pltpu.VMEM((2, half, slots // 2, patches), BF),
            pltpu.VMEM((2, half, slots // 2, patches), BF),
            pltpu.VMEM((2, half, slots // 2, patches), BF),
            pltpu.VMEM((n, imgs, own - GROUP, width), BF),
            pltpu.VMEM((slots, width), F32),
            pltpu.VMEM((n // 2, own, width), BF),
            pltpu.VMEM((n // 2, own, width), BF),
            pltpu.VMEM((n // 2, own, width), F32),
            pltpu.VMEM((m, n // 2, own, cols), BF),
            pltpu.VMEM((m, n // 2, own, cols), BF),
            pltpu.VMEM((2, 3, own // 2, cols), BF),
            pltpu.VMEM((2, 3, own // 2, cols), BF),
            pltpu.SemaphoreType.REGULAR, pltpu.SemaphoreType.REGULAR, pltpu.SemaphoreType.REGULAR,
            dma((4,)), dma((own // GROUP,)), dma((2,)), dma((2,)), dma((2,)), dma((2,)), dma((2,)), dma((2,)), dma((2,)), dma((2,)),
            dma((2,)), dma((own // GROUP, 2)), dma((2,)), dma((2,)), dma((2,)),
        ],
        compiler_params=pltpu.CompilerParams(
            collective_id=0, has_side_effects=True, vmem_limit_bytes=56 * 1000 * 1000
        ),
    )(tok, go, so, par)


def settle_kernel(arrived, gp_in, out, gp_out):
    out[...] = jnp.swapaxes(arrived[...], 0, 1)
    gp_out[...] = gp_in[...]


def settle(arrived, grad_par):
    all_img, own, width = arrived.shape
    small = pl.BlockSpec((GROUP, grad_par.shape[1]), lambda i: (i, 0))
    return pl.pallas_call(
        settle_kernel,
        grid=(own // GROUP,),
        out_shape=(
            jax.ShapeDtypeStruct((own, all_img, width), BF),
            jax.ShapeDtypeStruct(grad_par.shape, F32),
        ),
        in_specs=[pl.BlockSpec((all_img, GROUP, width), lambda i: (0, i, 0)), small],
        out_specs=(pl.BlockSpec((GROUP, all_img, width), lambda i: (i, 0, 0)), small),
    )(arrived, grad_par)


def finish_kernel(done, last, gt, gp, slot_out, tok_out, par_out, turned, sem):
    own = done.shape[0]
    group, all_img, width = turned.shape
    copies = []

    def put(src, dst, at):
        copies.append(pltpu.make_async_copy(src, dst, sem.at[at]))
        copies[-1].start()

    for g in range(own // group):
        rows = pl.ds(g * group, group)
        put(done.at[rows], slot_out.at[rows], 0)
    for b in range(gt.shape[0]):
        put(gt.at[b], tok_out.at[b], 1)
    put(gp, par_out, 2)
    tiles = width // LANES
    for part in range(2):

        def swap(c, carry):
            lanes = pl.ds(pl.multiple_of((part * (tiles // 2) + c) * LANES, LANES), LANES)
            turned[:, :, lanes] = jnp.swapaxes(last[:, :, :, lanes].reshape(all_img, group, LANES), 0, 1)
            return carry

        lax.fori_loop(0, tiles // 2, swap, 0)
        lanes = pl.ds(part * (width // 2), width // 2)
        put(turned.at[:, :, lanes], slot_out.at[pl.ds(own, group), :, lanes], 3)
    for copy in copies:
        copy.wait()


def finish(done, last, gt, gp):
    own, all_img, width = done.shape
    return pl.pallas_call(
        finish_kernel,
        out_shape=(
            jax.ShapeDtypeStruct((own + GROUP, all_img, width), BF),
            jax.ShapeDtypeStruct(gt.shape, BF),
            jax.ShapeDtypeStruct(gp.shape, F32),
        ),
        in_specs=[pl.BlockSpec(memory_space=pltpu.VMEM)] * 4,
        out_specs=(pl.BlockSpec(memory_space=pl.ANY),) * 3,
        scratch_shapes=[pltpu.VMEM((GROUP, all_img, width), BF), pltpu.SemaphoreType.DMA((4,))],
        compiler_params=pltpu.CompilerParams(vmem_limit_bytes=16 * 1000 * 1000),
    )(done, last, gt, gp)


def per_device(n, m, tokens, grad_out, slot_out, slot_params):
    tok = jnp.transpose(tokens, (1, 0, 2))
    go = jnp.transpose(grad_out, (1, 0, 2))
    if n == 8 and tok.shape[0] % 2 == 0 and tok.shape[0] > 2:
        grad_slot, grad_tok, grad_par = finish(*paired_exchange(n, m, tok, go, slot_out, slot_params))
    else:
        arrived, grad_tok, grad_par = exchange(n, m, tok, go, slot_out, slot_params)
        own, all_img, width = slot_out.shape
        grad_slot, grad_par = settle(arrived.reshape(all_img, own, width), grad_par)
    return jnp.transpose(grad_tok, (1, 0, 2)), grad_slot, grad_par


def solution(mesh):
    return jax.shard_map(
        functools.partial(per_device, mesh.shape["expert"], mesh.shape["dp"]),
        mesh=mesh,
        in_specs=(
            P(None, ("dp", "expert"), None),
            P(None, ("dp", "expert"), None),
            P("expert", "dp", None),
            P("expert", None),
        ),
        out_specs=(P(None, ("dp", "expert"), None), P("expert", "dp", None), P("expert", "dp")),
        check_vma=False,
    )
```

```python
import functools

import jax
import jax.numpy as jnp
from jax import lax
from jax.experimental import pallas as pl
from jax.experimental.pallas import tpu as pltpu
from jax.sharding import PartitionSpec as P

BF = jnp.bfloat16
F32 = jnp.float32
GROUP = 16
LANES = 128


def flip(index, mask, size):
    total, bit = 0, 1
    while bit < size:
        total = total + ((index // bit + mask // bit) % 2) * bit
        bit *= 2
    return total


def send_order(n, core):
    if n != 8:
        return list(range(n - 1, 0, -1))
    masks = []
    for low in range(2):
        masks += [6 + low - 4 * core, 2 + low + 2 * core, 4 + low + 2 * core]
    return masks + [1]


def rows_last(lhs, rhs):
    return lax.dot_general(lhs, rhs, (((1,), (1,)), ((), ())), preferred_element_type=F32)


def exchange_kernel(
    n, m, tok_hbm, go_hbm, so_hbm, par_hbm,
    grec, gt_out, gp_out,
    tok, go, so, par, allp, stage, rows, gs, comb, gt, acc, psend, precv, xsend, xrecv, gp,
    local_sem, p_send, p_recv, q_send, q_recv, a_send, a_recv, g_send, g_recv,
    z_send, z_recv, x_send, x_recv,
):
    me = lax.axis_index("expert")
    mz = lax.axis_index("dp")
    core = me % 2
    imgs = tok.shape[0]
    own = par.shape[0]
    all_img = so.shape[1]
    cols = allp.shape[1] // m
    width = allp.shape[1]
    slots = allp.shape[0]
    my_cols = pl.ds(pl.multiple_of(mz * cols, 128), cols)
    my_rows = pl.ds(pl.multiple_of(me * own, GROUP), own)

    loads = [
        pltpu.make_async_copy(src, dst, local_sem.at[i])
        for i, (src, dst) in enumerate([(par_hbm, par), (so_hbm, so), (tok_hbm, tok), (go_hbm, go)])
    ]
    for load in loads:
        load.start()

    barrier = pltpu.get_barrier_semaphore()
    for k in range(1, n):
        pl.semaphore_signal(barrier, inc=1, device_id=(mz, flip(me, k, n)), device_id_type=pl.DeviceIdType.MESH)
    for k in range(1, m):
        pl.semaphore_signal(barrier, inc=1, device_id=(flip(mz, k, m), me), device_id_type=pl.DeviceIdType.MESH)
    pl.semaphore_wait(barrier, n + m - 2)

    def to_expert(src, dst, send, recv, k):
        return pltpu.make_async_remote_copy(
            src_ref=src, dst_ref=dst, send_sem=send.at[k], recv_sem=recv.at[k],
            device_id=(mz, flip(me, k, n)), device_id_type=pl.DeviceIdType.MESH,
        )

    def to_dp(src, dst, send, recv, k):
        return pltpu.make_async_remote_copy(
            src_ref=src, dst_ref=dst, send_sem=send.at[k], recv_sem=recv.at[k],
            device_id=(flip(mz, k, m), me), device_id_type=pl.DeviceIdType.MESH,
        )

    loads[0].wait()
    p_copies = [to_expert(par.at[:, my_cols], allp.at[my_rows, my_cols], p_send, p_recv, k) for k in range(1, n)]
    for copy in p_copies:
        copy.start()
    allp[my_rows, my_cols] = par[:, my_cols]

    loads[1].wait()
    out_r = lax.broadcasted_iota(jnp.int32, (imgs * GROUP, GROUP * all_img), 0)
    in_c = lax.broadcasted_iota(jnp.int32, (imgs * GROUP, GROUP * all_img), 1)
    base = in_c - (out_r % GROUP) * all_img - out_r // GROUP

    def relayout(dest, out):
        pick = jnp.where(base == dest * imgs, 1.0, 0.0).astype(BF)

        def one(g, carry):
            s0 = pl.multiple_of(g * GROUP, GROUP)
            block = so[pl.ds(s0, GROUP)].reshape(GROUP * all_img, width)
            moved = jnp.dot(pick, block, preferred_element_type=F32).astype(BF)
            out[:, pl.ds(s0, GROUP), :] = moved.reshape(imgs, GROUP, width)
            return carry

        lax.fori_loop(0, own // GROUP, one, 0)

    order = send_order(n, core)
    a_copies = []
    for k in order:
        relayout(flip(me, k, n), stage.at[k])
        copy = to_expert(stage.at[k], rows.at[me], a_send, a_recv, k)
        copy.start()
        a_copies.append(copy)
    relayout(me, rows.at[me])

    for copy in p_copies:
        copy.wait_recv()
    q_copies = [to_dp(allp.at[:, my_cols], allp.at[:, my_cols], q_send, q_recv, k) for k in range(1, m)]
    for copy in q_copies:
        copy.start()
    loads[2].wait()
    loads[3].wait()
    for copy in q_copies:
        copy.wait_recv()

    def forward(b, carry):
        logits = rows_last(allp[...], tok[b])
        peak = jnp.max(logits, axis=0, keepdims=True)
        raised = jnp.exp(logits - peak)
        weights = raised / jnp.sum(raised, axis=0, keepdims=True)
        comb[b] = weights
        grads = jnp.dot(weights.astype(BF), go[b], preferred_element_type=F32).astype(BF)
        gs[:, b] = grads.reshape(n, own, width)
        return carry

    lax.fori_loop(0, imgs, forward, 0)

    keep = pltpu.make_async_copy(gs.at[me], grec.at[me], local_sem.at[4])
    keep.start()
    g_copies = []
    for k in order:
        copy = to_expert(gs.at[flip(me, k, n)], grec.at[me], g_send, g_recv, k)
        copy.start()
        g_copies.append(copy)

    for copy in a_copies:
        copy.wait_recv()
    acc[...] = jnp.zeros_like(acc)

    def backward(b, carry):
        grad_comb = rows_last(rows[:, b].reshape(slots, width), go[b])
        weights = comb[b]
        rowdot = jnp.sum(weights * grad_comb, axis=0, keepdims=True)
        wide = weights * (grad_comb - rowdot)
        acc[...] += jnp.dot(wide.astype(BF), tok[b], preferred_element_type=F32)
        gt[b] = jnp.dot(wide.T.astype(BF), allp[...], preferred_element_type=F32).astype(BF)
        return carry

    lax.fori_loop(0, imgs, backward, 0)

    for k in range(1, m):
        there = flip(mz, k, m)
        psend[k] = acc[:, pl.ds(pl.multiple_of(there * cols, 128), cols)].astype(BF)
    z_copies = [to_dp(psend.at[k], precv.at[k], z_send, z_recv, k) for k in range(1, m)]
    for copy in z_copies:
        copy.start()
    put = pltpu.make_async_copy(gt, gt_out, local_sem.at[5])
    put.start()
    for copy in z_copies:
        copy.wait_recv()
    total = acc[:, my_cols]
    for k in range(1, m):
        total = total + precv[k].astype(F32)
    acc[:, my_cols] = total
    for k in range(1, n):
        there = flip(me, k, n)
        xsend[k] = acc[pl.ds(pl.multiple_of(there * own, GROUP), own), my_cols].astype(BF)
    x_copies = [to_expert(xsend.at[k], xrecv.at[k], x_send, x_recv, k) for k in range(1, n)]
    for copy in x_copies:
        copy.start()
    for copy in x_copies:
        copy.wait_recv()
    owned = acc[my_rows, my_cols]
    for k in range(1, n):
        owned = owned + xrecv[k].astype(F32)
    gp[...] = owned
    give = pltpu.make_async_copy(gp, gp_out, local_sem.at[6])
    give.start()

    for copy in g_copies:
        copy.wait_recv()
    for copy in p_copies + a_copies + q_copies + g_copies + z_copies + x_copies:
        copy.wait_send()
    keep.wait()
    put.wait()
    give.wait()


def exchange(n, m, tok, go, so, par):
    imgs, patches, width = tok.shape
    own, all_img, _ = so.shape
    slots, cols = own * n, width // m
    dma = pltpu.SemaphoreType.DMA
    return pl.pallas_call(
        functools.partial(exchange_kernel, n, m),
        out_shape=(
            jax.ShapeDtypeStruct((n, imgs, own, width), BF),
            jax.ShapeDtypeStruct((imgs, patches, width), BF),
            jax.ShapeDtypeStruct((own, cols), F32),
        ),
        in_specs=[pl.BlockSpec(memory_space=pl.ANY)] * 4,
        out_specs=(pl.BlockSpec(memory_space=pl.ANY),) * 3,
        scratch_shapes=[
            pltpu.VMEM((imgs, patches, width), BF),
            pltpu.VMEM((imgs, patches, width), BF),
            pltpu.VMEM((own, all_img, width), BF),
            pltpu.VMEM((own, width), BF),
            pltpu.VMEM((slots, width), BF),
            pltpu.VMEM((n, imgs, own, width), BF),
            pltpu.VMEM((n, imgs, own, width), BF),
            pltpu.VMEM((n, imgs, own, width), BF),
            pltpu.VMEM((imgs, slots, patches), F32),
            pltpu.VMEM((imgs, patches, width), BF),
            pltpu.VMEM((slots, width), F32),
            pltpu.VMEM((m, slots, cols), BF),
            pltpu.VMEM((m, slots, cols), BF),
            pltpu.VMEM((n, own, cols), BF),
            pltpu.VMEM((n, own, cols), BF),
            pltpu.VMEM((own, cols), F32),
            dma((7,)),
            dma((n,)), dma((n,)), dma((m,)), dma((m,)),
            dma((n,)), dma((n,)), dma((n,)), dma((n,)),
            dma((m,)), dma((m,)), dma((n,)), dma((n,)),
        ],
        compiler_params=pltpu.CompilerParams(
            collective_id=0, has_side_effects=True, vmem_limit_bytes=66 * 1000 * 1000
        ),
    )(tok, go, so, par)


AXES = ((2, (4, 5, 1)), (4, (2, 3, 1)))


def side_spot(which, index):
    high = index // 4 if which == 0 else (index // 2) % 2
    return high * 2 + index % 2


def paired_kernel(
    n, m, tok_hbm, go_hbm, so_hbm, par_hbm,
    done, last, gt, gp,
    tok, go, mate, so, allp, stage, rows, gs, comb, gcf, low, low_send, gc_send, gc_recv,
    grec, acc, ksend, krecv, red, psend, precv, xsend, xrecv,
    ready, corner, planes, local_sem, keep_sem, p_sems, r_sems, q_sems, f_sems, k_sems, o_sems, a_sems, w_sems,
    c_sems, g_sems, z_sems, x_sems, y_sems,
):
    me = lax.axis_index("expert")
    mz = lax.axis_index("dp")
    imgs = tok.shape[0]
    half = imgs // 2
    own = par_hbm.shape[0]
    all_img = so.shape[1]
    slots, width = allp.shape
    patches = tok.shape[1]
    cols = width // m
    quarter = slots // 4
    my_cols = pl.ds(pl.multiple_of(mz * cols, 128), cols)
    my_rows = pl.ds(pl.multiple_of(me * own, GROUP), own)
    sides = ((me // 2) % 2, me // 4)

    def piece(which, other, p):
        side = 1 - sides[which] if other else sides[which]
        start = p * 2 * quarter + side * quarter if which == 0 else side * 2 * quarter + p * quarter
        return pl.ds(pl.multiple_of(start, quarter), quarter)

    def load(src, dst, at):
        copy = pltpu.make_async_copy(src, dst, local_sem.at[at])
        copy.start()
        return copy

    par_load = load(par_hbm.at[:, my_cols], allp.at[my_rows, my_cols], 0)

    gate = n - 1
    barrier = pltpu.get_barrier_semaphore()

    def tell(sem, plane, index):
        pl.semaphore_signal(sem, inc=1, device_id=(plane, index), device_id_type=pl.DeviceIdType.MESH)

    partner = flip(me, 1, n)
    high = me // 4
    early = (me + high + 1) % 2
    for mask in (2, 4):
        host = flip(me, mask, n) // 2 * 2 + 1 - high
        tell(barrier, mz, jnp.where(host == gate, gate - 1, host))

    @pl.when(partner != gate)
    def greet():
        tell(barrier, mz, partner)

    @pl.when(me < gate - 1)
    def meet():
        pl.semaphore_wait(barrier, 3)

    @pl.when(me == gate - 1)
    def meet_all():
        pl.semaphore_wait(barrier, 5)

    @pl.when(me != gate)
    def pass_on():
        tell(ready, mz, partner)

    @pl.when(me == gate)
    def enter():
        pl.semaphore_wait(ready, 1)

    def meet_side():
        @pl.when(me < gate - 1)
        def side():
            pl.semaphore_wait(ready, 1)

        tell(corner, mz, flip(me, 2, n))

    def meet_planes():
        pl.semaphore_wait(corner, 1)

        @pl.when(me == gate)
        def spread():
            for k in range(1, m):
                tell(barrier, flip(mz, k, m), gate)
            pl.semaphore_wait(barrier, m - 1)
            for k in range(1, n):
                tell(planes, mz, flip(me, k, n))

        @pl.when(me != gate)
        def follow():
            pl.semaphore_wait(planes, 1)

    def to_expert(src, dst, send, recv, k):
        return pltpu.make_async_remote_copy(
            src_ref=src, dst_ref=dst, send_sem=send, recv_sem=recv,
            device_id=(mz, flip(me, k, n)), device_id_type=pl.DeviceIdType.MESH,
        )

    def to_dp(src, dst, sems):
        for k in range(1, m):
            pltpu.make_async_remote_copy(
                src_ref=src(k), dst_ref=dst(k), send_sem=sems.at[0], recv_sem=sems.at[1],
                device_id=(flip(mz, k, m), me), device_id_type=pl.DeviceIdType.MESH,
            ).start()

    def send(src, dst, sems, k):
        to_expert(src, dst, sems.at[0], sems.at[1], k).start()

    groups = []

    def group(every, sems):
        groups.append(to_expert(every, every, sems.at[0], sems.at[1], 1))
        return groups[-1]

    def arrive(moved):
        moved.wait_recv()

    def rows_of(mask, start, size):
        return pl.ds(pl.multiple_of(flip(me, mask, n) * own + start, GROUP), size)

    def open_axis(q):
        send(par_hbm.at[:, my_cols], allp.at[my_rows, my_cols], p_sems, 2 + 2 * q)
        send(go_hbm.at[q * half], mate.at[q, 0], o_sems, 2 + 2 * q)

    open_axis(early)
    meet_side()
    open_axis(1 - early)
    so_load = load(so_hbm, so, 1)
    go_load = load(go_hbm, go, 2)
    arrive(group(allp.at[pl.ds(0, 2 * own), my_cols], p_sems))
    for q in range(2):
        block = allp.at[rows_of(4 - 2 * q, (1 - q) * (own // 2), own // 2), my_cols]
        send(block, block, r_sems, AXES[q][0])
        send(go_hbm.at[pl.ds(q * half + 1, half - 1)], mate.at[q, pl.ds(1, half - 1)], o_sems, AXES[q][0])
    tok_load = load(tok_hbm, tok, 3)
    r_moved = group(allp.at[pl.ds(0, own), my_cols], r_sems)
    o_moved = group(mate, o_sems)

    so_load.wait()
    out_r = lax.broadcasted_iota(jnp.int32, (imgs * GROUP, GROUP * all_img), 0)
    in_c = lax.broadcasted_iota(jnp.int32, (imgs * GROUP, GROUP * all_img), 1)
    base = in_c - (out_r % GROUP) * all_img - (out_r // GROUP) % half
    first = out_r < half * GROUP

    def relayout(q, dest, out):
        own_at = dest * imgs + q * half
        mate_at = flip(dest, AXES[q][0], n) * imgs + q * half
        pick = jnp.where(base == jnp.where(first, own_at, mate_at), 1.0, 0.0).astype(BF)

        def one(g, carry):
            s0 = pl.multiple_of(g * GROUP, GROUP)
            block = so[pl.ds(s0, GROUP)].reshape(GROUP * all_img, width)
            moved = jnp.dot(pick, block, preferred_element_type=F32).astype(BF)
            out[:, pl.ds(s0, GROUP), :] = moved.reshape(imgs, GROUP, width)
            return carry

        lax.fori_loop(0, own // GROUP, one, 0)

    for i in range(3):
        for q in range(2):
            k = AXES[q][1][i]
            relayout(q, flip(me, k, n), stage.at[q, i])
            send(stage.at[q, i], rows.at[q, side_spot(q, me)], a_sems, k)
    a_moved = group(stage, a_sems)
    for q in range(2):
        relayout(q, me, rows.at[q, side_spot(q, me)])

    par_load.wait()
    arrive(r_moved)
    meet_planes()
    for i in range(n // 2):
        block = allp.at[rows_of(2 * i, 0, own), my_cols]
        to_dp(lambda k: block, lambda k: block, q_sems)
    q_moved = group(precv.at[pl.ds(1, m - 1)], q_sems)
    go_load.wait()
    tok_load.wait()
    arrive(q_moved)
    for i in range(n // 2):
        block = allp.at[rows_of(2 * i, 0, own)]
        send(block, block, f_sems, 1)
    f_moved = group(allp.at[pl.ds(0, n // 2 * own)], f_sems)
    arrive(f_moved)

    for q in range(2):

        def forward(t, carry):
            b = q * half + t
            logits = rows_last(allp[...], tok[b])
            peak = jnp.max(logits, axis=0, keepdims=True)
            raised = jnp.exp(logits - peak)
            comb[b] = raised / jnp.sum(raised, axis=0, keepdims=True)
            for p in range(2):
                low[q, t, p * quarter : (p + 1) * quarter] = comb[b, piece(q, False, p)].astype(BF)
                low_send[q, t, p * quarter : (p + 1) * quarter] = comb[b, piece(q, True, p)].astype(BF)
            return carry

        lax.fori_loop(0, half, forward, 0)
        send(low_send.at[q], low.at[q, pl.ds(half, half)], w_sems, AXES[q][0])
    w_moved = group(low_send, w_sems)

    def slot_grads(q, i, grads_in):
        out = jnp.dot(low[q, i], grads_in, preferred_element_type=F32).astype(BF)
        gs[q, :, i] = out.reshape(4, own, width)

    def comb_grads(q, i, grads_in):
        return rows_last(rows[q, :, i].reshape(4 * own, width), grads_in)

    for q in range(2):

        def own_slots(t, carry):
            slot_grads(q, t, go[q * half + t])
            return carry

        lax.fori_loop(0, half, own_slots, 0)

    arrive(o_moved)
    arrive(a_moved)
    for q in range(2):

        def mate_comb(t, carry):
            gc_send[q, t] = comb_grads(q, half + t, mate[q, t]).astype(BF)
            return carry

        lax.fori_loop(0, half, mate_comb, 0)
        send(gc_send.at[q], gc_recv.at[q], c_sems, AXES[q][0])
    c_moved = group(gc_send, c_sems)

    chunks = own // GROUP

    def landing(holder, images, j):
        if j == chunks - 1:
            return last.at[holder, images]
        return grec.at[holder, images, pl.ds(j * GROUP, GROUP)]

    def return_grads(h, parts, steps=(0, 1, 2)):
        part = pl.ds(h * half, half)
        for j in parts:
            for i in steps:
                for q in range(2):
                    k = AXES[q][1][i]
                    holder = flip(me, AXES[q][0], n) if h else me
                    send(
                        gs.at[q, side_spot(q, flip(me, k, n)), part, pl.ds(j * GROUP, GROUP)],
                        landing(holder, pl.ds(q * half, half), j), g_sems.at[j], k,
                    )
            for q in range(2 if 2 in steps else 0):
                holder = flip(me, AXES[q][0], n) if h else me
                pltpu.make_async_copy(
                    gs.at[q, side_spot(q, me), part, pl.ds(j * GROUP, GROUP)],
                    landing(holder, pl.ds(q * half, half), j), keep_sem.at[j],
                ).start()

    def all_grads(j, holders):
        return last.at[:holders] if j == chunks - 1 else grec.at[:holders, :, pl.ds(j * GROUP, GROUP)]

    g_moved = [group(all_grads(j, n - 2), g_sems.at[j]) for j in range(chunks)]

    return_grads(0, range(chunks))
    arrive(w_moved)
    for q in range(2):

        def mate_slots(t, carry):
            slot_grads(q, half + t, mate[q, t])
            return carry

        lax.fori_loop(0, half, mate_slots, 0)
    return_grads(1, range(chunks - 2))

    for q in range(2):

        def own_comb(t, carry):
            grads = comb_grads(q, t, go[q * half + t])
            for p in range(2):
                gcf[q * half + t, piece(q, False, p)] = grads[p * quarter : (p + 1) * quarter]
            return carry

        lax.fori_loop(0, half, own_comb, 0)
    acc[...] = jnp.zeros_like(acc)
    arrive(c_moved)
    for q in range(2):

        def backward(t, carry):
            b = q * half + t
            for p in range(2):
                gcf[b, piece(q, True, p)] = gc_recv[q, t, p * quarter : (p + 1) * quarter].astype(F32)
            grad_comb = gcf[b]
            weights = comb[b]
            rowdot = jnp.sum(weights * grad_comb, axis=0, keepdims=True)
            wide = weights * (grad_comb - rowdot)
            gcf[b] = wide
            acc[...] += jnp.dot(wide.astype(BF), tok[b], preferred_element_type=F32)
            return carry

        lax.fori_loop(0, half, backward, 0)

    core = me % 2
    for i in range(n // 2):
        ksend[i] = acc[pl.ds(pl.multiple_of((2 * i + 1 - core) * own, GROUP), own)].astype(BF)
    send(ksend, krecv, k_sems, 1)
    k_moved = group(ksend, k_sems)
    arrive(k_moved)
    for i in range(n // 2):
        red[i] = acc[pl.ds(pl.multiple_of((2 * i + core) * own, GROUP), own)] + krecv[i].astype(F32)
    for k in range(1, m):
        there = flip(mz, k, m)
        psend[k] = red[:, :, pl.ds(pl.multiple_of(there * cols, 128), cols)].astype(BF)
    to_dp(lambda k: psend.at[k], lambda k: precv.at[k], z_sems)
    z_moved = group(psend.at[pl.ds(1, m - 1)], z_sems)

    def token_grads(b, carry):
        gt[b] = jnp.dot(gcf[b].T.astype(BF), allp[...], preferred_element_type=F32).astype(BF)
        return carry

    lax.fori_loop(0, imgs, token_grads, 0)
    arrive(z_moved)
    total = red[:, :, my_cols]
    for k in range(1, m):
        total = total + precv[k].astype(F32)
    red[:, :, my_cols] = total

    def share(mask, q):
        return flip(me, mask, n) // 2, slice(q * (own // 2), (q + 1) * (own // 2)), my_cols

    for q in range(2):
        for i, mask in enumerate((AXES[q][0], 6)):
            xsend[q, i] = red[share(mask, q)].astype(BF)
        send(xsend.at[q, pl.ds(0, 2)], xrecv.at[q, pl.ds(0, 2)], x_sems, AXES[q][0])
    x_moved = group(xsend.at[:, pl.ds(0, 2)], x_sems)
    return_grads(1, (chunks - 2,))
    return_grads(1, (chunks - 1,), (0,))

    def settle_grads(j):
        every = all_grads(j, 2)
        pltpu.make_async_copy(every, every, keep_sem.at[j]).wait()
        arrive(g_moved[j])

        def swap(c, carry):
            lanes = pl.ds(pl.multiple_of(c * LANES, LANES), LANES)
            block = grec[:, :, j * GROUP : (j + 1) * GROUP, lanes].reshape(n * imgs, GROUP, LANES)
            done[j * GROUP : (j + 1) * GROUP, :, lanes] = jnp.swapaxes(block, 0, 1)
            return carry

        lax.fori_loop(0, width // LANES, swap, 0)

    for j in range(chunks - 3):
        settle_grads(j)
    arrive(x_moved)
    for q in range(2):
        for i, mask in enumerate((0, 4 - 2 * q)):
            red[share(mask, q)] += xrecv[q, i].astype(F32)
        xsend[q, 2] = red[share(4 - 2 * q, q)].astype(BF)
        send(xsend.at[q, 2], xrecv.at[q, 2], y_sems, 4 - 2 * q)
    y_moved = group(xsend.at[:, 2], y_sems)
    return_grads(1, (chunks - 1,), (1, 2))
    for j in range(chunks - 3, chunks - 1):
        settle_grads(j)
    arrive(y_moved)
    for q in range(2):
        gp[q * (own // 2) : (q + 1) * (own // 2)] = red[share(0, q)] + xrecv[q, 2].astype(F32)
    every = all_grads(chunks - 1, 2)
    pltpu.make_async_copy(every, every, keep_sem.at[chunks - 1]).wait()
    for moved in groups:
        moved.wait_send()
    arrive(g_moved[chunks - 1])


def paired_exchange(n, m, tok, go, so, par):
    imgs, patches, width = tok.shape
    own, all_img, _ = so.shape
    slots, cols, half = own * n, width // m, imgs // 2
    dma = pltpu.SemaphoreType.DMA
    return pl.pallas_call(
        functools.partial(paired_kernel, n, m),
        out_shape=(
            pltpu.VMEM((own - GROUP, all_img, width), BF),
            pltpu.VMEM((n, imgs, GROUP, width), BF),
            pltpu.VMEM((imgs, patches, width), BF),
            pltpu.VMEM((own, cols), F32),
        ),
        in_specs=[pl.BlockSpec(memory_space=pl.ANY)] * 4,
        out_specs=(pl.BlockSpec(memory_space=pltpu.VMEM),) * 4,
        scratch_shapes=[
            pltpu.VMEM((imgs, patches, width), BF),
            pltpu.VMEM((imgs, patches, width), BF),
            pltpu.VMEM((2, half, patches, width), BF),
            pltpu.VMEM((own, all_img, width), BF),
            pltpu.VMEM((slots, width), BF),
            pltpu.VMEM((2, 3, imgs, own, width), BF),
            pltpu.VMEM((2, 4, imgs, own, width), BF),
            pltpu.VMEM((2, 4, imgs, own, width), BF),
            pltpu.VMEM((imgs, slots, patches), F32),
            pltpu.VMEM((imgs, slots, patches), F32),
            pltpu.VMEM((2, imgs, slots // 2, patches), BF),
            pltpu.VMEM((2, half, slots // 2, patches), BF),
            pltpu.VMEM((2, half, slots // 2, patches), BF),
            pltpu.VMEM((2, half, slots // 2, patches), BF),
            pltpu.VMEM((n, imgs, own - GROUP, width), BF),
            pltpu.VMEM((slots, width), F32),
            pltpu.VMEM((n // 2, own, width), BF),
            pltpu.VMEM((n // 2, own, width), BF),
            pltpu.VMEM((n // 2, own, width), F32),
            pltpu.VMEM((m, n // 2, own, cols), BF),
            pltpu.VMEM((m, n // 2, own, cols), BF),
            pltpu.VMEM((2, 3, own // 2, cols), BF),
            pltpu.VMEM((2, 3, own // 2, cols), BF),
            pltpu.SemaphoreType.REGULAR, pltpu.SemaphoreType.REGULAR, pltpu.SemaphoreType.REGULAR,
            dma((4,)), dma((own // GROUP,)), dma((2,)), dma((2,)), dma((2,)), dma((2,)), dma((2,)), dma((2,)), dma((2,)), dma((2,)),
            dma((2,)), dma((own // GROUP, 2)), dma((2,)), dma((2,)), dma((2,)),
        ],
        compiler_params=pltpu.CompilerParams(
            collective_id=0, has_side_effects=True, vmem_limit_bytes=56 * 1000 * 1000
        ),
    )(tok, go, so, par)


def settle_kernel(arrived, gp_in, out, gp_out):
    out[...] = jnp.swapaxes(arrived[...], 0, 1)
    gp_out[...] = gp_in[...]


def settle(arrived, grad_par):
    all_img, own, width = arrived.shape
    small = pl.BlockSpec((GROUP, grad_par.shape[1]), lambda i: (i, 0))
    return pl.pallas_call(
        settle_kernel,
        grid=(own // GROUP,),
        out_shape=(
            jax.ShapeDtypeStruct((own, all_img, width), BF),
            jax.ShapeDtypeStruct(grad_par.shape, F32),
        ),
        in_specs=[pl.BlockSpec((all_img, GROUP, width), lambda i: (0, i, 0)), small],
        out_specs=(pl.BlockSpec((GROUP, all_img, width), lambda i: (i, 0, 0)), small),
    )(arrived, grad_par)


def finish_kernel(done, last, gt, gp, slot_out, tok_out, par_out, turned, sem):
    own = done.shape[0]
    group, all_img, width = turned.shape
    copies = []

    def put(src, dst, at):
        copies.append(pltpu.make_async_copy(src, dst, sem.at[at]))
        copies[-1].start()

    for g in range(own // group):
        rows = pl.ds(g * group, group)
        put(done.at[rows], slot_out.at[rows], 0)
    for b in range(gt.shape[0]):
        put(gt.at[b], tok_out.at[b], 1)
    put(gp, par_out, 2)
    tiles = width // LANES
    for part in range(2):

        def swap(c, carry):
            lanes = pl.ds(pl.multiple_of((part * (tiles // 2) + c) * LANES, LANES), LANES)
            turned[:, :, lanes] = jnp.swapaxes(last[:, :, :, lanes].reshape(all_img, group, LANES), 0, 1)
            return carry

        lax.fori_loop(0, tiles // 2, swap, 0)
        lanes = pl.ds(part * (width // 2), width // 2)
        put(turned.at[:, :, lanes], slot_out.at[pl.ds(own, group), :, lanes], 3)
    for copy in copies:
        copy.wait()


def finish(done, last, gt, gp):
    own, all_img, width = done.shape
    return pl.pallas_call(
        finish_kernel,
        out_shape=(
            jax.ShapeDtypeStruct((own + GROUP, all_img, width), BF),
            jax.ShapeDtypeStruct(gt.shape, BF),
            jax.ShapeDtypeStruct(gp.shape, F32),
        ),
        in_specs=[pl.BlockSpec(memory_space=pltpu.VMEM)] * 4,
        out_specs=(pl.BlockSpec(memory_space=pl.ANY),) * 3,
        scratch_shapes=[pltpu.VMEM((GROUP, all_img, width), BF), pltpu.SemaphoreType.DMA((4,))],
        compiler_params=pltpu.CompilerParams(vmem_limit_bytes=16 * 1000 * 1000),
    )(done, last, gt, gp)


def per_device(n, m, tokens, grad_out, slot_out, slot_params):
    tok = jnp.transpose(tokens, (1, 0, 2))
    go = jnp.transpose(grad_out, (1, 0, 2))
    if n == 8 and tok.shape[0] % 2 == 0 and tok.shape[0] > 2:
        grad_slot, grad_tok, grad_par = finish(*paired_exchange(n, m, tok, go, slot_out, slot_params))
    else:
        arrived, grad_tok, grad_par = exchange(n, m, tok, go, slot_out, slot_params)
        own, all_img, width = slot_out.shape
        grad_slot, grad_par = settle(arrived.reshape(all_img, own, width), grad_par)
    return jnp.transpose(grad_tok, (1, 0, 2)), grad_slot, grad_par


def solution(mesh):
    return jax.shard_map(
        functools.partial(per_device, mesh.shape["expert"], mesh.shape["dp"]),
        mesh=mesh,
        in_specs=(
            P(None, ("dp", "expert"), None),
            P(None, ("dp", "expert"), None),
            P("expert", "dp", None),
            P("expert", None),
        ),
        out_specs=(P(None, ("dp", "expert"), None), P("expert", "dp", None), P("expert", "dp")),
        check_vma=False,
    )
```

```python
import functools

import jax
import jax.numpy as jnp
from jax import lax
from jax.experimental import pallas as pl
from jax.experimental.pallas import tpu as pltpu
from jax.sharding import PartitionSpec as P

BF = jnp.bfloat16
F32 = jnp.float32
GROUP = 16
LANES = 128


def flip(index, mask, size):
    total, bit = 0, 1
    while bit < size:
        total = total + ((index // bit + mask // bit) % 2) * bit
        bit *= 2
    return total


def send_order(n, core):
    if n != 8:
        return list(range(n - 1, 0, -1))
    masks = []
    for low in range(2):
        masks += [6 + low - 4 * core, 2 + low + 2 * core, 4 + low + 2 * core]
    return masks + [1]


def rows_last(lhs, rhs):
    return lax.dot_general(lhs, rhs, (((1,), (1,)), ((), ())), preferred_element_type=F32)


def exchange_kernel(
    n, m, tok_hbm, go_hbm, so_hbm, par_hbm,
    grec, gt_out, gp_out,
    tok, go, so, par, allp, stage, rows, gs, comb, gt, acc, psend, precv, xsend, xrecv, gp,
    local_sem, p_send, p_recv, q_send, q_recv, a_send, a_recv, g_send, g_recv,
    z_send, z_recv, x_send, x_recv,
):
    me = lax.axis_index("expert")
    mz = lax.axis_index("dp")
    core = me % 2
    imgs = tok.shape[0]
    own = par.shape[0]
    all_img = so.shape[1]
    cols = allp.shape[1] // m
    width = allp.shape[1]
    slots = allp.shape[0]
    my_cols = pl.ds(pl.multiple_of(mz * cols, 128), cols)
    my_rows = pl.ds(pl.multiple_of(me * own, GROUP), own)

    loads = [
        pltpu.make_async_copy(src, dst, local_sem.at[i])
        for i, (src, dst) in enumerate([(par_hbm, par), (so_hbm, so), (tok_hbm, tok), (go_hbm, go)])
    ]
    for load in loads:
        load.start()

    barrier = pltpu.get_barrier_semaphore()
    for k in range(1, n):
        pl.semaphore_signal(barrier, inc=1, device_id=(mz, flip(me, k, n)), device_id_type=pl.DeviceIdType.MESH)
    for k in range(1, m):
        pl.semaphore_signal(barrier, inc=1, device_id=(flip(mz, k, m), me), device_id_type=pl.DeviceIdType.MESH)
    pl.semaphore_wait(barrier, n + m - 2)

    def to_expert(src, dst, send, recv, k):
        return pltpu.make_async_remote_copy(
            src_ref=src, dst_ref=dst, send_sem=send.at[k], recv_sem=recv.at[k],
            device_id=(mz, flip(me, k, n)), device_id_type=pl.DeviceIdType.MESH,
        )

    def to_dp(src, dst, send, recv, k):
        return pltpu.make_async_remote_copy(
            src_ref=src, dst_ref=dst, send_sem=send.at[k], recv_sem=recv.at[k],
            device_id=(flip(mz, k, m), me), device_id_type=pl.DeviceIdType.MESH,
        )

    loads[0].wait()
    p_copies = [to_expert(par.at[:, my_cols], allp.at[my_rows, my_cols], p_send, p_recv, k) for k in range(1, n)]
    for copy in p_copies:
        copy.start()
    allp[my_rows, my_cols] = par[:, my_cols]

    loads[1].wait()
    out_r = lax.broadcasted_iota(jnp.int32, (imgs * GROUP, GROUP * all_img), 0)
    in_c = lax.broadcasted_iota(jnp.int32, (imgs * GROUP, GROUP * all_img), 1)
    base = in_c - (out_r % GROUP) * all_img - out_r // GROUP

    def relayout(dest, out):
        pick = jnp.where(base == dest * imgs, 1.0, 0.0).astype(BF)

        def one(g, carry):
            s0 = pl.multiple_of(g * GROUP, GROUP)
            block = so[pl.ds(s0, GROUP)].reshape(GROUP * all_img, width)
            moved = jnp.dot(pick, block, preferred_element_type=F32).astype(BF)
            out[:, pl.ds(s0, GROUP), :] = moved.reshape(imgs, GROUP, width)
            return carry

        lax.fori_loop(0, own // GROUP, one, 0)

    order = send_order(n, core)
    a_copies = []
    for k in order:
        relayout(flip(me, k, n), stage.at[k])
        copy = to_expert(stage.at[k], rows.at[me], a_send, a_recv, k)
        copy.start()
        a_copies.append(copy)
    relayout(me, rows.at[me])

    for copy in p_copies:
        copy.wait_recv()
    q_copies = [to_dp(allp.at[:, my_cols], allp.at[:, my_cols], q_send, q_recv, k) for k in range(1, m)]
    for copy in q_copies:
        copy.start()
    loads[2].wait()
    loads[3].wait()
    for copy in q_copies:
        copy.wait_recv()

    def forward(b, carry):
        logits = rows_last(allp[...], tok[b])
        peak = jnp.max(logits, axis=0, keepdims=True)
        raised = jnp.exp(logits - peak)
        weights = raised / jnp.sum(raised, axis=0, keepdims=True)
        comb[b] = weights
        grads = jnp.dot(weights.astype(BF), go[b], preferred_element_type=F32).astype(BF)
        gs[:, b] = grads.reshape(n, own, width)
        return carry

    lax.fori_loop(0, imgs, forward, 0)

    keep = pltpu.make_async_copy(gs.at[me], grec.at[me], local_sem.at[4])
    keep.start()
    g_copies = []
    for k in order:
        copy = to_expert(gs.at[flip(me, k, n)], grec.at[me], g_send, g_recv, k)
        copy.start()
        g_copies.append(copy)

    for copy in a_copies:
        copy.wait_recv()
    acc[...] = jnp.zeros_like(acc)

    def backward(b, carry):
        grad_comb = rows_last(rows[:, b].reshape(slots, width), go[b])
        weights = comb[b]
        rowdot = jnp.sum(weights * grad_comb, axis=0, keepdims=True)
        wide = weights * (grad_comb - rowdot)
        acc[...] += jnp.dot(wide.astype(BF), tok[b], preferred_element_type=F32)
        gt[b] = jnp.dot(wide.T.astype(BF), allp[...], preferred_element_type=F32).astype(BF)
        return carry

    lax.fori_loop(0, imgs, backward, 0)

    for k in range(1, m):
        there = flip(mz, k, m)
        psend[k] = acc[:, pl.ds(pl.multiple_of(there * cols, 128), cols)].astype(BF)
    z_copies = [to_dp(psend.at[k], precv.at[k], z_send, z_recv, k) for k in range(1, m)]
    for copy in z_copies:
        copy.start()
    put = pltpu.make_async_copy(gt, gt_out, local_sem.at[5])
    put.start()
    for copy in z_copies:
        copy.wait_recv()
    total = acc[:, my_cols]
    for k in range(1, m):
        total = total + precv[k].astype(F32)
    acc[:, my_cols] = total
    for k in range(1, n):
        there = flip(me, k, n)
        xsend[k] = acc[pl.ds(pl.multiple_of(there * own, GROUP), own), my_cols].astype(BF)
    x_copies = [to_expert(xsend.at[k], xrecv.at[k], x_send, x_recv, k) for k in range(1, n)]
    for copy in x_copies:
        copy.start()
    for copy in x_copies:
        copy.wait_recv()
    owned = acc[my_rows, my_cols]
    for k in range(1, n):
        owned = owned + xrecv[k].astype(F32)
    gp[...] = owned
    give = pltpu.make_async_copy(gp, gp_out, local_sem.at[6])
    give.start()

    for copy in g_copies:
        copy.wait_recv()
    for copy in p_copies + a_copies + q_copies + g_copies + z_copies + x_copies:
        copy.wait_send()
    keep.wait()
    put.wait()
    give.wait()


def exchange(n, m, tok, go, so, par):
    imgs, patches, width = tok.shape
    own, all_img, _ = so.shape
    slots, cols = own * n, width // m
    dma = pltpu.SemaphoreType.DMA
    return pl.pallas_call(
        functools.partial(exchange_kernel, n, m),
        out_shape=(
            jax.ShapeDtypeStruct((n, imgs, own, width), BF),
            jax.ShapeDtypeStruct((imgs, patches, width), BF),
            jax.ShapeDtypeStruct((own, cols), F32),
        ),
        in_specs=[pl.BlockSpec(memory_space=pl.ANY)] * 4,
        out_specs=(pl.BlockSpec(memory_space=pl.ANY),) * 3,
        scratch_shapes=[
            pltpu.VMEM((imgs, patches, width), BF),
            pltpu.VMEM((imgs, patches, width), BF),
            pltpu.VMEM((own, all_img, width), BF),
            pltpu.VMEM((own, width), BF),
            pltpu.VMEM((slots, width), BF),
            pltpu.VMEM((n, imgs, own, width), BF),
            pltpu.VMEM((n, imgs, own, width), BF),
            pltpu.VMEM((n, imgs, own, width), BF),
            pltpu.VMEM((imgs, slots, patches), F32),
            pltpu.VMEM((imgs, patches, width), BF),
            pltpu.VMEM((slots, width), F32),
            pltpu.VMEM((m, slots, cols), BF),
            pltpu.VMEM((m, slots, cols), BF),
            pltpu.VMEM((n, own, cols), BF),
            pltpu.VMEM((n, own, cols), BF),
            pltpu.VMEM((own, cols), F32),
            dma((7,)),
            dma((n,)), dma((n,)), dma((m,)), dma((m,)),
            dma((n,)), dma((n,)), dma((n,)), dma((n,)),
            dma((m,)), dma((m,)), dma((n,)), dma((n,)),
        ],
        compiler_params=pltpu.CompilerParams(
            collective_id=0, has_side_effects=True, vmem_limit_bytes=66 * 1000 * 1000
        ),
    )(tok, go, so, par)


AXES = ((2, (4, 5, 1)), (4, (2, 3, 1)))


def side_spot(which, index):
    high = index // 4 if which == 0 else (index // 2) % 2
    return high * 2 + index % 2


def paired_kernel(
    n, m, tok_hbm, go_hbm, so_hbm, par_hbm,
    done, last, gt, gp,
    tok, go, mate, so, allp, stage, rows, gs, comb, gcf, low, low_send, gc_send, gc_recv,
    grec, acc, ksend, krecv, red, psend, precv, xsend, xrecv,
    ready, corner, planes, local_sem, keep_sem, p_sems, q_sems, f_sems, o_sems, a_sems, w_sems,
    g_sems, z_sems, x_sems,
):
    me = lax.axis_index("expert")
    mz = lax.axis_index("dp")
    imgs = tok.shape[0]
    half = imgs // 2
    own = par_hbm.shape[0]
    all_img = so.shape[1]
    slots, width = allp.shape
    patches = tok.shape[1]
    cols = width // m
    quarter = slots // 4
    my_cols = pl.ds(pl.multiple_of(mz * cols, 128), cols)
    my_rows = pl.ds(pl.multiple_of(me * own, GROUP), own)
    sides = ((me // 2) % 2, me // 4)

    def piece(which, other, p):
        side = 1 - sides[which] if other else sides[which]
        start = p * 2 * quarter + side * quarter if which == 0 else side * 2 * quarter + p * quarter
        return pl.ds(pl.multiple_of(start, quarter), quarter)

    def load(src, dst, at):
        copy = pltpu.make_async_copy(src, dst, local_sem.at[at])
        copy.start()
        return copy

    par_load = load(par_hbm.at[:, my_cols], allp.at[my_rows, my_cols], 0)

    gate = n - 1
    barrier = pltpu.get_barrier_semaphore()

    def tell(sem, plane, index):
        pl.semaphore_signal(sem, inc=1, device_id=(plane, index), device_id_type=pl.DeviceIdType.MESH)

    partner = flip(me, 1, n)
    high = me // 4
    early = (me + high + 1) % 2
    for mask in (2, 4):
        host = flip(me, mask, n) // 2 * 2 + 1 - high
        tell(barrier, mz, jnp.where(host == gate, gate - 1, host))

    @pl.when(partner != gate)
    def greet():
        tell(barrier, mz, partner)

    @pl.when(me < gate - 1)
    def meet():
        pl.semaphore_wait(barrier, 3)

    @pl.when(me == gate - 1)
    def meet_all():
        pl.semaphore_wait(barrier, 5)

    @pl.when(me != gate)
    def pass_on():
        tell(ready, mz, partner)

    @pl.when(me == gate)
    def enter():
        pl.semaphore_wait(ready, 1)

    def meet_side():
        @pl.when(me < gate - 1)
        def side():
            pl.semaphore_wait(ready, 1)

        tell(corner, mz, flip(me, 2, n))

    def meet_planes():
        pl.semaphore_wait(corner, 1)

        @pl.when(me == gate)
        def spread():
            for k in range(1, m):
                tell(barrier, flip(mz, k, m), gate)
            pl.semaphore_wait(barrier, m - 1)
            for k in range(1, n):
                tell(planes, mz, flip(me, k, n))

        @pl.when(me != gate)
        def follow():
            pl.semaphore_wait(planes, 1)

    def to_expert(src, dst, send, recv, k):
        return pltpu.make_async_remote_copy(
            src_ref=src, dst_ref=dst, send_sem=send, recv_sem=recv,
            device_id=(mz, flip(me, k, n)), device_id_type=pl.DeviceIdType.MESH,
        )

    def to_dp(src, dst, sems):
        for k in range(1, m):
            pltpu.make_async_remote_copy(
                src_ref=src(k), dst_ref=dst(k), send_sem=sems.at[0], recv_sem=sems.at[1],
                device_id=(flip(mz, k, m), me), device_id_type=pl.DeviceIdType.MESH,
            ).start()

    def send(src, dst, sems, k, at=1):
        to_expert(src, dst, sems.at[0], sems.at[at], k).start()

    groups = []

    def group(every, sems):
        groups.append(to_expert(every, every, sems.at[0], sems.at[1], 1))
        return groups[-1]

    def landed(every, sems, at):
        return to_expert(every, every, sems.at[0], sems.at[at], 1)

    def arrive(moved):
        moved.wait_recv()

    def rows_of(mask, start, size):
        return pl.ds(pl.multiple_of(flip(me, mask, n) * own + start, GROUP), size)

    def open_axis(q):
        send(par_hbm.at[:, my_cols], allp.at[my_rows, my_cols], p_sems, 2 + 2 * q)
        send(go_hbm.at[pl.ds(q * half, half)], mate.at[q], o_sems, 2 + 2 * q)

    open_axis(early)
    meet_side()
    open_axis(1 - early)
    so_load = load(so_hbm, so, 1)
    go_load = load(go_hbm, go, 2)
    arrive(landed(allp.at[pl.ds(0, 2 * own), my_cols], p_sems, 1))
    for q in range(2):
        block = allp.at[rows_of(4 - 2 * q, (1 - q) * (own // 2), own // 2), my_cols]
        send(block, block, p_sems, AXES[q][0], 2)
    tok_load = load(tok_hbm, tok, 3)
    r_moved = landed(allp.at[pl.ds(0, own), my_cols], p_sems, 2)
    group(allp.at[pl.ds(0, 3 * own), my_cols], p_sems)
    o_moved = group(mate, o_sems)

    so_load.wait()
    out_r = lax.broadcasted_iota(jnp.int32, (imgs * GROUP, GROUP * all_img), 0)
    in_c = lax.broadcasted_iota(jnp.int32, (imgs * GROUP, GROUP * all_img), 1)
    base = in_c - (out_r % GROUP) * all_img - (out_r // GROUP) % half
    first = out_r < half * GROUP

    def relayout(q, dest, out):
        own_at = dest * imgs + q * half
        mate_at = flip(dest, AXES[q][0], n) * imgs + q * half
        pick = jnp.where(base == jnp.where(first, own_at, mate_at), 1.0, 0.0).astype(BF)

        def one(g, carry):
            s0 = pl.multiple_of(g * GROUP, GROUP)
            block = so[pl.ds(s0, GROUP)].reshape(GROUP * all_img, width)
            moved = jnp.dot(pick, block, preferred_element_type=F32).astype(BF)
            out[:, pl.ds(s0, GROUP), :] = moved.reshape(imgs, GROUP, width)
            return carry

        lax.fori_loop(0, own // GROUP, one, 0)

    for i in range(3):
        for q in range(2):
            k = AXES[q][1][i]
            relayout(q, flip(me, k, n), stage.at[q, i])
            send(stage.at[q, i], rows.at[q, side_spot(q, me)], a_sems, k)
    a_moved = group(stage, a_sems)
    for q in range(2):
        relayout(q, me, rows.at[q, side_spot(q, me)])

    par_load.wait()
    arrive(r_moved)
    meet_planes()
    for i in range(n // 2):
        block = allp.at[rows_of(2 * i, 0, own), my_cols]
        to_dp(lambda k: block, lambda k: block, q_sems)
    q_moved = group(precv.at[pl.ds(1, m - 1)], q_sems)
    go_load.wait()
    tok_load.wait()
    arrive(q_moved)
    for i in range(n // 2):
        block = allp.at[rows_of(2 * i, 0, own)]
        send(block, block, f_sems, 1)
    f_moved = landed(allp.at[pl.ds(0, n // 2 * own)], f_sems, 1)
    arrive(f_moved)

    for q in range(2):

        def forward(t, carry):
            b = q * half + t
            logits = rows_last(allp[...], tok[b])
            peak = jnp.max(logits, axis=0, keepdims=True)
            raised = jnp.exp(logits - peak)
            comb[b] = raised / jnp.sum(raised, axis=0, keepdims=True)
            for p in range(2):
                low[q, t, p * quarter : (p + 1) * quarter] = comb[b, piece(q, False, p)].astype(BF)
                low_send[q, t, p * quarter : (p + 1) * quarter] = comb[b, piece(q, True, p)].astype(BF)
            return carry

        lax.fori_loop(0, half, forward, 0)
        send(low_send.at[q], low.at[q, pl.ds(half, half)], w_sems, AXES[q][0])
    w_moved = landed(low_send, w_sems, 1)

    def slot_grads(q, i, grads_in):
        out = jnp.dot(low[q, i], grads_in, preferred_element_type=F32).astype(BF)
        gs[q, :, i] = out.reshape(4, own, width)

    def comb_grads(q, i, grads_in):
        return rows_last(rows[q, :, i].reshape(4 * own, width), grads_in)

    for q in range(2):

        def own_slots(t, carry):
            slot_grads(q, t, go[q * half + t])
            return carry

        lax.fori_loop(0, half, own_slots, 0)

    arrive(o_moved)
    arrive(a_moved)
    for q in range(2):

        def mate_comb(t, carry):
            gc_send[q, t] = comb_grads(q, half + t, mate[q, t]).astype(BF)
            return carry

        lax.fori_loop(0, half, mate_comb, 0)
        send(gc_send.at[q], gc_recv.at[q], w_sems, AXES[q][0], 2)
    c_moved = landed(gc_send, w_sems, 2)
    group(low, w_sems)

    chunks = own // GROUP

    def landing(holder, images, j):
        if j == chunks - 1:
            return last.at[holder, images]
        return grec.at[holder, images, pl.ds(j * GROUP, GROUP)]

    def return_grads(h, parts, steps=(0, 1, 2)):
        part = pl.ds(h * half, half)
        for j in parts:
            for i in steps:
                for q in range(2):
                    k = AXES[q][1][i]
                    holder = flip(me, AXES[q][0], n) if h else me
                    send(
                        gs.at[q, side_spot(q, flip(me, k, n)), part, pl.ds(j * GROUP, GROUP)],
                        landing(holder, pl.ds(q * half, half), j), g_sems, k, 1 + j,
                    )
            for q in range(2 if 2 in steps else 0):
                holder = flip(me, AXES[q][0], n) if h else me
                pltpu.make_async_copy(
                    gs.at[q, side_spot(q, me), part, pl.ds(j * GROUP, GROUP)],
                    landing(holder, pl.ds(q * half, half), j), keep_sem.at[j // (chunks - 1)],
                ).start()

    def all_grads(j, holders):
        return last.at[:holders] if j == chunks - 1 else grec.at[:holders, :, pl.ds(j * GROUP, GROUP)]

    g_moved = [landed(all_grads(j, n - 2), g_sems, 1 + j) for j in range(chunks)]
    group(gs.at[:, pl.ds(0, 3)], g_sems)

    return_grads(0, range(chunks))
    arrive(w_moved)
    for q in range(2):

        def mate_slots(t, carry):
            slot_grads(q, half + t, mate[q, t])
            return carry

        lax.fori_loop(0, half, mate_slots, 0)
    return_grads(1, range(chunks - 2))

    for q in range(2):

        def own_comb(t, carry):
            grads = comb_grads(q, t, go[q * half + t])
            for p in range(2):
                gcf[q * half + t, piece(q, False, p)] = grads[p * quarter : (p + 1) * quarter]
            return carry

        lax.fori_loop(0, half, own_comb, 0)
    acc[...] = jnp.zeros_like(acc)
    arrive(c_moved)
    for q in range(2):

        def backward(t, carry):
            b = q * half + t
            for p in range(2):
                gcf[b, piece(q, True, p)] = gc_recv[q, t, p * quarter : (p + 1) * quarter].astype(F32)
            grad_comb = gcf[b]
            weights = comb[b]
            rowdot = jnp.sum(weights * grad_comb, axis=0, keepdims=True)
            wide = weights * (grad_comb - rowdot)
            gcf[b] = wide
            acc[...] += jnp.dot(wide.astype(BF), tok[b], preferred_element_type=F32)
            return carry

        lax.fori_loop(0, half, backward, 0)

    core = me % 2
    for i in range(n // 2):
        ksend[i] = acc[pl.ds(pl.multiple_of((2 * i + 1 - core) * own, GROUP), own)].astype(BF)
    send(ksend, krecv, f_sems, 1, 2)
    k_moved = landed(ksend, f_sems, 2)
    group(allp, f_sems)
    arrive(k_moved)
    for i in range(n // 2):
        red[i] = acc[pl.ds(pl.multiple_of((2 * i + core) * own, GROUP), own)] + krecv[i].astype(F32)
    for k in range(1, m):
        there = flip(mz, k, m)
        psend[k] = red[:, :, pl.ds(pl.multiple_of(there * cols, 128), cols)].astype(BF)
    to_dp(lambda k: psend.at[k], lambda k: precv.at[k], z_sems)
    z_moved = group(psend.at[pl.ds(1, m - 1)], z_sems)

    def token_grads(b, carry):
        gt[b] = jnp.dot(gcf[b].T.astype(BF), allp[...], preferred_element_type=F32).astype(BF)
        return carry

    lax.fori_loop(0, imgs, token_grads, 0)
    arrive(z_moved)
    total = red[:, :, my_cols]
    for k in range(1, m):
        total = total + precv[k].astype(F32)
    red[:, :, my_cols] = total

    def share(mask, q):
        return flip(me, mask, n) // 2, slice(q * (own // 2), (q + 1) * (own // 2)), my_cols

    for q in range(2):
        for i, mask in enumerate((AXES[q][0], 6)):
            xsend[q, i] = red[share(mask, q)].astype(BF)
        send(xsend.at[q, pl.ds(0, 2)], xrecv.at[q, pl.ds(0, 2)], x_sems, AXES[q][0])
    x_moved = landed(xsend.at[:, pl.ds(0, 2)], x_sems, 1)
    return_grads(1, (chunks - 2,))
    return_grads(1, (chunks - 1,), (0,))

    def settle_grads(j):
        arrive(g_moved[j])

        def swap(c, carry):
            lanes = pl.ds(pl.multiple_of(c * LANES, LANES), LANES)
            block = grec[:, :, j * GROUP : (j + 1) * GROUP, lanes].reshape(n * imgs, GROUP, LANES)
            done[j * GROUP : (j + 1) * GROUP, :, lanes] = jnp.swapaxes(block, 0, 1)
            return carry

        lax.fori_loop(0, width // LANES, swap, 0)

    pltpu.make_async_copy(grec.at[:2], grec.at[:2], keep_sem.at[0]).wait()
    for j in range(chunks - 3):
        settle_grads(j)
    arrive(x_moved)
    for q in range(2):
        for i, mask in enumerate((0, 4 - 2 * q)):
            red[share(mask, q)] += xrecv[q, i].astype(F32)
        xsend[q, 2] = red[share(4 - 2 * q, q)].astype(BF)
        send(xsend.at[q, 2], xrecv.at[q, 2], x_sems, 4 - 2 * q, 2)
    y_moved = landed(xsend.at[:, 2], x_sems, 2)
    group(xsend, x_sems)
    return_grads(1, (chunks - 1,), (1, 2))
    for j in range(chunks - 3, chunks - 1):
        settle_grads(j)
    arrive(y_moved)
    for q in range(2):
        gp[q * (own // 2) : (q + 1) * (own // 2)] = red[share(0, q)] + xrecv[q, 2].astype(F32)
    every = all_grads(chunks - 1, 2)
    pltpu.make_async_copy(every, every, keep_sem.at[1]).wait()
    for moved in groups:
        moved.wait_send()
    arrive(g_moved[chunks - 1])


def paired_exchange(n, m, tok, go, so, par):
    imgs, patches, width = tok.shape
    own, all_img, _ = so.shape
    slots, cols, half = own * n, width // m, imgs // 2
    dma = pltpu.SemaphoreType.DMA
    return pl.pallas_call(
        functools.partial(paired_kernel, n, m),
        out_shape=(
            pltpu.VMEM((own - GROUP, all_img, width), BF),
            pltpu.VMEM((n, imgs, GROUP, width), BF),
            pltpu.VMEM((imgs, patches, width), BF),
            pltpu.VMEM((own, cols), F32),
        ),
        in_specs=[pl.BlockSpec(memory_space=pl.ANY)] * 4,
        out_specs=(pl.BlockSpec(memory_space=pltpu.VMEM),) * 4,
        scratch_shapes=[
            pltpu.VMEM((imgs, patches, width), BF),
            pltpu.VMEM((imgs, patches, width), BF),
            pltpu.VMEM((2, half, patches, width), BF),
            pltpu.VMEM((own, all_img, width), BF),
            pltpu.VMEM((slots, width), BF),
            pltpu.VMEM((2, 3, imgs, own, width), BF),
            pltpu.VMEM((2, 4, imgs, own, width), BF),
            pltpu.VMEM((2, 4, imgs, own, width), BF),
            pltpu.VMEM((imgs, slots, patches), F32),
            pltpu.VMEM((imgs, slots, patches), F32),
            pltpu.VMEM((2, imgs, slots // 2, patches), BF),
            pltpu.VMEM((2, half, slots // 2, patches), BF),
            pltpu.VMEM((2, half, slots // 2, patches), BF),
            pltpu.VMEM((2, half, slots // 2, patches), BF),
            pltpu.VMEM((n, imgs, own - GROUP, width), BF),
            pltpu.VMEM((slots, width), F32),
            pltpu.VMEM((n // 2, own, width), BF),
            pltpu.VMEM((n // 2, own, width), BF),
            pltpu.VMEM((n // 2, own, width), F32),
            pltpu.VMEM((m, n // 2, own, cols), BF),
            pltpu.VMEM((m, n // 2, own, cols), BF),
            pltpu.VMEM((2, 3, own // 2, cols), BF),
            pltpu.VMEM((2, 3, own // 2, cols), BF),
            pltpu.SemaphoreType.REGULAR, pltpu.SemaphoreType.REGULAR, pltpu.SemaphoreType.REGULAR,
            dma((4,)), dma((2,)), dma((3,)), dma((2,)), dma((3,)), dma((2,)), dma((2,)), dma((3,)),
            dma((own // GROUP + 1,)), dma((2,)), dma((3,)),
        ],
        compiler_params=pltpu.CompilerParams(
            collective_id=0, has_side_effects=True, vmem_limit_bytes=56 * 1000 * 1000
        ),
    )(tok, go, so, par)


def settle_kernel(arrived, gp_in, out, gp_out):
    out[...] = jnp.swapaxes(arrived[...], 0, 1)
    gp_out[...] = gp_in[...]


def settle(arrived, grad_par):
    all_img, own, width = arrived.shape
    small = pl.BlockSpec((GROUP, grad_par.shape[1]), lambda i: (i, 0))
    return pl.pallas_call(
        settle_kernel,
        grid=(own // GROUP,),
        out_shape=(
            jax.ShapeDtypeStruct((own, all_img, width), BF),
            jax.ShapeDtypeStruct(grad_par.shape, F32),
        ),
        in_specs=[pl.BlockSpec((all_img, GROUP, width), lambda i: (0, i, 0)), small],
        out_specs=(pl.BlockSpec((GROUP, all_img, width), lambda i: (i, 0, 0)), small),
    )(arrived, grad_par)


def finish_kernel(done, last, gt, gp, slot_out, tok_out, par_out, turned, sem):
    own = done.shape[0]
    group, all_img, width = turned.shape
    copies = []

    def put(src, dst, at):
        copies.append(pltpu.make_async_copy(src, dst, sem.at[at]))
        copies[-1].start()

    for g in range(own // group):
        rows = pl.ds(g * group, group)
        put(done.at[rows], slot_out.at[rows], 0)
    for b in range(gt.shape[0]):
        put(gt.at[b], tok_out.at[b], 1)
    put(gp, par_out, 2)
    tiles = width // LANES
    for part in range(2):

        def swap(c, carry):
            lanes = pl.ds(pl.multiple_of((part * (tiles // 2) + c) * LANES, LANES), LANES)
            turned[:, :, lanes] = jnp.swapaxes(last[:, :, :, lanes].reshape(all_img, group, LANES), 0, 1)
            return carry

        lax.fori_loop(0, tiles // 2, swap, 0)
        lanes = pl.ds(part * (width // 2), width // 2)
        put(turned.at[:, :, lanes], slot_out.at[pl.ds(own, group), :, lanes], 3)
    for copy in copies:
        copy.wait()


def finish(done, last, gt, gp):
    own, all_img, width = done.shape
    return pl.pallas_call(
        finish_kernel,
        out_shape=(
            jax.ShapeDtypeStruct((own + GROUP, all_img, width), BF),
            jax.ShapeDtypeStruct(gt.shape, BF),
            jax.ShapeDtypeStruct(gp.shape, F32),
        ),
        in_specs=[pl.BlockSpec(memory_space=pltpu.VMEM)] * 4,
        out_specs=(pl.BlockSpec(memory_space=pl.ANY),) * 3,
        scratch_shapes=[pltpu.VMEM((GROUP, all_img, width), BF), pltpu.SemaphoreType.DMA((4,))],
        compiler_params=pltpu.CompilerParams(vmem_limit_bytes=16 * 1000 * 1000),
    )(done, last, gt, gp)


def per_device(n, m, tokens, grad_out, slot_out, slot_params):
    tok = jnp.transpose(tokens, (1, 0, 2))
    go = jnp.transpose(grad_out, (1, 0, 2))
    if n == 8 and tok.shape[0] % 2 == 0 and tok.shape[0] > 2:
        grad_slot, grad_tok, grad_par = finish(*paired_exchange(n, m, tok, go, slot_out, slot_params))
    else:
        arrived, grad_tok, grad_par = exchange(n, m, tok, go, slot_out, slot_params)
        own, all_img, width = slot_out.shape
        grad_slot, grad_par = settle(arrived.reshape(all_img, own, width), grad_par)
    return jnp.transpose(grad_tok, (1, 0, 2)), grad_slot, grad_par


def solution(mesh):
    return jax.shard_map(
        functools.partial(per_device, mesh.shape["expert"], mesh.shape["dp"]),
        mesh=mesh,
        in_specs=(
            P(None, ("dp", "expert"), None),
            P(None, ("dp", "expert"), None),
            P("expert", "dp", None),
            P("expert", None),
        ),
        out_specs=(P(None, ("dp", "expert"), None), P("expert", "dp", None), P("expert", "dp")),
        check_vma=False,
    )
```

```python
import functools

import jax
import jax.numpy as jnp
from jax import lax
from jax.experimental import pallas as pl
from jax.experimental.pallas import tpu as pltpu
from jax.sharding import PartitionSpec as P

BF = jnp.bfloat16
F32 = jnp.float32
GROUP = 16
LANES = 128


def flip(index, mask, size):
    total, bit = 0, 1
    while bit < size:
        total = total + ((index // bit + mask // bit) % 2) * bit
        bit *= 2
    return total


def send_order(n, core):
    if n != 8:
        return list(range(n - 1, 0, -1))
    masks = []
    for low in range(2):
        masks += [6 + low - 4 * core, 2 + low + 2 * core, 4 + low + 2 * core]
    return masks + [1]


def rows_last(lhs, rhs):
    return lax.dot_general(lhs, rhs, (((1,), (1,)), ((), ())), preferred_element_type=F32)


def exchange_kernel(
    n, m, tok_hbm, go_hbm, so_hbm, par_hbm,
    grec, gt_out, gp_out,
    tok, go, so, par, allp, stage, rows, gs, comb, gt, acc, psend, precv, xsend, xrecv, gp,
    local_sem, p_send, p_recv, q_send, q_recv, a_send, a_recv, g_send, g_recv,
    z_send, z_recv, x_send, x_recv,
):
    me = lax.axis_index("expert")
    mz = lax.axis_index("dp")
    core = me % 2
    imgs = tok.shape[0]
    own = par.shape[0]
    all_img = so.shape[1]
    cols = allp.shape[1] // m
    width = allp.shape[1]
    slots = allp.shape[0]
    my_cols = pl.ds(pl.multiple_of(mz * cols, 128), cols)
    my_rows = pl.ds(pl.multiple_of(me * own, GROUP), own)

    loads = [
        pltpu.make_async_copy(src, dst, local_sem.at[i])
        for i, (src, dst) in enumerate([(par_hbm, par), (so_hbm, so), (tok_hbm, tok), (go_hbm, go)])
    ]
    for load in loads:
        load.start()

    barrier = pltpu.get_barrier_semaphore()
    for k in range(1, n):
        pl.semaphore_signal(barrier, inc=1, device_id=(mz, flip(me, k, n)), device_id_type=pl.DeviceIdType.MESH)
    for k in range(1, m):
        pl.semaphore_signal(barrier, inc=1, device_id=(flip(mz, k, m), me), device_id_type=pl.DeviceIdType.MESH)
    pl.semaphore_wait(barrier, n + m - 2)

    def to_expert(src, dst, send, recv, k):
        return pltpu.make_async_remote_copy(
            src_ref=src, dst_ref=dst, send_sem=send.at[k], recv_sem=recv.at[k],
            device_id=(mz, flip(me, k, n)), device_id_type=pl.DeviceIdType.MESH,
        )

    def to_dp(src, dst, send, recv, k):
        return pltpu.make_async_remote_copy(
            src_ref=src, dst_ref=dst, send_sem=send.at[k], recv_sem=recv.at[k],
            device_id=(flip(mz, k, m), me), device_id_type=pl.DeviceIdType.MESH,
        )

    loads[0].wait()
    p_copies = [to_expert(par.at[:, my_cols], allp.at[my_rows, my_cols], p_send, p_recv, k) for k in range(1, n)]
    for copy in p_copies:
        copy.start()
    allp[my_rows, my_cols] = par[:, my_cols]

    loads[1].wait()
    out_r = lax.broadcasted_iota(jnp.int32, (imgs * GROUP, GROUP * all_img), 0)
    in_c = lax.broadcasted_iota(jnp.int32, (imgs * GROUP, GROUP * all_img), 1)
    base = in_c - (out_r % GROUP) * all_img - out_r // GROUP

    def relayout(dest, out):
        pick = jnp.where(base == dest * imgs, 1.0, 0.0).astype(BF)

        def one(g, carry):
            s0 = pl.multiple_of(g * GROUP, GROUP)
            block = so[pl.ds(s0, GROUP)].reshape(GROUP * all_img, width)
            moved = jnp.dot(pick, block, preferred_element_type=F32).astype(BF)
            out[:, pl.ds(s0, GROUP), :] = moved.reshape(imgs, GROUP, width)
            return carry

        lax.fori_loop(0, own // GROUP, one, 0)

    order = send_order(n, core)
    a_copies = []
    for k in order:
        relayout(flip(me, k, n), stage.at[k])
        copy = to_expert(stage.at[k], rows.at[me], a_send, a_recv, k)
        copy.start()
        a_copies.append(copy)
    relayout(me, rows.at[me])

    for copy in p_copies:
        copy.wait_recv()
    q_copies = [to_dp(allp.at[:, my_cols], allp.at[:, my_cols], q_send, q_recv, k) for k in range(1, m)]
    for copy in q_copies:
        copy.start()
    loads[2].wait()
    loads[3].wait()
    for copy in q_copies:
        copy.wait_recv()

    def forward(b, carry):
        logits = rows_last(allp[...], tok[b])
        peak = jnp.max(logits, axis=0, keepdims=True)
        raised = jnp.exp(logits - peak)
        weights = raised / jnp.sum(raised, axis=0, keepdims=True)
        comb[b] = weights
        grads = jnp.dot(weights.astype(BF), go[b], preferred_element_type=F32).astype(BF)
        gs[:, b] = grads.reshape(n, own, width)
        return carry

    lax.fori_loop(0, imgs, forward, 0)

    keep = pltpu.make_async_copy(gs.at[me], grec.at[me], local_sem.at[4])
    keep.start()
    g_copies = []
    for k in order:
        copy = to_expert(gs.at[flip(me, k, n)], grec.at[me], g_send, g_recv, k)
        copy.start()
        g_copies.append(copy)

    for copy in a_copies:
        copy.wait_recv()
    acc[...] = jnp.zeros_like(acc)

    def backward(b, carry):
        grad_comb = rows_last(rows[:, b].reshape(slots, width), go[b])
        weights = comb[b]
        rowdot = jnp.sum(weights * grad_comb, axis=0, keepdims=True)
        wide = weights * (grad_comb - rowdot)
        acc[...] += jnp.dot(wide.astype(BF), tok[b], preferred_element_type=F32)
        gt[b] = jnp.dot(wide.T.astype(BF), allp[...], preferred_element_type=F32).astype(BF)
        return carry

    lax.fori_loop(0, imgs, backward, 0)

    for k in range(1, m):
        there = flip(mz, k, m)
        psend[k] = acc[:, pl.ds(pl.multiple_of(there * cols, 128), cols)].astype(BF)
    z_copies = [to_dp(psend.at[k], precv.at[k], z_send, z_recv, k) for k in range(1, m)]
    for copy in z_copies:
        copy.start()
    put = pltpu.make_async_copy(gt, gt_out, local_sem.at[5])
    put.start()
    for copy in z_copies:
        copy.wait_recv()
    total = acc[:, my_cols]
    for k in range(1, m):
        total = total + precv[k].astype(F32)
    acc[:, my_cols] = total
    for k in range(1, n):
        there = flip(me, k, n)
        xsend[k] = acc[pl.ds(pl.multiple_of(there * own, GROUP), own), my_cols].astype(BF)
    x_copies = [to_expert(xsend.at[k], xrecv.at[k], x_send, x_recv, k) for k in range(1, n)]
    for copy in x_copies:
        copy.start()
    for copy in x_copies:
        copy.wait_recv()
    owned = acc[my_rows, my_cols]
    for k in range(1, n):
        owned = owned + xrecv[k].astype(F32)
    gp[...] = owned
    give = pltpu.make_async_copy(gp, gp_out, local_sem.at[6])
    give.start()

    for copy in g_copies:
        copy.wait_recv()
    for copy in p_copies + a_copies + q_copies + g_copies + z_copies + x_copies:
        copy.wait_send()
    keep.wait()
    put.wait()
    give.wait()


def exchange(n, m, tok, go, so, par):
    imgs, patches, width = tok.shape
    own, all_img, _ = so.shape
    slots, cols = own * n, width // m
    dma = pltpu.SemaphoreType.DMA
    return pl.pallas_call(
        functools.partial(exchange_kernel, n, m),
        out_shape=(
            jax.ShapeDtypeStruct((n, imgs, own, width), BF),
            jax.ShapeDtypeStruct((imgs, patches, width), BF),
            jax.ShapeDtypeStruct((own, cols), F32),
        ),
        in_specs=[pl.BlockSpec(memory_space=pl.ANY)] * 4,
        out_specs=(pl.BlockSpec(memory_space=pl.ANY),) * 3,
        scratch_shapes=[
            pltpu.VMEM((imgs, patches, width), BF),
            pltpu.VMEM((imgs, patches, width), BF),
            pltpu.VMEM((own, all_img, width), BF),
            pltpu.VMEM((own, width), BF),
            pltpu.VMEM((slots, width), BF),
            pltpu.VMEM((n, imgs, own, width), BF),
            pltpu.VMEM((n, imgs, own, width), BF),
            pltpu.VMEM((n, imgs, own, width), BF),
            pltpu.VMEM((imgs, slots, patches), F32),
            pltpu.VMEM((imgs, patches, width), BF),
            pltpu.VMEM((slots, width), F32),
            pltpu.VMEM((m, slots, cols), BF),
            pltpu.VMEM((m, slots, cols), BF),
            pltpu.VMEM((n, own, cols), BF),
            pltpu.VMEM((n, own, cols), BF),
            pltpu.VMEM((own, cols), F32),
            dma((7,)),
            dma((n,)), dma((n,)), dma((m,)), dma((m,)),
            dma((n,)), dma((n,)), dma((n,)), dma((n,)),
            dma((m,)), dma((m,)), dma((n,)), dma((n,)),
        ],
        compiler_params=pltpu.CompilerParams(
            collective_id=0, has_side_effects=True, vmem_limit_bytes=66 * 1000 * 1000
        ),
    )(tok, go, so, par)


AXES = ((2, (4, 5, 1)), (4, (2, 3, 1)))


def side_spot(which, index):
    high = index // 4 if which == 0 else (index // 2) % 2
    return high * 2 + index % 2


def paired_kernel(
    n, m, tok_hbm, go_hbm, so_hbm, par_hbm,
    done, last, gt, gp,
    tok, go, mate, so, allp, stage, rows, gs, comb, gcf, low, low_send, gc_send, gc_recv,
    grec, acc, ksend, krecv, red, psend, precv, xsend, xrecv,
    ready, corner, planes, local_sem, keep_sem, p_sems, q_sems, f_sems, o_sems, a_sems, w_sems,
    g_sems, z_sems, x_sems,
):
    me = lax.axis_index("expert")
    mz = lax.axis_index("dp")
    imgs = tok.shape[0]
    half = imgs // 2
    own = par_hbm.shape[0]
    all_img = so.shape[1]
    slots, width = allp.shape
    patches = tok.shape[1]
    cols = width // m
    quarter = slots // 4
    my_cols = pl.ds(pl.multiple_of(mz * cols, 128), cols)
    my_rows = pl.ds(pl.multiple_of(me * own, GROUP), own)
    sides = ((me // 2) % 2, me // 4)

    def piece(which, other, p):
        side = 1 - sides[which] if other else sides[which]
        start = p * 2 * quarter + side * quarter if which == 0 else side * 2 * quarter + p * quarter
        return pl.ds(pl.multiple_of(start, quarter), quarter)

    def load(src, dst, at):
        copy = pltpu.make_async_copy(src, dst, local_sem.at[at])
        copy.start()
        return copy

    gate = n - 1
    barrier = pltpu.get_barrier_semaphore()

    def tell(sem, plane, index):
        pl.semaphore_signal(sem, inc=1, device_id=(plane, index), device_id_type=pl.DeviceIdType.MESH)

    partner = flip(me, 1, n)
    high = me // 4
    early = (me + high + 1) % 2
    for mask in (2, 4):
        host = flip(me, mask, n) // 2 * 2 + 1 - high
        tell(barrier, mz, jnp.where(host == gate, gate - 1, host))

    @pl.when(partner != gate)
    def greet():
        tell(barrier, mz, partner)

    @pl.when(me < gate - 1)
    def meet():
        pl.semaphore_wait(barrier, 3)

    @pl.when(me == gate - 1)
    def meet_all():
        pl.semaphore_wait(barrier, 5)

    @pl.when(me != gate)
    def pass_on():
        tell(ready, mz, partner)

    @pl.when(me == gate)
    def enter():
        pl.semaphore_wait(ready, 1)

    def meet_side():
        @pl.when(me < gate - 1)
        def side():
            pl.semaphore_wait(ready, 1)

        tell(corner, mz, flip(me, 2, n))

    def meet_planes():
        pl.semaphore_wait(corner, 1)

        @pl.when(me == gate)
        def spread():
            for k in range(1, m):
                tell(barrier, flip(mz, k, m), gate)
            pl.semaphore_wait(barrier, m - 1)
            for k in range(1, n):
                tell(planes, mz, flip(me, k, n))

        @pl.when(me != gate)
        def follow():
            pl.semaphore_wait(planes, 1)

    def to_expert(src, dst, send, recv, k):
        return pltpu.make_async_remote_copy(
            src_ref=src, dst_ref=dst, send_sem=send, recv_sem=recv,
            device_id=(mz, flip(me, k, n)), device_id_type=pl.DeviceIdType.MESH,
        )

    def to_dp(src, dst, sems):
        for k in range(1, m):
            pltpu.make_async_remote_copy(
                src_ref=src(k), dst_ref=dst(k), send_sem=sems.at[0], recv_sem=sems.at[1],
                device_id=(flip(mz, k, m), me), device_id_type=pl.DeviceIdType.MESH,
            ).start()

    def send(src, dst, sems, k, at=1):
        to_expert(src, dst, sems.at[0], sems.at[at], k).start()

    groups = []

    def group(every, sems):
        groups.append(to_expert(every, every, sems.at[0], sems.at[1], 1))
        return groups[-1]

    def landed(every, sems, at):
        return to_expert(every, every, sems.at[0], sems.at[at], 1)

    def arrive(moved):
        moved.wait_recv()

    def rows_of(mask, start, size):
        return pl.ds(pl.multiple_of(flip(me, mask, n) * own + start, GROUP), size)

    def open_axis(q):
        send(par_hbm.at[:, my_cols], allp.at[my_rows, my_cols], p_sems, 2 + 2 * q)
        send(go_hbm.at[q * half], mate.at[q, 0], o_sems, 2 + 2 * q)

    open_axis(early)
    meet_side()
    open_axis(1 - early)
    par_load = load(par_hbm.at[:, my_cols], allp.at[my_rows, my_cols], 0)
    so_load = load(so_hbm, so, 1)
    go_load = load(go_hbm, go, 2)
    arrive(landed(allp.at[pl.ds(0, 2 * own), my_cols], p_sems, 1))
    for q in range(2):
        block = allp.at[rows_of(4 - 2 * q, (1 - q) * (own // 2), own // 2), my_cols]
        send(block, block, p_sems, AXES[q][0], 2)
        send(go_hbm.at[pl.ds(q * half + 1, half - 1)], mate.at[q, pl.ds(1, half - 1)], o_sems, AXES[q][0])
    tok_load = load(tok_hbm, tok, 3)
    r_moved = landed(allp.at[pl.ds(0, own), my_cols], p_sems, 2)
    group(allp.at[pl.ds(0, 3 * own), my_cols], p_sems)
    o_moved = group(mate, o_sems)

    so_load.wait()
    out_r = lax.broadcasted_iota(jnp.int32, (imgs * GROUP, GROUP * all_img), 0)
    in_c = lax.broadcasted_iota(jnp.int32, (imgs * GROUP, GROUP * all_img), 1)
    base = in_c - (out_r % GROUP) * all_img - (out_r // GROUP) % half
    first = out_r < half * GROUP

    def relayout(q, dest, out):
        own_at = dest * imgs + q * half
        mate_at = flip(dest, AXES[q][0], n) * imgs + q * half
        pick = jnp.where(base == jnp.where(first, own_at, mate_at), 1.0, 0.0).astype(BF)

        def one(g, carry):
            s0 = pl.multiple_of(g * GROUP, GROUP)
            block = so[pl.ds(s0, GROUP)].reshape(GROUP * all_img, width)
            moved = jnp.dot(pick, block, preferred_element_type=F32).astype(BF)
            out[:, pl.ds(s0, GROUP), :] = moved.reshape(imgs, GROUP, width)
            return carry

        lax.fori_loop(0, own // GROUP, one, 0)

    for i in range(3):
        for q in range(2):
            k = AXES[q][1][i]
            relayout(q, flip(me, k, n), stage.at[q, i])
            send(stage.at[q, i], rows.at[q, side_spot(q, me)], a_sems, k)
    a_moved = group(stage, a_sems)
    for q in range(2):
        relayout(q, me, rows.at[q, side_spot(q, me)])

    par_load.wait()
    arrive(r_moved)
    meet_planes()
    for i in range(n // 2):
        block = allp.at[rows_of(2 * i, 0, own), my_cols]
        to_dp(lambda k: block, lambda k: block, q_sems)
    q_moved = group(precv.at[pl.ds(1, m - 1)], q_sems)
    go_load.wait()
    tok_load.wait()
    arrive(q_moved)
    for i in range(n // 2):
        block = allp.at[rows_of(2 * i, 0, own)]
        send(block, block, f_sems, 1)
    f_moved = landed(allp.at[pl.ds(0, n // 2 * own)], f_sems, 1)
    arrive(f_moved)

    for q in range(2):

        def forward(t, carry):
            b = q * half + t
            logits = rows_last(allp[...], tok[b])
            peak = jnp.max(logits, axis=0, keepdims=True)
            raised = jnp.exp(logits - peak)
            comb[b] = raised / jnp.sum(raised, axis=0, keepdims=True)
            for p in range(2):
                low[q, t, p * quarter : (p + 1) * quarter] = comb[b, piece(q, False, p)].astype(BF)
                low_send[q, t, p * quarter : (p + 1) * quarter] = comb[b, piece(q, True, p)].astype(BF)
            return carry

        lax.fori_loop(0, half, forward, 0)
        send(low_send.at[q], low.at[q, pl.ds(half, half)], w_sems, AXES[q][0])
    w_moved = landed(low_send, w_sems, 1)

    def slot_grads(q, i, grads_in):
        out = jnp.dot(low[q, i], grads_in, preferred_element_type=F32).astype(BF)
        gs[q, :, i] = out.reshape(4, own, width)

    def comb_grads(q, i, grads_in):
        return rows_last(rows[q, :, i].reshape(4 * own, width), grads_in)

    for q in range(2):

        def own_slots(t, carry):
            slot_grads(q, t, go[q * half + t])
            return carry

        lax.fori_loop(0, half, own_slots, 0)

    arrive(o_moved)
    arrive(a_moved)
    for q in range(2):

        def mate_comb(t, carry):
            gc_send[q, t] = comb_grads(q, half + t, mate[q, t]).astype(BF)
            return carry

        lax.fori_loop(0, half, mate_comb, 0)
        send(gc_send.at[q], gc_recv.at[q], w_sems, AXES[q][0], 2)
    c_moved = landed(gc_send, w_sems, 2)
    group(low, w_sems)

    chunks = own // GROUP

    def landing(holder, images, j):
        if j == chunks - 1:
            return last.at[holder, images]
        return grec.at[holder, images, pl.ds(j * GROUP, GROUP)]

    def return_grads(h, parts, steps=(0, 1, 2)):
        part = pl.ds(h * half, half)
        for j in parts:
            for i in steps:
                for q in range(2):
                    k = AXES[q][1][i]
                    holder = flip(me, AXES[q][0], n) if h else me
                    send(
                        gs.at[q, side_spot(q, flip(me, k, n)), part, pl.ds(j * GROUP, GROUP)],
                        landing(holder, pl.ds(q * half, half), j), g_sems, k, 1 + j,
                    )
            for q in range(2 if 2 in steps else 0):
                holder = flip(me, AXES[q][0], n) if h else me
                pltpu.make_async_copy(
                    gs.at[q, side_spot(q, me), part, pl.ds(j * GROUP, GROUP)],
                    landing(holder, pl.ds(q * half, half), j), keep_sem.at[j // (chunks - 1)],
                ).start()

    def all_grads(j, holders):
        return last.at[:holders] if j == chunks - 1 else grec.at[:holders, :, pl.ds(j * GROUP, GROUP)]

    g_moved = [landed(all_grads(j, n - 2), g_sems, 1 + j) for j in range(chunks)]
    group(gs.at[:, pl.ds(0, 3)], g_sems)

    return_grads(0, range(chunks))
    arrive(w_moved)
    for q in range(2):

        def mate_slots(t, carry):
            slot_grads(q, half + t, mate[q, t])
            return carry

        lax.fori_loop(0, half, mate_slots, 0)
    return_grads(1, range(chunks - 2))

    for q in range(2):

        def own_comb(t, carry):
            grads = comb_grads(q, t, go[q * half + t])
            for p in range(2):
                gcf[q * half + t, piece(q, False, p)] = grads[p * quarter : (p + 1) * quarter]
            return carry

        lax.fori_loop(0, half, own_comb, 0)
    acc[...] = jnp.zeros_like(acc)
    arrive(c_moved)
    for q in range(2):

        def backward(t, carry):
            b = q * half + t
            for p in range(2):
                gcf[b, piece(q, True, p)] = gc_recv[q, t, p * quarter : (p + 1) * quarter].astype(F32)
            grad_comb = gcf[b]
            weights = comb[b]
            rowdot = jnp.sum(weights * grad_comb, axis=0, keepdims=True)
            wide = weights * (grad_comb - rowdot)
            gcf[b] = wide
            acc[...] += jnp.dot(wide.astype(BF), tok[b], preferred_element_type=F32)
            return carry

        lax.fori_loop(0, half, backward, 0)

    core = me % 2
    for i in range(n // 2):
        ksend[i] = acc[pl.ds(pl.multiple_of((2 * i + 1 - core) * own, GROUP), own)].astype(BF)
    send(ksend, krecv, f_sems, 1, 2)
    k_moved = landed(ksend, f_sems, 2)
    group(allp, f_sems)
    arrive(k_moved)
    for i in range(n // 2):
        red[i] = acc[pl.ds(pl.multiple_of((2 * i + core) * own, GROUP), own)] + krecv[i].astype(F32)
    for k in range(1, m):
        there = flip(mz, k, m)
        psend[k] = red[:, :, pl.ds(pl.multiple_of(there * cols, 128), cols)].astype(BF)
    to_dp(lambda k: psend.at[k], lambda k: precv.at[k], z_sems)
    z_moved = group(psend.at[pl.ds(1, m - 1)], z_sems)

    def token_grads(b, carry):
        gt[b] = jnp.dot(gcf[b].T.astype(BF), allp[...], preferred_element_type=F32).astype(BF)
        return carry

    lax.fori_loop(0, imgs, token_grads, 0)
    arrive(z_moved)
    total = red[:, :, my_cols]
    for k in range(1, m):
        total = total + precv[k].astype(F32)
    red[:, :, my_cols] = total

    def share(mask, q):
        return flip(me, mask, n) // 2, slice(q * (own // 2), (q + 1) * (own // 2)), my_cols

    for q in range(2):
        for i, mask in enumerate((AXES[q][0], 6)):
            xsend[q, i] = red[share(mask, q)].astype(BF)
        send(xsend.at[q, pl.ds(0, 2)], xrecv.at[q, pl.ds(0, 2)], x_sems, AXES[q][0])
    x_moved = landed(xsend.at[:, pl.ds(0, 2)], x_sems, 1)
    return_grads(1, (chunks - 2,))
    return_grads(1, (chunks - 1,), (0,))

    def settle_grads(j):
        arrive(g_moved[j])

        def swap(c, carry):
            lanes = pl.ds(pl.multiple_of(c * LANES, LANES), LANES)
            block = grec[:, :, j * GROUP : (j + 1) * GROUP, lanes].reshape(n * imgs, GROUP, LANES)
            done[j * GROUP : (j + 1) * GROUP, :, lanes] = jnp.swapaxes(block, 0, 1)
            return carry

        lax.fori_loop(0, width // LANES, swap, 0)

    pltpu.make_async_copy(grec.at[:2], grec.at[:2], keep_sem.at[0]).wait()
    for j in range(chunks - 3):
        settle_grads(j)
    arrive(x_moved)
    for q in range(2):
        for i, mask in enumerate((0, 4 - 2 * q)):
            red[share(mask, q)] += xrecv[q, i].astype(F32)
        xsend[q, 2] = red[share(4 - 2 * q, q)].astype(BF)
        send(xsend.at[q, 2], xrecv.at[q, 2], x_sems, 4 - 2 * q, 2)
    y_moved = landed(xsend.at[:, 2], x_sems, 2)
    group(xsend, x_sems)
    return_grads(1, (chunks - 1,), (1, 2))
    for j in range(chunks - 3, chunks - 1):
        settle_grads(j)
    arrive(y_moved)
    for q in range(2):
        gp[q * (own // 2) : (q + 1) * (own // 2)] = red[share(0, q)] + xrecv[q, 2].astype(F32)
    every = all_grads(chunks - 1, 2)
    pltpu.make_async_copy(every, every, keep_sem.at[1]).wait()
    for moved in groups:
        moved.wait_send()
    arrive(g_moved[chunks - 1])


def paired_exchange(n, m, tok, go, so, par):
    imgs, patches, width = tok.shape
    own, all_img, _ = so.shape
    slots, cols, half = own * n, width // m, imgs // 2
    dma = pltpu.SemaphoreType.DMA
    return pl.pallas_call(
        functools.partial(paired_kernel, n, m),
        out_shape=(
            pltpu.VMEM((own - GROUP, all_img, width), BF),
            pltpu.VMEM((n, imgs, GROUP, width), BF),
            pltpu.VMEM((imgs, patches, width), BF),
            pltpu.VMEM((own, cols), F32),
        ),
        in_specs=[pl.BlockSpec(memory_space=pl.ANY)] * 4,
        out_specs=(pl.BlockSpec(memory_space=pltpu.VMEM),) * 4,
        scratch_shapes=[
            pltpu.VMEM((imgs, patches, width), BF),
            pltpu.VMEM((imgs, patches, width), BF),
            pltpu.VMEM((2, half, patches, width), BF),
            pltpu.VMEM((own, all_img, width), BF),
            pltpu.VMEM((slots, width), BF),
            pltpu.VMEM((2, 3, imgs, own, width), BF),
            pltpu.VMEM((2, 4, imgs, own, width), BF),
            pltpu.VMEM((2, 4, imgs, own, width), BF),
            pltpu.VMEM((imgs, slots, patches), F32),
            pltpu.VMEM((imgs, slots, patches), F32),
            pltpu.VMEM((2, imgs, slots // 2, patches), BF),
            pltpu.VMEM((2, half, slots // 2, patches), BF),
            pltpu.VMEM((2, half, slots // 2, patches), BF),
            pltpu.VMEM((2, half, slots // 2, patches), BF),
            pltpu.VMEM((n, imgs, own - GROUP, width), BF),
            pltpu.VMEM((slots, width), F32),
            pltpu.VMEM((n // 2, own, width), BF),
            pltpu.VMEM((n // 2, own, width), BF),
            pltpu.VMEM((n // 2, own, width), F32),
            pltpu.VMEM((m, n // 2, own, cols), BF),
            pltpu.VMEM((m, n // 2, own, cols), BF),
            pltpu.VMEM((2, 3, own // 2, cols), BF),
            pltpu.VMEM((2, 3, own // 2, cols), BF),
            pltpu.SemaphoreType.REGULAR, pltpu.SemaphoreType.REGULAR, pltpu.SemaphoreType.REGULAR,
            dma((4,)), dma((2,)), dma((3,)), dma((2,)), dma((3,)), dma((2,)), dma((2,)), dma((3,)),
            dma((own // GROUP + 1,)), dma((2,)), dma((3,)),
        ],
        compiler_params=pltpu.CompilerParams(
            collective_id=0, has_side_effects=True, vmem_limit_bytes=56 * 1000 * 1000
        ),
    )(tok, go, so, par)


def settle_kernel(arrived, gp_in, out, gp_out):
    out[...] = jnp.swapaxes(arrived[...], 0, 1)
    gp_out[...] = gp_in[...]


def settle(arrived, grad_par):
    all_img, own, width = arrived.shape
    small = pl.BlockSpec((GROUP, grad_par.shape[1]), lambda i: (i, 0))
    return pl.pallas_call(
        settle_kernel,
        grid=(own // GROUP,),
        out_shape=(
            jax.ShapeDtypeStruct((own, all_img, width), BF),
            jax.ShapeDtypeStruct(grad_par.shape, F32),
        ),
        in_specs=[pl.BlockSpec((all_img, GROUP, width), lambda i: (0, i, 0)), small],
        out_specs=(pl.BlockSpec((GROUP, all_img, width), lambda i: (i, 0, 0)), small),
    )(arrived, grad_par)


def finish_kernel(done, last, gt, gp, slot_out, tok_out, par_out, turned, sem):
    own = done.shape[0]
    group, all_img, width = turned.shape
    copies = []

    def put(src, dst, at):
        copies.append(pltpu.make_async_copy(src, dst, sem.at[at]))
        copies[-1].start()

    for g in range(own // group):
        rows = pl.ds(g * group, group)
        put(done.at[rows], slot_out.at[rows], 0)
    for b in range(gt.shape[0]):
        put(gt.at[b], tok_out.at[b], 1)
    put(gp, par_out, 2)
    tiles = width // LANES
    for part in range(2):

        def swap(c, carry):
            lanes = pl.ds(pl.multiple_of((part * (tiles // 2) + c) * LANES, LANES), LANES)
            turned[:, :, lanes] = jnp.swapaxes(last[:, :, :, lanes].reshape(all_img, group, LANES), 0, 1)
            return carry

        lax.fori_loop(0, tiles // 2, swap, 0)
        lanes = pl.ds(part * (width // 2), width // 2)
        put(turned.at[:, :, lanes], slot_out.at[pl.ds(own, group), :, lanes], 3)
    for copy in copies:
        copy.wait()


def finish(done, last, gt, gp):
    own, all_img, width = done.shape
    return pl.pallas_call(
        finish_kernel,
        out_shape=(
            jax.ShapeDtypeStruct((own + GROUP, all_img, width), BF),
            jax.ShapeDtypeStruct(gt.shape, BF),
            jax.ShapeDtypeStruct(gp.shape, F32),
        ),
        in_specs=[pl.BlockSpec(memory_space=pltpu.VMEM)] * 4,
        out_specs=(pl.BlockSpec(memory_space=pl.ANY),) * 3,
        scratch_shapes=[pltpu.VMEM((GROUP, all_img, width), BF), pltpu.SemaphoreType.DMA((4,))],
        compiler_params=pltpu.CompilerParams(vmem_limit_bytes=16 * 1000 * 1000),
    )(done, last, gt, gp)


def per_device(n, m, tokens, grad_out, slot_out, slot_params):
    tok = jnp.transpose(tokens, (1, 0, 2))
    go = jnp.transpose(grad_out, (1, 0, 2))
    if n == 8 and tok.shape[0] % 2 == 0 and tok.shape[0] > 2:
        grad_slot, grad_tok, grad_par = finish(*paired_exchange(n, m, tok, go, slot_out, slot_params))
    else:
        arrived, grad_tok, grad_par = exchange(n, m, tok, go, slot_out, slot_params)
        own, all_img, width = slot_out.shape
        grad_slot, grad_par = settle(arrived.reshape(all_img, own, width), grad_par)
    return jnp.transpose(grad_tok, (1, 0, 2)), grad_slot, grad_par


def solution(mesh):
    return jax.shard_map(
        functools.partial(per_device, mesh.shape["expert"], mesh.shape["dp"]),
        mesh=mesh,
        in_specs=(
            P(None, ("dp", "expert"), None),
            P(None, ("dp", "expert"), None),
            P("expert", "dp", None),
            P("expert", None),
        ),
        out_specs=(P(None, ("dp", "expert"), None), P("expert", "dp", None), P("expert", "dp")),
        check_vma=False,
    )
```
